16 devices in a mesh: replica: 2 (over z), model: 8 (over y, x, core).
Axes of the slice: x: 2, y: 2, z: 2, core: 2. Of those that a mesh axis runs over, the one named last changes fastest.
Arguments:
- prompt: bfloat16 [16, 1536, 2048], P('replica', 'model'), parts along dimension 0
- lengths: int32 [16], P('replica'), parts along dimension 0
- new_tok: bfloat16 [16, 2048], P('replica'), parts along dimension 0
- norm_attn: bfloat16 [1, 2048], replicated
- w_q: bfloat16 [1, 2048, 2048], P(None, None, 'model')
- w_k: bfloat16 [1, 2048, 2048], P(None, None, 'model')
- w_v: bfloat16 [1, 2048, 2048], P(None, None, 'model')
- w_o: bfloat16 [1, 2048, 2048], P(None, 'model')
- norm_mlp: bfloat16 [1, 2048], replicated
- w_gate: bfloat16 [1, 2048, 8192], P(None, None, 'model')
- w_up: bfloat16 [1, 2048, 8192], P(None, None, 'model')
- w_down: bfloat16 [1, 8192, 2048], P(None, 'model')
Outputs:
- output 1: bfloat16 [16, 2048], P('replica'), parts along dimension 0
- output 2: bfloat16 [16, 2048], P('replica'), parts along dimension 0
- output 3: bfloat16 [1, 16, 1537, 16, 128], P(None, 'replica', None, 'model'), parts along dimension 1
- output 4: bfloat16 [1, 16, 1537, 16, 128], P(None, 'replica', None, 'model'), parts along dimension 1
There are 2 independent parts. The reference program is written for one: setup_inputs(seed, part) draws one part's arguments, and reference() takes and returns one part's arrays. A program takes and returns all parts, laid end to end along the dimension named above; an argument that names none is the same for every part.
All inputs are finite; a program needn't handle non-finite values.
Results may differ from the reference program's by a relative error of at most 0.0109076.
Values are sent between devices in bfloat16 or wider.
A program may use at most 1 GiB of HBM per device.

```python
import jax
import jax.numpy as jnp
from jax import lax

BATCH_SIZE = 8
SEQ_LEN = 1536
Q_BLOCK = 192
D_MODEL = 2048
NUM_HEADS = 16
KV_HEADS = 16
HEAD_DIM = 128
FF_DIM = 8192
N_LAYERS = 1

Q_WIDTH = NUM_HEADS * HEAD_DIM
KV_WIDTH = KV_HEADS * HEAD_DIM
GROUP_SIZE = NUM_HEADS // KV_HEADS
N_QBLOCKS = SEQ_LEN // Q_BLOCK
N_TOKENS = BATCH_SIZE * SEQ_LEN


def setup_inputs(seed: int = 0, part: int = 0) -> dict:
    part_keys = jax.random.split(jax.random.fold_in(jax.random.key(seed), part), 4)
    shared_keys = jax.random.split(jax.random.key(seed + 1), 9)
    qk_scale = (2.0 / D_MODEL) ** 0.5
    in_scale = D_MODEL ** -0.5

    def normal_bf16(rng_key, dims, scale_val):
        return (jax.random.normal(rng_key, dims, jnp.float32) * scale_val).astype(jnp.bfloat16)

    def gain_bf16(rng_key):
        return jax.random.uniform(rng_key, (N_LAYERS, D_MODEL), jnp.float32, 0.6, 1.4).astype(jnp.bfloat16)

    lengths = jax.random.randint(part_keys[1], (BATCH_SIZE,), SEQ_LEN // 2 + 1, SEQ_LEN + 1)
    full_row = jax.random.randint(part_keys[2], (), 0, BATCH_SIZE)
    lengths = jnp.where(jnp.arange(BATCH_SIZE) == full_row, SEQ_LEN, lengths).astype(jnp.int32)
    return {
        'prompt': normal_bf16(part_keys[0], (BATCH_SIZE, SEQ_LEN, D_MODEL), 1.0),
        'lengths': lengths,
        'new_tok': normal_bf16(part_keys[3], (BATCH_SIZE, D_MODEL), 1.0),
        'norm_attn': gain_bf16(shared_keys[0]),
        'w_q': normal_bf16(shared_keys[1], (N_LAYERS, D_MODEL, Q_WIDTH), qk_scale),
        'w_k': normal_bf16(shared_keys[2], (N_LAYERS, D_MODEL, KV_WIDTH), qk_scale),
        'w_v': normal_bf16(shared_keys[3], (N_LAYERS, D_MODEL, KV_WIDTH), in_scale),
        'w_o': normal_bf16(shared_keys[4], (N_LAYERS, Q_WIDTH, D_MODEL), Q_WIDTH ** -0.5),
        'norm_mlp': gain_bf16(shared_keys[5]),
        'w_gate': normal_bf16(shared_keys[6], (N_LAYERS, D_MODEL, FF_DIM), in_scale),
        'w_up': normal_bf16(shared_keys[7], (N_LAYERS, D_MODEL, FF_DIM), in_scale),
        'w_down': normal_bf16(shared_keys[8], (N_LAYERS, FF_DIM, D_MODEL), FF_DIM ** -0.5),
    }


def rms_norm(hidden, gain_vec):
    hid_f32 = hidden.astype(jnp.float32)
    inv_rms = lax.rsqrt(jnp.mean(hid_f32 * hid_f32, axis=-1, keepdims=True) + 1e-5)
    return (hid_f32 * inv_rms * gain_vec.astype(jnp.float32)).astype(jnp.bfloat16)


def rotary(heads_f32, positions):
    half_dim = HEAD_DIM // 2
    inv_freq = 10000.0 ** (-2.0 * jnp.arange(half_dim, dtype=jnp.float32) / HEAD_DIM)
    angles = positions.astype(jnp.float32)[..., None] * inv_freq
    cos_tab = jnp.cos(angles)[..., None, :]
    sin_tab = jnp.sin(angles)[..., None, :]
    lo_half = heads_f32[..., :half_dim]
    hi_half = heads_f32[..., half_dim:]
    return jnp.concatenate([lo_half * cos_tab - hi_half * sin_tab, hi_half * cos_tab + lo_half * sin_tab], axis=-1)


def prefill_attention(queries, key_rot, val_proj, lengths):
    q_blocks = jnp.moveaxis(queries.astype(jnp.float32).reshape(BATCH_SIZE, N_QBLOCKS, Q_BLOCK, KV_HEADS, GROUP_SIZE, HEAD_DIM), 1, 0)
    key_f32 = key_rot.astype(jnp.float32)
    val_f32 = val_proj.astype(jnp.float32)
    key_pos = jnp.arange(SEQ_LEN)
    key_valid = key_pos[None, :] < lengths[:, None]

    def one_block(block_args):
        q_blk, blk_idx = block_args
        q_pos = blk_idx * Q_BLOCK + jnp.arange(Q_BLOCK)
        scores = jnp.einsum('bqhgd,bkhd->bqhgk', q_blk, key_f32) * (HEAD_DIM ** -0.5)
        visible = (key_pos[None, None, :] <= q_pos[None, :, None]) & key_valid[:, None, :]
        scores = jnp.where(visible[:, :, None, None, :], scores, -1e30)
        attn_prob = jax.nn.softmax(scores, axis=-1)
        return jnp.einsum('bqhgk,bkhd->bqhgd', attn_prob, val_f32)

    blocks_out = lax.map(one_block, (q_blocks, jnp.arange(N_QBLOCKS)))
    return jnp.moveaxis(blocks_out, 0, 1).reshape(BATCH_SIZE, SEQ_LEN, Q_WIDTH).astype(jnp.bfloat16)


def decode_attention(q_new, key_cache, value_cache, lengths):
    q_f32 = q_new.astype(jnp.float32).reshape(BATCH_SIZE, KV_HEADS, GROUP_SIZE, HEAD_DIM)
    scores = jnp.einsum('bhgd,bkhd->bhgk', q_f32, key_cache.astype(jnp.float32)) * (HEAD_DIM ** -0.5)
    cache_pos = jnp.arange(SEQ_LEN + 1)
    visible = (cache_pos[None, :] < lengths[:, None]) | (cache_pos[None, :] == SEQ_LEN)
    scores = jnp.where(visible[:, None, None, :], scores, -1e30)
    attn_prob = jax.nn.softmax(scores, axis=-1)
    out_f32 = jnp.einsum('bhgk,bkhd->bhgd', attn_prob, value_cache.astype(jnp.float32))
    return out_f32.reshape(BATCH_SIZE, Q_WIDTH).astype(jnp.bfloat16)


def reference(prompt, lengths, new_tok, norm_attn, w_q, w_k, w_v, w_o, norm_mlp, w_gate, w_up, w_down):
    seq_pos = jnp.arange(SEQ_LEN)

    def layer_step(loop_state, layer_w):
        hidden, dec_hidden = loop_state
        g_attn, wq_l, wk_l, wv_l, wo_l, g_mlp, wg_l, wu_l, wd_l = layer_w
        normed = rms_norm(hidden, g_attn).reshape(N_TOKENS, D_MODEL)
        q_rot = rotary(jnp.dot(normed, wq_l, preferred_element_type=jnp.float32).reshape(BATCH_SIZE, SEQ_LEN, NUM_HEADS, HEAD_DIM), seq_pos).astype(jnp.bfloat16)
        k_rot = rotary(jnp.dot(normed, wk_l, preferred_element_type=jnp.float32).reshape(BATCH_SIZE, SEQ_LEN, KV_HEADS, HEAD_DIM), seq_pos).astype(jnp.bfloat16)
        v_proj = jnp.dot(normed, wv_l, preferred_element_type=jnp.float32).astype(jnp.bfloat16).reshape(BATCH_SIZE, SEQ_LEN, KV_HEADS, HEAD_DIM)
        attn_out = prefill_attention(q_rot, k_rot, v_proj, lengths).reshape(N_TOKENS, Q_WIDTH)
        hidden = (hidden.astype(jnp.float32) + jnp.dot(attn_out, wo_l, preferred_element_type=jnp.float32).reshape(BATCH_SIZE, SEQ_LEN, D_MODEL)).astype(jnp.bfloat16)
        normed = rms_norm(hidden, g_mlp).reshape(N_TOKENS, D_MODEL)
        mlp_mid = (jax.nn.silu(jnp.dot(normed, wg_l, preferred_element_type=jnp.float32)) * jnp.dot(normed, wu_l, preferred_element_type=jnp.float32)).astype(jnp.bfloat16)
        hidden = (hidden.astype(jnp.float32) + jnp.dot(mlp_mid, wd_l, preferred_element_type=jnp.float32).reshape(BATCH_SIZE, SEQ_LEN, D_MODEL)).astype(jnp.bfloat16)

        tok_norm = rms_norm(dec_hidden, g_attn)
        q_new = rotary(jnp.dot(tok_norm, wq_l, preferred_element_type=jnp.float32).reshape(BATCH_SIZE, NUM_HEADS, HEAD_DIM), lengths).astype(jnp.bfloat16)
        k_new = rotary(jnp.dot(tok_norm, wk_l, preferred_element_type=jnp.float32).reshape(BATCH_SIZE, KV_HEADS, HEAD_DIM), lengths).astype(jnp.bfloat16)
        v_new = jnp.dot(tok_norm, wv_l, preferred_element_type=jnp.float32).astype(jnp.bfloat16).reshape(BATCH_SIZE, KV_HEADS, HEAD_DIM)
        key_cache = jnp.concatenate([k_rot, k_new[:, None]], axis=1)
        value_cache = jnp.concatenate([v_proj, v_new[:, None]], axis=1)
        tok_attn = decode_attention(q_new, key_cache, value_cache, lengths)
        dec_hidden = (dec_hidden.astype(jnp.float32) + jnp.dot(tok_attn, wo_l, preferred_element_type=jnp.float32)).astype(jnp.bfloat16)
        tok_norm = rms_norm(dec_hidden, g_mlp)
        tok_mid = (jax.nn.silu(jnp.dot(tok_norm, wg_l, preferred_element_type=jnp.float32)) * jnp.dot(tok_norm, wu_l, preferred_element_type=jnp.float32)).astype(jnp.bfloat16)
        dec_hidden = (dec_hidden.astype(jnp.float32) + jnp.dot(tok_mid, wd_l, preferred_element_type=jnp.float32)).astype(jnp.bfloat16)
        return (hidden, dec_hidden), (key_cache, value_cache)

    (hidden, dec_hidden), (key_cache, value_cache) = lax.scan(layer_step, (prompt, new_tok), (norm_attn, w_q, w_k, w_v, w_o, norm_mlp, w_gate, w_up, w_down))
    last_sel = seq_pos[None, :] == (lengths - 1)[:, None]
    last_hidden = jnp.sum(jnp.where(last_sel[:, :, None], hidden.astype(jnp.float32), 0.0), axis=1).astype(jnp.bfloat16)
    return dec_hidden, last_hidden, key_cache, value_cache
```

```python
import jax
import jax.numpy as jnp
from jax import lax
from jax.experimental import pallas as pl
from jax.experimental.pallas import tpu as pltpu
from jax.sharding import PartitionSpec as P

HEAD_DIM = 128
NEG_BIG = -1e30
BATCH = 8
SEQ_LOC = 192
D_MODEL = 2048
SHARD = 256
ROWS = 2 * SEQ_LOC
MESH = pl.DeviceIdType.MESH


def rms_norm(hidden, gain_vec):
    hid_f32 = hidden.astype(jnp.float32)
    inv_rms = lax.rsqrt(jnp.mean(hid_f32 * hid_f32, axis=-1, keepdims=True) + 1e-5)
    return (hid_f32 * inv_rms * gain_vec.astype(jnp.float32)).astype(jnp.bfloat16)


def rope_tables(positions):
    half_dim = HEAD_DIM // 2
    inv_freq = 10000.0 ** (-2.0 * jnp.arange(half_dim, dtype=jnp.float32) / HEAD_DIM)
    angles = positions.astype(jnp.float32)[..., None] * inv_freq
    cos_tab, sin_tab = jnp.cos(angles), jnp.sin(angles)
    return jnp.concatenate([cos_tab, cos_tab], -1), jnp.concatenate([-sin_tab, sin_tab], -1)


def rotary(heads_f32, positions):
    cos_tab, sin_tab = rope_tables(positions)
    half_dim = HEAD_DIM // 2
    swapped = jnp.concatenate([heads_f32[..., half_dim:], heads_f32[..., :half_dim]], axis=-1)
    return heads_f32 * cos_tab[..., None, :] + swapped * sin_tab[..., None, :]


def kv_kernel(prompt, gain, tabc, tabs, wk, wv, kv_out, xbuf, xrecv, wbuf, tmp, stage,
              lsem, xsem, ysend, yrecv, wsend, wrecv, osend, orecv, ssem):
    rep = lax.axis_index('replica')
    me = lax.axis_index('model')
    core = lax.rem(me, 2)
    xpos = lax.rem(me // 2, 2)
    ypos = me // 4
    sib = me + 1 - 2 * core
    xnb = me + 2 - 4 * xpos
    xsb = xnb + 1 - 2 * core
    ynb = me + 4 - 8 * ypos
    znb = 1 - rep

    barrier = pltpu.get_barrier_semaphore()
    for peer in ((rep, sib), (rep, xnb), (rep, xsb), (rep, ynb), (znb, me)):
        pl.semaphore_signal(barrier, inc=1, device_id=peer, device_id_type=MESH)
    pl.semaphore_wait(barrier, 5)

    def remote(src, dst, send, recv, peer):
        return pltpu.make_async_remote_copy(src_ref=src, dst_ref=dst, send_sem=send, recv_sem=recv, device_id=peer, device_id_type=MESH)

    def y_copy(b):
        return remote(prompt.at[b], xrecv.at[b], ysend.at[b], yrecv.at[b], (rep, ynb))

    def x_load(b):
        return pltpu.make_async_copy(prompt.at[b], xbuf.at[b], xsem.at[b])

    wk_load = pltpu.make_async_copy(wk, wbuf.at[0, 0], lsem.at[0])
    wv_load = pltpu.make_async_copy(wv, wbuf.at[0, 1], lsem.at[1])
    wk_load.start()
    wv_load.start()

    @pl.loop(0, BATCH)
    def _(b):
        y_copy(b).start()
        x_load(b).start()

    wk_load.wait()
    wv_load.wait()
    w_x = remote(wbuf.at[0, rep], wbuf.at[2, rep], wsend.at[0], wrecv.at[0], (rep, xnb))
    w_s = remote(wbuf.at[0], wbuf.at[1], wsend.at[1], wrecv.at[1], (rep, sib))
    w_z = remote(wbuf.at[2, rep], wbuf.at[2, rep], wsend.at[2], wrecv.at[2], (znb, me))
    w_xs = remote(wbuf.at[2, rep], wbuf.at[3, rep], wsend.at[3], wrecv.at[3], (rep, sib))
    w_zs = remote(wbuf.at[2, znb], wbuf.at[3, znb], wsend.at[4], wrecv.at[4], (rep, sib))
    w_x.start()
    w_s.start()

    def out_copy(s, b, o, kv):
        blk = me if s == 0 else ynb
        dst = kv_out.at[kv, b, pl.ds(pl.multiple_of(blk * ROWS, ROWS), ROWS), :]
        src = stage.at[s, b, o, kv]
        if o == 0:
            return pltpu.make_async_copy(src, dst, ssem.at[s, b, kv])
        peer = (sib, xnb, xsb)[o - 1]
        return remote(src, dst, osend.at[o - 1, s, b, kv], orecv.at[o - 1, s, b, kv], (rep, peer))

    def normalize(buf, b):
        x = buf[b].astype(jnp.float32)
        inv = lax.rsqrt(jnp.mean(x * x, axis=-1, keepdims=True) + 1e-5)
        buf[b] = (x * inv * gain[...].astype(jnp.float32)).astype(jnp.bfloat16)

    def project(buf, s, b, o, kv):
        acc = jnp.dot(buf[b], wbuf[o, kv], preferred_element_type=jnp.float32)
        c, sn = tabc[kv, s], tabs[kv, s]
        for h in range(2):
            a = acc[:, h * HEAD_DIM:(h + 1) * HEAD_DIM]
            tmp[pl.ds(h, SEQ_LOC, stride=2), :] = a * c + pltpu.roll(a, HEAD_DIM // 2, 1) * sn
        stage[s, b, o, kv] = tmp[...].astype(jnp.bfloat16)

    @pl.loop(0, BATCH)
    def _(b):
        x_load(b).wait()
        normalize(xbuf, b)

        @pl.loop(0, 2)
        def _(kv):
            project(xbuf, 0, b, 0, kv)
            out_copy(0, b, 0, kv).start()

    w_s.wait_recv()

    @pl.loop(0, BATCH)
    def _(b):
        @pl.loop(0, 2)
        def _(kv):
            project(xbuf, 0, b, 1, kv)
            out_copy(0, b, 1, kv).start()

    w_x.wait_recv()
    w_z.start()
    w_xs.start()
    w_xs.wait_recv()

    def own_x_phase(kv):
        @pl.loop(0, BATCH)
        def _(b):
            for o in (2, 3):
                project(xbuf, 0, b, o, kv)
            for o in (2, 3):
                out_copy(0, b, o, kv).start()

    own_x_phase(rep)
    w_z.wait_recv()
    w_zs.start()
    w_zs.wait_recv()
    own_x_phase(znb)

    @pl.loop(0, BATCH)
    def _(b):
        y_copy(b).wait_recv()
        normalize(xrecv, b)

        @pl.loop(0, 2)
        def _(kv):
            for o in (2, 3, 1, 0):
                project(xrecv, 1, b, o, kv)
                out_copy(1, b, o, kv).start()

    for w in (w_x, w_s, w_z, w_xs, w_zs):
        w.wait_send()

    @pl.loop(0, BATCH)
    def _(b):
        y_copy(b).wait_send()
        for s in range(2):
            for kv in range(2):
                out_copy(s, b, 0, kv).wait()
                for o in (1, 2, 3):
                    out_copy(s, b, o, kv).wait()


def prompt_kv(prompt, gain, tabc, tabs, wk, wv):
    vmem = pl.BlockSpec(memory_space=pltpu.VMEM)
    anym = pl.BlockSpec(memory_space=pl.ANY)
    dma = pltpu.SemaphoreType.DMA
    bf = jnp.bfloat16
    return pl.pallas_call(
        kv_kernel,
        out_shape=jax.ShapeDtypeStruct((2, BATCH, 8 * ROWS, HEAD_DIM), bf),
        in_specs=[anym, vmem, vmem, vmem, anym, anym],
        out_specs=anym,
        scratch_shapes=[
            pltpu.VMEM((BATCH, SEQ_LOC, D_MODEL), bf),
            pltpu.VMEM((BATCH, SEQ_LOC, D_MODEL), bf),
            pltpu.VMEM((4, 2, D_MODEL, SHARD), bf),
            pltpu.VMEM((ROWS, HEAD_DIM), jnp.float32),
            pltpu.VMEM((2, BATCH, 4, 2, ROWS, HEAD_DIM), bf),
            dma((2,)), dma((BATCH,)), dma((BATCH,)), dma((BATCH,)), dma((5,)), dma((5,)),
            dma((3, 2, BATCH, 2)), dma((3, 2, BATCH, 2)), dma((2, BATCH, 2)),
        ],
        compiler_params=pltpu.CompilerParams(collective_id=0, has_side_effects=True, vmem_limit_bytes=56 * 1024 * 1024),
        cost_estimate=pl.CostEstimate(flops=26_000_000_000, bytes_accessed=40_000_000, transcendentals=0),
        name='prompt_kv',
    )(prompt, gain, tabc, tabs, wk, wv)


def solution(mesh):
    seq_spec = P('replica', 'model', None)
    col_spec = P(None, None, 'model')
    row_spec = P(None, 'model', None)
    gain_spec = P(None, None)
    tok_spec = P('replica', None)
    cache_spec = P(None, 'replica', None, 'model', None)
    in_specs = (seq_spec, P('replica'), tok_spec, gain_spec, col_spec, col_spec, col_spec, row_spec, gain_spec, col_spec, col_spec, row_spec)
    out_specs = (tok_spec, tok_spec, cache_spec, cache_spec)

    def per_device(prompt, lengths, new_tok, norm_attn, w_q, w_k, w_v, w_o, norm_mlp, w_gate, w_up, w_down):
        f32, bf = jnp.float32, jnp.bfloat16
        me = lax.axis_index('model')
        n_batch, seq_loc, d_model = prompt.shape
        seq_len = seq_loc * mesh.shape['model']
        pos = jnp.stack([me * seq_loc, lax.rem(me + 4, 8) * seq_loc])[:, None] + jnp.arange(seq_loc)[None, :]
        cos_k, sin_k = rope_tables(pos)
        tabc = jnp.stack([cos_k, jnp.ones_like(cos_k)])
        tabs = jnp.stack([sin_k, jnp.zeros_like(sin_k)])
        kv = prompt_kv(prompt, norm_attn, tabc, tabs, w_k[0], w_v[0]).reshape(2, n_batch, seq_len, 2, HEAD_DIM)

        seq_pos = me * seq_loc + jnp.arange(seq_loc)
        last_sel = (seq_pos[None, :] == (lengths - 1)[:, None]).astype(bf)
        last_part = jnp.einsum('bs,bsd->bd', last_sel, prompt, preferred_element_type=f32)
        last_row = lax.psum(last_part, 'model').astype(bf)
        rows = jnp.concatenate([new_tok, last_row], axis=0)
        row_pos = jnp.concatenate([lengths, lengths - 1])
        normed = rms_norm(rows, norm_attn[0])
        q = rotary(jnp.dot(normed, w_q[0], preferred_element_type=f32).reshape(2 * n_batch, 2, HEAD_DIM), row_pos).astype(bf)
        k_new = rotary(jnp.dot(normed[:n_batch], w_k[0], preferred_element_type=f32).reshape(n_batch, 2, HEAD_DIM), lengths).astype(bf)
        v_new = jnp.dot(normed[:n_batch], w_v[0], preferred_element_type=f32).astype(bf).reshape(n_batch, 2, HEAD_DIM)

        q2 = jnp.moveaxis(q.reshape(2, n_batch, 2, HEAD_DIM), 0, 1)
        scores = jnp.einsum('bghd,bkhd->bghk', q2, kv[0], preferred_element_type=f32) * (HEAD_DIM ** -0.5)
        visible = jnp.arange(seq_len)[None, :] < lengths[:, None]
        scores = jnp.where(visible[:, None, None, :], scores, NEG_BIG)
        self_score = jnp.sum(q2[:, 0].astype(f32) * k_new.astype(f32), axis=-1) * (HEAD_DIM ** -0.5)
        self_score = jnp.stack([self_score, jnp.full_like(self_score, NEG_BIG)], axis=1)
        top = jnp.maximum(jnp.max(scores, axis=-1), self_score)
        prob = jnp.exp(scores - top[..., None])
        self_prob = jnp.exp(self_score - top)
        acc = jnp.einsum('bghk,bkhd->bghd', prob.astype(bf), kv[1], preferred_element_type=f32)
        acc = acc + self_prob[..., None] * v_new.astype(f32)[:, None]
        attn = (acc / (jnp.sum(prob, axis=-1) + self_prob)[..., None]).astype(bf)
        attn = jnp.moveaxis(attn, 1, 0).reshape(2 * n_batch, 2 * HEAD_DIM)
        attn_part = jnp.dot(attn, w_o[0], preferred_element_type=f32)
        hid = (rows.astype(f32) + lax.psum(attn_part, 'model')).astype(bf)
        normed = rms_norm(hid, norm_mlp[0])
        mid = (jax.nn.silu(jnp.dot(normed, w_gate[0], preferred_element_type=f32)) * jnp.dot(normed, w_up[0], preferred_element_type=f32)).astype(bf)
        mlp_part = jnp.dot(mid, w_down[0], preferred_element_type=f32)
        hid = (hid.astype(f32) + lax.psum(mlp_part, 'model')).astype(bf)

        key_cache = jnp.concatenate([kv[0], k_new[:, None]], axis=1)[None]
        val_cache = jnp.concatenate([kv[1], v_new[:, None]], axis=1)[None]
        return hid[:n_batch], hid[n_batch:], key_cache, val_cache

    return jax.shard_map(per_device, mesh=mesh, in_specs=in_specs, out_specs=out_specs, check_vma=False)
```

```python
import jax
import jax.numpy as jnp
import numpy as np
from jax import lax
from jax.experimental import pallas as pl
from jax.experimental.pallas import tpu as pltpu
from jax.sharding import PartitionSpec as P

HEAD_DIM = 128
HALF = HEAD_DIM // 2
NEG_BIG = -1e30
BATCH = 8
SEQ_LOC = 192
SEQ_LEN = 1536
D_MODEL = 2048
SHARD = 256
FF_LOC = 1024
ROWS = 2 * SEQ_LOC
TAB_ROWS = SEQ_LEN + 8
MESH = pl.DeviceIdType.MESH
BF = jnp.bfloat16
F32 = jnp.float32
SCALE = HEAD_DIM ** -0.5


def rope_table():
    inv_freq = np.float32(10000.0) ** (np.float32(-2.0) * np.arange(HALF, dtype=np.float32) / np.float32(HEAD_DIM))
    angles = np.arange(TAB_ROWS, dtype=np.float32)[:, None] * inv_freq.astype(np.float32)
    return np.concatenate([np.cos(angles), np.sin(angles)], axis=-1).astype(np.float32)


def norm_rows(x, gain):
    inv = lax.rsqrt(jnp.mean(x * x, axis=-1, keepdims=True) + 1e-5)
    return (x * inv * gain.astype(F32)).astype(BF)


def spread(tab):
    swapped = pltpu.roll(tab, HALF, 1)
    low = lax.broadcasted_iota(jnp.int32, tab.shape, 1) < HALF
    return jnp.where(low, tab, swapped), jnp.where(low, -swapped, tab)


def rotate(a, c, s):
    return a * c + pltpu.roll(a, HALF, 1) * s


def layer_kernel(lens, prompt, new_tok, gain_a, gain_m, table, wq, wk, wv, wo, wg, wu, wd,
                 kv_out, new_out, dec_out, last_out,
                 xbuf, xrecv, wbuf, wqb, wob, wgb, wub, wdb, tab, tmp, stage,
                 lastf, lsend, lrecv, rows, qall, part, precv, kself, vself, attn, flat,
                 psend, rrecv, hid, norm2,
                 lsem, xsem, ysend, yrecv, wsend, wrecv, osend, orecv, ssem,
                 l_s, l_r, q_s, q_r, p_s, p_r, r_s, r_r, a_s, a_r):
    rep = lax.axis_index('replica')
    me = lax.axis_index('model')
    core = lax.rem(me, 2)
    xpos = lax.rem(me // 2, 2)
    ypos = me // 4
    flips = (1 - 2 * core, 2 - 4 * xpos, 4 - 8 * ypos)
    near = [me + sum(f for i, f in enumerate(flips) if d >> i & 1) for d in range(8)]
    sib, xnb, xsb, ynb = near[1], near[2], near[3], near[4]
    znb = 1 - rep

    barrier = pltpu.get_barrier_semaphore()
    for peer in [(rep, near[d]) for d in range(1, 8)] + [(znb, me)]:
        pl.semaphore_signal(barrier, inc=1, device_id=peer, device_id_type=MESH)
    pl.semaphore_wait(barrier, 8)

    def remote(src, dst, send, recv, peer):
        return pltpu.make_async_remote_copy(src_ref=src, dst_ref=dst, send_sem=send, recv_sem=recv, device_id=peer, device_id_type=MESH)

    def y_copy(b):
        return remote(prompt.at[b], xrecv.at[b], ysend.at[b], yrecv.at[b], (rep, ynb))

    def x_load(b):
        return pltpu.make_async_copy(prompt.at[b], xbuf.at[b], xsem.at[b])

    loads = [pltpu.make_async_copy(a, b, lsem.at[i]) for i, (a, b) in enumerate((
        (wk.at[0], wbuf.at[0, 0]), (wv.at[0], wbuf.at[0, 1]), (table, tab), (wq.at[0], wqb), (wo.at[0], wob),
        (wg.at[0], wgb), (wu.at[0], wub), (wd.at[0], wdb)))]
    loads[0].start()
    loads[1].start()
    y_copy(0).start()

    @pl.loop(0, BATCH)
    def _(b):
        x_load(b).start()

    for load in loads[2:]:
        load.start()
    loads[0].wait()
    loads[1].wait()
    w_x = remote(wbuf.at[0, rep], wbuf.at[2, rep], wsend.at[0], wrecv.at[0], (rep, xnb))
    w_s = remote(wbuf.at[0], wbuf.at[1], wsend.at[1], wrecv.at[1], (rep, sib))
    w_z = remote(wbuf.at[2, rep], wbuf.at[2, rep], wsend.at[2], wrecv.at[2], (znb, me))
    w_xs = remote(wbuf.at[2, rep], wbuf.at[3, rep], wsend.at[3], wrecv.at[3], (rep, sib))
    w_zs = remote(wbuf.at[2, znb], wbuf.at[3, znb], wsend.at[4], wrecv.at[4], (rep, sib))
    w_x.start()
    w_s.start()

    def out_copy(s, b, o, kv):
        blk = me if s == 0 else ynb
        dst = kv_out.at[kv, b, pl.ds(pl.multiple_of(blk * ROWS, ROWS), ROWS), :]
        src = stage.at[s, b, o, kv]
        if o == 0:
            return pltpu.make_async_copy(src, dst, ssem.at[s, b, kv])
        return remote(src, dst, osend.at[o - 1, s, b, kv], orecv.at[o - 1, s, b, kv], (rep, near[o]))

    def project(buf, s, b, o, kv):
        acc = jnp.dot(buf[b], wbuf[o, kv], preferred_element_type=F32)
        blk = me if s == 0 else ynb
        c, sn = spread(tab[pl.ds(pl.multiple_of(blk * SEQ_LOC, SEQ_LOC), SEQ_LOC), :])
        is_k = kv == 0
        c = jnp.where(is_k, c, 1.0)
        sn = jnp.where(is_k, sn, 0.0)
        for h in range(2):
            tmp[pl.ds(h, SEQ_LOC, stride=2), :] = rotate(acc[:, h * HEAD_DIM:(h + 1) * HEAD_DIM], c, sn)
        stage[s, b, o, kv] = tmp[...].astype(BF)

    @pl.loop(0, BATCH)
    def _(b):
        x_load(b).wait()
        x = xbuf[b].astype(F32)
        here = me * SEQ_LOC + lax.broadcasted_iota(jnp.int32, (SEQ_LOC, 1), 0) == lens[b] - 1
        lastf[pl.ds(b, 1), :] = jnp.sum(jnp.where(here, x, 0.0), axis=0, keepdims=True)
        xbuf[b] = norm_rows(x, gain_a[...])

    l_copy = [remote(lsend.at[i], lrecv.at[i], l_s.at[i], l_r.at[i], (rep, near[d])) for i, d in enumerate((4, 1, 2))]
    lsend[0] = lastf[...].astype(BF)
    loads[2].wait()
    l_copy[0].start()

    @pl.loop(1, BATCH)
    def _(b):
        y_copy(b).start()

    @pl.loop(0, BATCH)
    def _(b):
        @pl.loop(0, 2)
        def _(kv):
            project(xbuf, 0, b, 0, kv)
            out_copy(0, b, 0, kv).start()

    def join_last(i):
        l_copy[i].wait_recv()
        return (lsend[i].astype(F32) + lrecv[i].astype(F32)).astype(BF)

    lsend[1] = join_last(0)
    w_s.wait_recv()
    l_copy[1].start()

    @pl.loop(0, BATCH)
    def _(b):
        @pl.loop(0, 2)
        def _(kv):
            project(xbuf, 0, b, 1, kv)
            out_copy(0, b, 1, kv).start()

    lsend[2] = join_last(1)

    w_x.wait_recv()
    w_z.start()
    w_xs.start()
    l_copy[2].start()
    w_xs.wait_recv()

    def own_x_phase(kv):
        @pl.loop(0, BATCH)
        def _(b):
            for o in (2, 3):
                project(xbuf, 0, b, o, kv)
            for o in (2, 3):
                out_copy(0, b, o, kv).start()

    own_x_phase(rep)

    rows[0:BATCH, :] = new_tok[...].astype(F32)
    rows[BATCH:2 * BATCH, :] = join_last(2).astype(F32)
    loads[3].wait()
    n16 = norm_rows(rows[...], gain_a[...])
    q16 = jnp.dot(n16, wqb[...], preferred_element_type=F32)
    k16 = jnp.dot(n16, wbuf[0, 0], preferred_element_type=F32)
    v16 = jnp.dot(n16, wbuf[0, 1], preferred_element_type=F32)
    for b in range(BATCH):
        flat[pl.ds(b, 1), 0:HEAD_DIM] = tab[pl.ds(jnp.clip(lens[b], 0, SEQ_LEN), 1), :]
        flat[pl.ds(BATCH + b, 1), 0:HEAD_DIM] = tab[pl.ds(jnp.clip(lens[b] - 1, 0, SEQ_LEN), 1), :]
    c16, s16 = spread(flat[:, 0:HEAD_DIM])
    kself[...] = jnp.zeros_like(kself)
    vself[...] = jnp.zeros_like(vself)
    for h in range(2):
        lanes = slice(h * HEAD_DIM, (h + 1) * HEAD_DIM)
        qh = rotate(q16[:, lanes], c16, s16).astype(BF).astype(F32)
        kh = rotate(k16[:, lanes], c16, s16)[:BATCH].astype(BF).astype(F32)
        vh = v16[:BATCH, lanes].astype(BF).astype(F32)
        for g in range(2):
            qall[0, :, 2 * g + h, :] = qh[g * BATCH:(g + 1) * BATCH]
        kself[:, h, :] = kh
        vself[:, h, :] = vh
        tmp[pl.ds(h, BATCH, stride=2), :] = kh
        tmp[pl.ds(2 * BATCH + h, BATCH, stride=2), :] = vh
    new_out[0] = tmp[0:2 * BATCH, :].astype(BF)
    new_out[1] = tmp[2 * BATCH:4 * BATCH, :].astype(BF)
    low = lax.broadcasted_iota(jnp.int32, (4, HEAD_DIM), 1) < HALF
    part[:, 0] = jnp.zeros((4, BATCH, 4, HEAD_DIM), F32)
    part[:, 1] = jnp.broadcast_to(jnp.where(low, NEG_BIG, 0.0), (4, BATCH, 4, HEAD_DIM))
    q_copy = [remote(qall.at[0], qall.at[d], q_s.at[d - 1], q_r.at[d - 1], (rep, near[d])) for d in (1, 2, 3)]
    for c in q_copy:
        c.start()

    w_z.wait_recv()
    w_zs.start()
    w_zs.wait_recv()
    own_x_phase(znb)
    for c in q_copy:
        c.wait_recv()

    lane = lax.broadcasted_iota(jnp.int32, (4, ROWS), 1)
    same_head = lane % 2 == lax.broadcasted_iota(jnp.int32, (4, ROWS), 0) % 2

    def attend(s, b):
        blk = me if s == 0 else ynb
        seen = same_head & (blk * SEQ_LOC + lane // 2 < lens[b])
        for o in range(4):
            sc = lax.dot_general(qall[o, b].astype(BF), stage[s, b, o, 0], (((1,), (1,)), ((), ())), preferred_element_type=F32) * SCALE
            sc = jnp.where(seen, sc, NEG_BIG)
            old = part[o, 1, b]
            m_old, l_old = old[:, 0:1], old[:, HALF:HALF + 1]
            m_new = jnp.maximum(m_old, jnp.max(sc, axis=-1, keepdims=True))
            p = jnp.where(seen, jnp.exp(sc - m_new), 0.0)
            fade = jnp.exp(m_old - m_new)
            l_new = l_old * fade + jnp.sum(p, axis=-1, keepdims=True)
            part[o, 0, b] = part[o, 0, b] * fade + jnp.dot(p.astype(BF), stage[s, b, o, 1], preferred_element_type=F32)
            part[o, 1, b] = jnp.where(low, m_new, l_new)

    @pl.loop(0, BATCH)
    def _(b):
        attend(0, b)
        y_copy(b).wait_recv()
        xrecv[b] = norm_rows(xrecv[b].astype(F32), gain_a[...])

        @pl.loop(0, 2)
        def _(kv):
            for o in (2, 3, 1, 0):
                project(xrecv, 1, b, o, kv)
                out_copy(1, b, o, kv).start()

        attend(1, b)

    p_copy = [remote(part.at[d], precv.at[d - 1], p_s.at[d - 1], p_r.at[d - 1], (rep, near[d])) for d in (1, 2, 3)]
    for c in p_copy:
        c.start()
    for load in loads[4:]:
        load.wait()
    first = lax.broadcasted_iota(jnp.int32, (BATCH, 4, 1), 1) < 2
    s_self = jnp.where(first, jnp.sum(qall[0] * kself[...], axis=-1, keepdims=True) * SCALE, NEG_BIG)
    for c in p_copy:
        c.wait_recv()
    accs = [part[0, 0]] + [precv[i, 0] for i in range(3)]
    stats = [part[0, 1]] + [precv[i, 1] for i in range(3)]
    tops = [st[:, :, 0:1] for st in stats]
    top = s_self
    for t in tops:
        top = jnp.maximum(top, t)
    e_self = jnp.where(first, jnp.exp(s_self - top), 0.0)
    den = e_self
    num = e_self * vself[...]
    for t, st, ac in zip(tops, stats, accs):
        e = jnp.exp(t - top)
        den = den + e * st[:, :, HALF:HALF + 1]
        num = num + e * ac
    attn[...] = num / den
    for g in range(2):
        for h in range(2):
            flat[g * BATCH:(g + 1) * BATCH, h * HEAD_DIM:(h + 1) * HEAD_DIM] = attn[:, 2 * g + h, :]

    def reduce_columns(i, base):
        sends = [remote(psend.at[i, near[d]], rrecv.at[i, d - 1], r_s.at[i, d - 1], r_r.at[i, d - 1], (rep, near[d])) for d in range(1, 8)]
        for c in sends:
            c.start()
        total = psend[i, me]
        for d in range(1, 8):
            sends[d - 1].wait_recv()
            total = total + rrecv[i, d - 1]
        hid[i, me] = (base + total).astype(BF)
        gets = [remote(hid.at[i, me], hid.at[i, me], a_s.at[i, d - 1], a_r.at[i, d - 1], (rep, near[d])) for d in range(1, 8)]
        for c in gets:
            c.start()
        for d in range(1, 8):
            remote(hid.at[i, near[d]], hid.at[i, near[d]], a_s.at[i, d - 1], a_r.at[i, d - 1], (rep, near[d])).wait_recv()
        return sends + gets

    a16 = flat[...].astype(BF)
    for j in range(8):
        psend[0, j] = jnp.dot(a16, wob[:, j * SHARD:(j + 1) * SHARD], preferred_element_type=F32)
    mine = pl.ds(pl.multiple_of(me * SHARD, SHARD), SHARD)
    done = reduce_columns(0, rows[:, mine])

    sq = jnp.zeros((2 * BATCH, 1), F32)
    for j in range(8):
        hj = hid[0, j].astype(F32)
        sq = sq + jnp.sum(hj * hj, axis=-1, keepdims=True)
    inv = lax.rsqrt(sq / D_MODEL + 1e-5)
    for j in range(8):
        cols = slice(j * SHARD, (j + 1) * SHARD)
        norm2[:, cols] = (hid[0, j].astype(F32) * inv * gain_m[:, cols].astype(F32)).astype(BF)
    n2 = norm2[...]
    gate = jnp.dot(n2, wgb[...], preferred_element_type=F32)
    up = jnp.dot(n2, wub[...], preferred_element_type=F32)
    mid = (gate * jax.nn.sigmoid(gate) * up).astype(BF)
    for j in range(8):
        psend[1, j] = jnp.dot(mid, wdb[:, j * SHARD:(j + 1) * SHARD], preferred_element_type=F32)
    done += reduce_columns(1, hid[0, me].astype(F32))
    for j in range(8):
        cols = slice(j * SHARD, (j + 1) * SHARD)
        dec_out[:, cols] = hid[1, j][:BATCH]
        last_out[:, cols] = hid[1, j][BATCH:]

    for c in [w_x, w_s, w_z, w_xs, w_zs] + l_copy + q_copy + p_copy + done:
        c.wait_send()

    @pl.loop(0, BATCH)
    def _(b):
        y_copy(b).wait_send()
        for s in range(2):
            for kv in range(2):
                for o in range(4):
                    out_copy(s, b, o, kv).wait()


def layer(lens, prompt, new_tok, gain_a, gain_m, table, wq, wk, wv, wo, wg, wu, wd):
    vmem = pl.BlockSpec(memory_space=pltpu.VMEM)
    anym = pl.BlockSpec(memory_space=pl.ANY)
    dma = pltpu.SemaphoreType.DMA
    v = pltpu.VMEM
    return pl.pallas_call(
        layer_kernel,
        out_shape=(
            jax.ShapeDtypeStruct((2, BATCH, 8 * ROWS, HEAD_DIM), BF),
            jax.ShapeDtypeStruct((2, 2 * BATCH, HEAD_DIM), BF),
            jax.ShapeDtypeStruct((BATCH, D_MODEL), BF),
            jax.ShapeDtypeStruct((BATCH, D_MODEL), BF),
        ),
        in_specs=[pl.BlockSpec(memory_space=pltpu.SMEM), anym, vmem, vmem, vmem] + [anym] * 8,
        out_specs=(anym, vmem, vmem, vmem),
        scratch_shapes=[
            v((BATCH, SEQ_LOC, D_MODEL), BF), v((BATCH, SEQ_LOC, D_MODEL), BF), v((4, 2, D_MODEL, SHARD), BF),
            v((D_MODEL, SHARD), BF), v((SHARD, D_MODEL), BF), v((D_MODEL, FF_LOC), BF), v((D_MODEL, FF_LOC), BF), v((FF_LOC, D_MODEL), BF),
            v((TAB_ROWS, HEAD_DIM), F32), v((ROWS, HEAD_DIM), F32), v((2, BATCH, 4, 2, ROWS, HEAD_DIM), BF),
            v((BATCH, D_MODEL), F32), v((3, BATCH, D_MODEL), BF), v((3, BATCH, D_MODEL), BF), v((2 * BATCH, D_MODEL), F32),
            v((4, BATCH, 4, HEAD_DIM), F32), v((4, 2, BATCH, 4, HEAD_DIM), F32), v((3, 2, BATCH, 4, HEAD_DIM), F32),
            v((BATCH, 4, HEAD_DIM), F32), v((BATCH, 4, HEAD_DIM), F32), v((BATCH, 4, HEAD_DIM), F32), v((2 * BATCH, SHARD), F32),
            v((2, 8, 2 * BATCH, SHARD), F32), v((2, 7, 2 * BATCH, SHARD), F32), v((2, 8, 2 * BATCH, SHARD), BF), v((2 * BATCH, D_MODEL), BF),
            dma((8,)), dma((BATCH,)), dma((BATCH,)), dma((BATCH,)), dma((5,)), dma((5,)),
            dma((3, 2, BATCH, 2)), dma((3, 2, BATCH, 2)), dma((2, BATCH, 2)),
            dma((3,)), dma((3,)), dma((3,)), dma((3,)), dma((3,)), dma((3,)),
            dma((2, 7)), dma((2, 7)), dma((2, 7)), dma((2, 7)),
        ],
        compiler_params=pltpu.CompilerParams(collective_id=0, has_side_effects=True, vmem_limit_bytes=62 * 1024 * 1024),
        cost_estimate=pl.CostEstimate(flops=26_000_000_000, bytes_accessed=60_000_000, transcendentals=0),
        name='layer',
    )(lens, prompt, new_tok, gain_a, gain_m, table, wq, wk, wv, wo, wg, wu, wd)


def cache_kernel(kv, new, key_out, val_out, buf, row, load, store, row_sem):
    outs = (key_out, val_out)
    ins = [[pltpu.make_async_copy(kv.at[i, b], buf.at[i, b], load.at[i, b]) for b in range(BATCH)] for i in range(2)]
    rows_in = pltpu.make_async_copy(new, row, row_sem.at[0])
    rows_in.start()
    for i in range(2):
        for b in range(BATCH):
            ins[i][b].start()
    rows_in.wait()
    puts = [pltpu.make_async_copy(row.at[i], outs[i].at[0, :, pl.ds(SEQ_LEN, 1)], row_sem.at[1 + i]) for i in range(2)]
    for c in puts:
        c.start()
    for i in range(2):
        for b in range(BATCH):
            ins[i][b].wait()
            puts.append(pltpu.make_async_copy(buf.at[i, b], outs[i].at[0, b, pl.ds(0, SEQ_LEN)], store.at[i, b]))
            puts[-1].start()
    for c in puts:
        c.wait()


def caches(kv, new):
    anym = pl.BlockSpec(memory_space=pl.ANY)
    dma = pltpu.SemaphoreType.DMA
    shape = jax.ShapeDtypeStruct((1, BATCH, SEQ_LEN + 1, 2, HEAD_DIM), BF)
    return pl.pallas_call(
        cache_kernel,
        out_shape=(shape, shape),
        in_specs=[anym, anym],
        out_specs=(anym, anym),
        scratch_shapes=[
            pltpu.VMEM((2, BATCH, SEQ_LEN, 2, HEAD_DIM), BF), pltpu.VMEM((2, BATCH, 1, 2, HEAD_DIM), BF),
            dma((2, BATCH)), dma((2, BATCH)), dma((3,)),
        ],
        compiler_params=pltpu.CompilerParams(vmem_limit_bytes=62 * 1024 * 1024),
        cost_estimate=pl.CostEstimate(flops=0, bytes_accessed=50_000_000, transcendentals=0),
        name='caches',
    )(kv, new)


def solution(mesh):
    seq_spec = P('replica', 'model', None)
    col_spec = P(None, None, 'model')
    row_spec = P(None, 'model', None)
    gain_spec = P(None, None)
    tok_spec = P('replica', None)
    cache_spec = P(None, 'replica', None, 'model', None)
    in_specs = (seq_spec, P('replica'), tok_spec, gain_spec, col_spec, col_spec, col_spec, row_spec, gain_spec, col_spec, col_spec, row_spec)
    out_specs = (tok_spec, tok_spec, cache_spec, cache_spec)
    table = rope_table()

    def per_device(prompt, lengths, new_tok, norm_attn, w_q, w_k, w_v, w_o, norm_mlp, w_gate, w_up, w_down):
        kv, new, dec, last = layer(lengths, prompt, new_tok, norm_attn, norm_mlp, jnp.asarray(table), w_q, w_k, w_v, w_o, w_gate, w_up, w_down)
        keys, vals = caches(kv.reshape(2, BATCH, SEQ_LEN, 2, HEAD_DIM), new.reshape(2, BATCH, 1, 2, HEAD_DIM))
        return dec, last, keys, vals

    return jax.shard_map(per_device, mesh=mesh, in_specs=in_specs, out_specs=out_specs, check_vma=False)
```

```python
import jax
import jax.numpy as jnp
import numpy as np
from jax import lax
from jax.experimental import pallas as pl
from jax.experimental.pallas import tpu as pltpu
from jax.sharding import PartitionSpec as P

HEAD_DIM = 128
HALF = HEAD_DIM // 2
NEG_BIG = -1e30
BATCH = 8
SEQ_LOC = 192
SEQ_LEN = 1536
D_MODEL = 2048
SHARD = 256
FF_LOC = 1024
ROWS = 2 * SEQ_LOC
TAB_ROWS = SEQ_LEN + 8
MESH = pl.DeviceIdType.MESH
BF = jnp.bfloat16
F32 = jnp.float32
SCALE = HEAD_DIM ** -0.5


def rope_table():
    inv_freq = np.float32(10000.0) ** (np.float32(-2.0) * np.arange(HALF, dtype=np.float32) / np.float32(HEAD_DIM))
    angles = np.arange(TAB_ROWS, dtype=np.float32)[:, None] * inv_freq.astype(np.float32)
    return np.concatenate([np.cos(angles), np.sin(angles)], axis=-1).astype(np.float32)


def norm_rows(x, gain):
    inv = lax.rsqrt(jnp.mean(x * x, axis=-1, keepdims=True) + 1e-5)
    return (x * inv * gain.astype(F32)).astype(BF)


def spread(tab):
    swapped = pltpu.roll(tab, HALF, 1)
    low = lax.broadcasted_iota(jnp.int32, tab.shape, 1) < HALF
    return jnp.where(low, tab, swapped), jnp.where(low, -swapped, tab)


def rotate(a, c, s):
    return a * c + pltpu.roll(a, HALF, 1) * s


def layer_kernel(lens, prompt, new_tok, gain_a, gain_m, table, wq, wk, wv, wo, wg, wu, wd,
                 kv_out, new_out, dec_out, last_out,
                 xbuf, xrecv, wbuf, wqb, wob, wgb, wub, wdb, tab, tmp, stage,
                 lastf, lsend, lrecv, rows, qall, part, precv, kself, vself, attn, flat,
                 psend, rrecv, hid, norm2,
                 lsem, xsem, ysend, yrecv, wsend, wrecv, osend, orecv, ssem,
                 l_s, l_r, q_s, q_r, p_s, p_r, r_s, r_r, a_s, a_r):
    rep = lax.axis_index('replica')
    me = lax.axis_index('model')
    core = lax.rem(me, 2)
    xpos = lax.rem(me // 2, 2)
    ypos = me // 4
    flips = (1 - 2 * core, 2 - 4 * xpos, 4 - 8 * ypos)
    near = [me + sum(f for i, f in enumerate(flips) if d >> i & 1) for d in range(8)]
    sib, xnb, xsb, ynb = near[1], near[2], near[3], near[4]
    znb = 1 - rep

    barrier = pltpu.get_barrier_semaphore()
    for peer in [(rep, near[d]) for d in range(1, 8)] + [(znb, me)]:
        pl.semaphore_signal(barrier, inc=1, device_id=peer, device_id_type=MESH)
    pl.semaphore_wait(barrier, 8)

    def remote(src, dst, send, recv, peer):
        return pltpu.make_async_remote_copy(src_ref=src, dst_ref=dst, send_sem=send, recv_sem=recv, device_id=peer, device_id_type=MESH)

    def y_copy(b):
        return remote(prompt.at[b], xrecv.at[b], ysend.at[b], yrecv.at[b], (rep, ynb))

    def x_load(b):
        return pltpu.make_async_copy(prompt.at[b], xbuf.at[b], xsem.at[b])

    loads = [pltpu.make_async_copy(a, b, lsem.at[i]) for i, (a, b) in enumerate((
        (wk.at[0], wbuf.at[0, 0]), (wv.at[0], wbuf.at[0, 1]), (table, tab), (wq.at[0], wqb), (wo.at[0], wob),
        (wg.at[0], wgb), (wu.at[0], wub), (wd.at[0], wdb)))]
    for i, w in enumerate((wk, wv)):
        @pl.when(rep == i)
        def _():
            remote(w.at[0], wbuf.at[2, rep], wsend.at[0], wrecv.at[0], (rep, xnb)).start()

    y_copy(0).start()
    loads[0].start()
    loads[1].start()

    @pl.loop(0, BATCH)
    def _(b):
        x_load(b).start()

    for load in loads[2:]:
        load.start()
    w_x = remote(wbuf.at[0, rep], wbuf.at[2, rep], wsend.at[0], wrecv.at[0], (rep, xnb))
    w_s = remote(wbuf.at[0], wbuf.at[1], wsend.at[1], wrecv.at[1], (rep, sib))
    w_z = remote(wbuf.at[2, rep], wbuf.at[2, rep], wsend.at[2], wrecv.at[2], (znb, me))
    w_xs = remote(wbuf.at[2, rep], wbuf.at[3, rep], wsend.at[3], wrecv.at[3], (rep, sib))
    w_zs = remote(wbuf.at[2, znb], wbuf.at[3, znb], wsend.at[4], wrecv.at[4], (rep, sib))
    loads[0].wait()
    loads[1].wait()
    w_s.start()

    def out_copy(s, b, o, kv):
        blk = me if s == 0 else ynb
        dst = kv_out.at[kv, b, pl.ds(pl.multiple_of(blk * ROWS, ROWS), ROWS), :]
        src = stage.at[s, b, o, kv]
        if o == 0:
            return pltpu.make_async_copy(src, dst, ssem.at[s, b, kv])
        return remote(src, dst, osend.at[o - 1, s, b, kv], orecv.at[o - 1, s, b, kv], (rep, near[o]))

    def project(buf, s, b, o, kv):
        acc = jnp.dot(buf[b], wbuf[o, kv], preferred_element_type=F32)
        blk = me if s == 0 else ynb
        c, sn = spread(tab[pl.ds(pl.multiple_of(blk * SEQ_LOC, SEQ_LOC), SEQ_LOC), :])
        is_k = kv == 0
        c = jnp.where(is_k, c, 1.0)
        sn = jnp.where(is_k, sn, 0.0)
        for h in range(2):
            tmp[pl.ds(h, SEQ_LOC, stride=2), :] = rotate(acc[:, h * HEAD_DIM:(h + 1) * HEAD_DIM], c, sn)
        stage[s, b, o, kv] = tmp[...].astype(BF)

    @pl.loop(0, BATCH)
    def _(b):
        x_load(b).wait()
        x = xbuf[b].astype(F32)
        here = me * SEQ_LOC + lax.broadcasted_iota(jnp.int32, (SEQ_LOC, 1), 0) == lens[b] - 1
        lastf[pl.ds(b, 1), :] = jnp.sum(jnp.where(here, x, 0.0), axis=0, keepdims=True)
        xbuf[b] = norm_rows(x, gain_a[...])

    l_copy = [remote(lsend.at[i], lrecv.at[i], l_s.at[i], l_r.at[i], (rep, near[d])) for i, d in enumerate((4, 1, 2))]
    lsend[0] = lastf[...].astype(BF)
    loads[2].wait()
    l_copy[0].start()

    @pl.loop(1, BATCH)
    def _(b):
        y_copy(b).start()

    @pl.loop(0, BATCH)
    def _(b):
        @pl.loop(0, 2)
        def _(kv):
            project(xbuf, 0, b, 0, kv)
            out_copy(0, b, 0, kv).start()

    def join_last(i):
        l_copy[i].wait_recv()
        return (lsend[i].astype(F32) + lrecv[i].astype(F32)).astype(BF)

    lsend[1] = join_last(0)
    w_s.wait_recv()
    l_copy[1].start()

    @pl.loop(0, BATCH)
    def _(b):
        @pl.loop(0, 2)
        def _(kv):
            project(xbuf, 0, b, 1, kv)
            out_copy(0, b, 1, kv).start()

    lsend[2] = join_last(1)

    w_x.wait_recv()
    w_z.start()
    w_xs.start()
    l_copy[2].start()

    def own_x_phase(kv, o):
        @pl.loop(0, BATCH)
        def _(b):
            project(xbuf, 0, b, o, kv)
            out_copy(0, b, o, kv).start()

    own_x_phase(rep, 2)
    w_xs.wait_recv()
    own_x_phase(rep, 3)

    rows[0:BATCH, :] = new_tok[...].astype(F32)
    rows[BATCH:2 * BATCH, :] = join_last(2).astype(F32)
    loads[3].wait()
    n16 = norm_rows(rows[...], gain_a[...])
    q16 = jnp.dot(n16, wqb[...], preferred_element_type=F32)
    k16 = jnp.dot(n16, wbuf[0, 0], preferred_element_type=F32)
    v16 = jnp.dot(n16, wbuf[0, 1], preferred_element_type=F32)
    for b in range(BATCH):
        flat[pl.ds(b, 1), 0:HEAD_DIM] = tab[pl.ds(jnp.clip(lens[b], 0, SEQ_LEN), 1), :]
        flat[pl.ds(BATCH + b, 1), 0:HEAD_DIM] = tab[pl.ds(jnp.clip(lens[b] - 1, 0, SEQ_LEN), 1), :]
    c16, s16 = spread(flat[:, 0:HEAD_DIM])
    kself[...] = jnp.zeros_like(kself)
    vself[...] = jnp.zeros_like(vself)
    for h in range(2):
        lanes = slice(h * HEAD_DIM, (h + 1) * HEAD_DIM)
        qh = rotate(q16[:, lanes], c16, s16).astype(BF).astype(F32)
        kh = rotate(k16[:, lanes], c16, s16)[:BATCH].astype(BF).astype(F32)
        vh = v16[:BATCH, lanes].astype(BF).astype(F32)
        for g in range(2):
            qall[0, :, 2 * g + h, :] = qh[g * BATCH:(g + 1) * BATCH]
        kself[:, h, :] = kh
        vself[:, h, :] = vh
        tmp[pl.ds(h, BATCH, stride=2), :] = kh
        tmp[pl.ds(2 * BATCH + h, BATCH, stride=2), :] = vh
    new_out[0] = tmp[0:2 * BATCH, :].astype(BF)
    new_out[1] = tmp[2 * BATCH:4 * BATCH, :].astype(BF)
    low = lax.broadcasted_iota(jnp.int32, (4, HEAD_DIM), 1) < HALF
    part[:, 0] = jnp.zeros((4, BATCH, 4, HEAD_DIM), F32)
    part[:, 1] = jnp.broadcast_to(jnp.where(low, NEG_BIG, 0.0), (4, BATCH, 4, HEAD_DIM))
    q_copy = [remote(qall.at[0], qall.at[d], q_s.at[d - 1], q_r.at[d - 1], (rep, near[d])) for d in (1, 2, 3)]
    for c in q_copy:
        c.start()

    w_z.wait_recv()
    w_zs.start()
    w_zs.wait_recv()
    own_x_phase(znb, 2)
    own_x_phase(znb, 3)
    for c in q_copy:
        c.wait_recv()

    lane = lax.broadcasted_iota(jnp.int32, (4, ROWS), 1)
    same_head = lane % 2 == lax.broadcasted_iota(jnp.int32, (4, ROWS), 0) % 2

    def attend(s, b):
        blk = me if s == 0 else ynb
        seen = same_head & (blk * SEQ_LOC + lane // 2 < lens[b])
        for o in range(4):
            sc = lax.dot_general(qall[o, b].astype(BF), stage[s, b, o, 0], (((1,), (1,)), ((), ())), preferred_element_type=F32) * SCALE
            sc = jnp.where(seen, sc, NEG_BIG)
            old = part[o, 1, b]
            m_old, l_old = old[:, 0:1], old[:, HALF:HALF + 1]
            m_new = jnp.maximum(m_old, jnp.max(sc, axis=-1, keepdims=True))
            p = jnp.where(seen, jnp.exp(sc - m_new), 0.0)
            fade = jnp.exp(m_old - m_new)
            l_new = l_old * fade + jnp.sum(p, axis=-1, keepdims=True)
            part[o, 0, b] = part[o, 0, b] * fade + jnp.dot(p.astype(BF), stage[s, b, o, 1], preferred_element_type=F32)
            part[o, 1, b] = jnp.where(low, m_new, l_new)

    waiting = [(b, kv, o) for b in range(5, BATCH) for kv in range(2) for o in (2, 3)]

    def leave(b, kv, o):
        out_copy(1, b, o, kv).start()

    @pl.loop(0, BATCH)
    def _(b):
        attend(0, b)
        y_copy(b).wait_recv()

        @pl.when(b == BATCH - 1)
        def _():
            for job in waiting[2:5]:
                leave(*job)
        xrecv[b] = norm_rows(xrecv[b].astype(F32), gain_a[...])

        @pl.loop(0, 2)
        def _(kv):
            for o in (2, 3):
                project(xrecv, 1, b, o, kv)

                @pl.when(b < 5)
                def _():
                    out_copy(1, b, o, kv).start()

            for o in (1, 0):
                project(xrecv, 1, b, o, kv)
                out_copy(1, b, o, kv).start()

        @pl.when(b == BATCH - 2)
        def _():
            for job in waiting[0:2]:
                leave(*job)

        attend(1, b)

    p_copy = [remote(part.at[d], precv.at[d - 1], p_s.at[d - 1], p_r.at[d - 1], (rep, near[d])) for d in (1, 2, 3)]
    for c in p_copy:
        c.start()
    for job in waiting[5:7]:
        leave(*job)
    for load in loads[4:]:
        load.wait()
    first = lax.broadcasted_iota(jnp.int32, (BATCH, 4, 1), 1) < 2
    s_self = jnp.where(first, jnp.sum(qall[0] * kself[...], axis=-1, keepdims=True) * SCALE, NEG_BIG)
    for c in p_copy:
        c.wait_recv()
    accs = [part[0, 0]] + [precv[i, 0] for i in range(3)]
    stats = [part[0, 1]] + [precv[i, 1] for i in range(3)]
    tops = [st[:, :, 0:1] for st in stats]
    top = s_self
    for t in tops:
        top = jnp.maximum(top, t)
    e_self = jnp.where(first, jnp.exp(s_self - top), 0.0)
    den = e_self
    num = e_self * vself[...]
    for t, st, ac in zip(tops, stats, accs):
        e = jnp.exp(t - top)
        den = den + e * st[:, :, HALF:HALF + 1]
        num = num + e * ac
    attn[...] = num / den
    for g in range(2):
        for h in range(2):
            flat[g * BATCH:(g + 1) * BATCH, h * HEAD_DIM:(h + 1) * HEAD_DIM] = attn[:, 2 * g + h, :]

    def reduce_columns(i, base, jobs):
        sends = [remote(psend.at[i, near[d]], rrecv.at[i, d - 1], r_s.at[i, d - 1], r_r.at[i, d - 1], (rep, near[d])) for d in range(1, 8)]
        for c in sends:
            c.start()
        for job in jobs[0]:
            leave(*job)
        total = psend[i, me]
        for d in range(1, 8):
            sends[d - 1].wait_recv()
            total = total + rrecv[i, d - 1]
        hid[i, me] = (base + total).astype(BF)
        gets = [remote(hid.at[i, me], hid.at[i, me], a_s.at[i, d - 1], a_r.at[i, d - 1], (rep, near[d])) for d in range(1, 8)]
        for c in gets:
            c.start()
        for job in jobs[1]:
            leave(*job)
        for d in range(1, 8):
            remote(hid.at[i, near[d]], hid.at[i, near[d]], a_s.at[i, d - 1], a_r.at[i, d - 1], (rep, near[d])).wait_recv()
        return sends + gets

    a16 = flat[...].astype(BF)
    for j in range(8):
        psend[0, j] = jnp.dot(a16, wob[:, j * SHARD:(j + 1) * SHARD], preferred_element_type=F32)
    mine = pl.ds(pl.multiple_of(me * SHARD, SHARD), SHARD)
    done = reduce_columns(0, rows[:, mine], (waiting[7:8], waiting[8:11]))

    sq = jnp.zeros((2 * BATCH, 1), F32)
    for j in range(8):
        hj = hid[0, j].astype(F32)
        sq = sq + jnp.sum(hj * hj, axis=-1, keepdims=True)
    inv = lax.rsqrt(sq / D_MODEL + 1e-5)
    for j in range(8):
        cols = slice(j * SHARD, (j + 1) * SHARD)
        norm2[:, cols] = (hid[0, j].astype(F32) * inv * gain_m[:, cols].astype(F32)).astype(BF)
    n2 = norm2[...]
    gate = jnp.dot(n2, wgb[...], preferred_element_type=F32)
    up = jnp.dot(n2, wub[...], preferred_element_type=F32)
    mid = (gate * jax.nn.sigmoid(gate) * up).astype(BF)
    for j in range(8):
        psend[1, j] = jnp.dot(mid, wdb[:, j * SHARD:(j + 1) * SHARD], preferred_element_type=F32)
    done += reduce_columns(1, hid[0, me].astype(F32), (waiting[11:12], ()))
    for j in range(8):
        cols = slice(j * SHARD, (j + 1) * SHARD)
        dec_out[:, cols] = hid[1, j][:BATCH]
        last_out[:, cols] = hid[1, j][BATCH:]

    for c in [w_x, w_s, w_z, w_xs, w_zs] + l_copy + q_copy + p_copy + done:
        c.wait_send()

    @pl.loop(0, BATCH)
    def _(b):
        y_copy(b).wait_send()
        for s in range(2):
            for kv in range(2):
                for o in range(4):
                    out_copy(s, b, o, kv).wait()


def layer(lens, prompt, new_tok, gain_a, gain_m, table, wq, wk, wv, wo, wg, wu, wd):
    vmem = pl.BlockSpec(memory_space=pltpu.VMEM)
    anym = pl.BlockSpec(memory_space=pl.ANY)
    dma = pltpu.SemaphoreType.DMA
    v = pltpu.VMEM
    return pl.pallas_call(
        layer_kernel,
        out_shape=(
            jax.ShapeDtypeStruct((2, BATCH, 8 * ROWS, HEAD_DIM), BF),
            jax.ShapeDtypeStruct((2, 2 * BATCH, HEAD_DIM), BF),
            jax.ShapeDtypeStruct((BATCH, D_MODEL), BF),
            jax.ShapeDtypeStruct((BATCH, D_MODEL), BF),
        ),
        in_specs=[pl.BlockSpec(memory_space=pltpu.SMEM), anym, vmem, vmem, vmem] + [anym] * 8,
        out_specs=(anym, vmem, vmem, vmem),
        scratch_shapes=[
            v((BATCH, SEQ_LOC, D_MODEL), BF), v((BATCH, SEQ_LOC, D_MODEL), BF), v((4, 2, D_MODEL, SHARD), BF),
            v((D_MODEL, SHARD), BF), v((SHARD, D_MODEL), BF), v((D_MODEL, FF_LOC), BF), v((D_MODEL, FF_LOC), BF), v((FF_LOC, D_MODEL), BF),
            v((TAB_ROWS, HEAD_DIM), F32), v((ROWS, HEAD_DIM), F32), v((2, BATCH, 4, 2, ROWS, HEAD_DIM), BF),
            v((BATCH, D_MODEL), F32), v((3, BATCH, D_MODEL), BF), v((3, BATCH, D_MODEL), BF), v((2 * BATCH, D_MODEL), F32),
            v((4, BATCH, 4, HEAD_DIM), F32), v((4, 2, BATCH, 4, HEAD_DIM), F32), v((3, 2, BATCH, 4, HEAD_DIM), F32),
            v((BATCH, 4, HEAD_DIM), F32), v((BATCH, 4, HEAD_DIM), F32), v((BATCH, 4, HEAD_DIM), F32), v((2 * BATCH, SHARD), F32),
            v((2, 8, 2 * BATCH, SHARD), F32), v((2, 7, 2 * BATCH, SHARD), F32), v((2, 8, 2 * BATCH, SHARD), BF), v((2 * BATCH, D_MODEL), BF),
            dma((8,)), dma((BATCH,)), dma((BATCH,)), dma((BATCH,)), dma((5,)), dma((5,)),
            dma((3, 2, BATCH, 2)), dma((3, 2, BATCH, 2)), dma((2, BATCH, 2)),
            dma((3,)), dma((3,)), dma((3,)), dma((3,)), dma((3,)), dma((3,)),
            dma((2, 7)), dma((2, 7)), dma((2, 7)), dma((2, 7)),
        ],
        compiler_params=pltpu.CompilerParams(collective_id=0, has_side_effects=True, vmem_limit_bytes=62 * 1024 * 1024),
        cost_estimate=pl.CostEstimate(flops=26_000_000_000, bytes_accessed=60_000_000, transcendentals=0),
        name='layer',
    )(lens, prompt, new_tok, gain_a, gain_m, table, wq, wk, wv, wo, wg, wu, wd)


def cache_kernel(kv, new, key_out, val_out, buf, row, load, store, row_sem):
    outs = (key_out, val_out)
    ins = [[pltpu.make_async_copy(kv.at[i, b], buf.at[i, b], load.at[i, b]) for b in range(BATCH)] for i in range(2)]
    rows_in = pltpu.make_async_copy(new, row, row_sem.at[0])
    rows_in.start()
    for i in range(2):
        for b in range(BATCH):
            ins[i][b].start()
    rows_in.wait()
    puts = [pltpu.make_async_copy(row.at[i], outs[i].at[0, :, pl.ds(SEQ_LEN, 1)], row_sem.at[1 + i]) for i in range(2)]
    for c in puts:
        c.start()
    for i in range(2):
        for b in range(BATCH):
            ins[i][b].wait()
            puts.append(pltpu.make_async_copy(buf.at[i, b], outs[i].at[0, b, pl.ds(0, SEQ_LEN)], store.at[i, b]))
            puts[-1].start()
    for c in puts:
        c.wait()


def caches(kv, new):
    anym = pl.BlockSpec(memory_space=pl.ANY)
    dma = pltpu.SemaphoreType.DMA
    shape = jax.ShapeDtypeStruct((1, BATCH, SEQ_LEN + 1, 2, HEAD_DIM), BF)
    return pl.pallas_call(
        cache_kernel,
        out_shape=(shape, shape),
        in_specs=[anym, anym],
        out_specs=(anym, anym),
        scratch_shapes=[
            pltpu.VMEM((2, BATCH, SEQ_LEN, 2, HEAD_DIM), BF), pltpu.VMEM((2, BATCH, 1, 2, HEAD_DIM), BF),
            dma((2, BATCH)), dma((2, BATCH)), dma((3,)),
        ],
        compiler_params=pltpu.CompilerParams(vmem_limit_bytes=62 * 1024 * 1024),
        cost_estimate=pl.CostEstimate(flops=0, bytes_accessed=50_000_000, transcendentals=0),
        name='caches',
    )(kv, new)


def solution(mesh):
    seq_spec = P('replica', 'model', None)
    col_spec = P(None, None, 'model')
    row_spec = P(None, 'model', None)
    gain_spec = P(None, None)
    tok_spec = P('replica', None)
    cache_spec = P(None, 'replica', None, 'model', None)
    in_specs = (seq_spec, P('replica'), tok_spec, gain_spec, col_spec, col_spec, col_spec, row_spec, gain_spec, col_spec, col_spec, row_spec)
    out_specs = (tok_spec, tok_spec, cache_spec, cache_spec)
    table = rope_table()

    def per_device(prompt, lengths, new_tok, norm_attn, w_q, w_k, w_v, w_o, norm_mlp, w_gate, w_up, w_down):
        kv, new, dec, last = layer(lengths, prompt, new_tok, norm_attn, norm_mlp, jnp.asarray(table), w_q, w_k, w_v, w_o, w_gate, w_up, w_down)
        keys, vals = caches(kv.reshape(2, BATCH, SEQ_LEN, 2, HEAD_DIM), new.reshape(2, BATCH, 1, 2, HEAD_DIM))
        return dec, last, keys, vals

    return jax.shard_map(per_device, mesh=mesh, in_specs=in_specs, out_specs=out_specs, check_vma=False)
```

```python
import jax
import jax.numpy as jnp
import numpy as np
from jax import lax
from jax.experimental import pallas as pl
from jax.experimental.pallas import tpu as pltpu
from jax.sharding import PartitionSpec as P

HEAD_DIM = 128
HALF = HEAD_DIM // 2
NEG_BIG = -1e30
BATCH = 8
SEQ_LOC = 192
SEQ_LEN = 1536
D_MODEL = 2048
SHARD = 256
FF_LOC = 1024
ROWS = 2 * SEQ_LOC
TAB_ROWS = SEQ_LEN + 8
MESH = pl.DeviceIdType.MESH
BF = jnp.bfloat16
F32 = jnp.float32
SCALE = HEAD_DIM ** -0.5


def rope_table():
    inv_freq = np.float32(10000.0) ** (np.float32(-2.0) * np.arange(HALF, dtype=np.float32) / np.float32(HEAD_DIM))
    angles = np.arange(TAB_ROWS, dtype=np.float32)[:, None] * inv_freq.astype(np.float32)
    return np.concatenate([np.cos(angles), np.sin(angles)], axis=-1).astype(np.float32)


def norm_rows(x, gain):
    inv = lax.rsqrt(jnp.mean(x * x, axis=-1, keepdims=True) + 1e-5)
    return (x * inv * gain.astype(F32)).astype(BF)


def spread(tab):
    swapped = pltpu.roll(tab, HALF, 1)
    low = lax.broadcasted_iota(jnp.int32, tab.shape, 1) < HALF
    return jnp.where(low, tab, swapped), jnp.where(low, -swapped, tab)


def rotate(a, c, s):
    return a * c + pltpu.roll(a, HALF, 1) * s


def layer_kernel(lens, prompt, new_tok, gain_a, gain_m, table, wq, wk, wv, wo, wg, wu, wd,
                 kv_out, new_out, dec_out, last_out,
                 xbuf, xrecv, wbuf, wqb, wob, wgb, wub, wdb, tab, tmp, stage,
                 lastf, lsend, lrecv, rows, qall, part, precv, kself, vself, attn, flat,
                 psend, rrecv, hid, norm2,
                 lsem, xsem, ysend, yrecv, wsend, wrecv, osend, orecv, ssem,
                 l_s, l_r, q_s, q_r, p_s, p_r, r_s, r_r, a_s, a_r):
    rep = lax.axis_index('replica')
    me = lax.axis_index('model')
    core = lax.rem(me, 2)
    xpos = lax.rem(me // 2, 2)
    ypos = me // 4
    flips = (1 - 2 * core, 2 - 4 * xpos, 4 - 8 * ypos)
    near = [me + sum(f for i, f in enumerate(flips) if d >> i & 1) for d in range(8)]
    sib, xnb, xsb, ynb = near[1], near[2], near[3], near[4]
    znb = 1 - rep

    barrier = pltpu.get_barrier_semaphore()
    for peer in [(rep, near[d]) for d in range(1, 8)] + [(znb, me)]:
        pl.semaphore_signal(barrier, inc=1, device_id=peer, device_id_type=MESH)
    pl.semaphore_wait(barrier, 8)

    def remote(src, dst, send, recv, peer):
        return pltpu.make_async_remote_copy(src_ref=src, dst_ref=dst, send_sem=send, recv_sem=recv, device_id=peer, device_id_type=MESH)

    def y_copy(b):
        return remote(prompt.at[b], xrecv.at[b], ysend.at[b], yrecv.at[b], (rep, ynb))

    def x_load(b):
        return pltpu.make_async_copy(prompt.at[b], xbuf.at[b], xsem.at[b])

    loads = [pltpu.make_async_copy(a, b, lsem.at[i]) for i, (a, b) in enumerate((
        (wk.at[0], wbuf.at[0, 0]), (wv.at[0], wbuf.at[0, 1]), (table, tab), (wq.at[0], wqb), (wo.at[0], wob),
        (wg.at[0], wgb), (wu.at[0], wub), (wd.at[0], wdb)))]
    for i, w in enumerate((wk, wv)):
        @pl.when(rep == i)
        def _():
            remote(w.at[0], wbuf.at[2, rep], wsend.at[0], wrecv.at[0], (rep, xnb)).start()

    y_copy(0).start()
    loads[0].start()
    loads[1].start()

    @pl.loop(0, BATCH)
    def _(b):
        x_load(b).start()

    for load in loads[2:]:
        load.start()
    w_x = remote(wbuf.at[0, rep], wbuf.at[2, rep], wsend.at[0], wrecv.at[0], (rep, xnb))
    w_s = remote(wbuf.at[0], wbuf.at[1], wsend.at[1], wrecv.at[1], (rep, sib))
    w_z = remote(wbuf.at[2, rep], wbuf.at[2, rep], wsend.at[2], wrecv.at[2], (znb, me))
    w_xs = remote(wbuf.at[2, rep], wbuf.at[3, rep], wsend.at[3], wrecv.at[3], (rep, sib))
    w_zs = remote(wbuf.at[2, znb], wbuf.at[3, znb], wsend.at[4], wrecv.at[4], (rep, sib))
    loads[0].wait()
    loads[1].wait()
    w_s.start()

    def out_copy(s, b, o, kv):
        blk = me if s == 0 else ynb
        dst = kv_out.at[kv, b, pl.ds(pl.multiple_of(blk * ROWS, ROWS), ROWS), :]
        src = stage.at[s, b, o, kv]
        if o == 0:
            return pltpu.make_async_copy(src, dst, ssem.at[s, b, kv])
        return remote(src, dst, osend.at[o - 1, s, b, kv], orecv.at[o - 1, s, b, kv], (rep, near[o]))

    def project(buf, s, b, o, kv):
        acc = jnp.dot(buf[b], wbuf[o, kv], preferred_element_type=F32)
        blk = me if s == 0 else ynb
        c, sn = spread(tab[pl.ds(pl.multiple_of(blk * SEQ_LOC, SEQ_LOC), SEQ_LOC), :])
        is_k = kv == 0
        c = jnp.where(is_k, c, 1.0)
        sn = jnp.where(is_k, sn, 0.0)
        for h in range(2):
            tmp[pl.ds(h, SEQ_LOC, stride=2), :] = rotate(acc[:, h * HEAD_DIM:(h + 1) * HEAD_DIM], c, sn)
        stage[s, b, o, kv] = tmp[...].astype(BF)

    @pl.loop(0, BATCH)
    def _(b):
        x_load(b).wait()
        x = xbuf[b].astype(F32)
        here = me * SEQ_LOC + lax.broadcasted_iota(jnp.int32, (SEQ_LOC, 1), 0) == lens[b] - 1
        lastf[pl.ds(b, 1), :] = jnp.sum(jnp.where(here, x, 0.0), axis=0, keepdims=True)
        xbuf[b] = norm_rows(x, gain_a[...])

    l_copy = [remote(lsend.at[i], lrecv.at[i], l_s.at[i], l_r.at[i], (rep, near[d])) for i, d in enumerate((4, 1, 2))]
    lsend[0] = lastf[...].astype(BF)
    loads[2].wait()
    l_copy[0].start()

    @pl.loop(1, BATCH)
    def _(b):
        y_copy(b).start()

    @pl.loop(0, BATCH)
    def _(b):
        @pl.loop(0, 2)
        def _(kv):
            project(xbuf, 0, b, 0, kv)
            out_copy(0, b, 0, kv).start()

    def join_last(i):
        l_copy[i].wait_recv()
        return (lsend[i].astype(F32) + lrecv[i].astype(F32)).astype(BF)

    lsend[1] = join_last(0)
    w_s.wait_recv()
    l_copy[1].start()

    @pl.loop(0, BATCH)
    def _(b):
        @pl.loop(0, 2)
        def _(kv):
            project(xbuf, 0, b, 1, kv)
            out_copy(0, b, 1, kv).start()

    lsend[2] = join_last(1)

    w_x.wait_recv()
    w_z.start()
    w_xs.start()
    l_copy[2].start()

    def own_x_phase(kv, o):
        @pl.loop(0, BATCH)
        def _(b):
            project(xbuf, 0, b, o, kv)
            out_copy(0, b, o, kv).start()

    own_x_phase(rep, 2)
    w_xs.wait_recv()
    own_x_phase(rep, 3)

    rows[0:BATCH, :] = new_tok[...].astype(F32)
    rows[BATCH:2 * BATCH, :] = join_last(2).astype(F32)
    loads[3].wait()
    n16 = norm_rows(rows[...], gain_a[...])
    q16 = jnp.dot(n16, wqb[...], preferred_element_type=F32)
    k16 = jnp.dot(n16, wbuf[0, 0], preferred_element_type=F32)
    v16 = jnp.dot(n16, wbuf[0, 1], preferred_element_type=F32)
    for b in range(BATCH):
        flat[pl.ds(b, 1), 0:HEAD_DIM] = tab[pl.ds(jnp.clip(lens[b], 0, SEQ_LEN), 1), :]
        flat[pl.ds(BATCH + b, 1), 0:HEAD_DIM] = tab[pl.ds(jnp.clip(lens[b] - 1, 0, SEQ_LEN), 1), :]
    c16, s16 = spread(flat[:, 0:HEAD_DIM])
    kself[...] = jnp.zeros_like(kself)
    vself[...] = jnp.zeros_like(vself)
    for h in range(2):
        lanes = slice(h * HEAD_DIM, (h + 1) * HEAD_DIM)
        qh = rotate(q16[:, lanes], c16, s16).astype(BF).astype(F32)
        kh = rotate(k16[:, lanes], c16, s16)[:BATCH].astype(BF).astype(F32)
        vh = v16[:BATCH, lanes].astype(BF).astype(F32)
        for g in range(2):
            qall[0, :, 2 * g + h, :] = qh[g * BATCH:(g + 1) * BATCH]
        kself[:, h, :] = kh
        vself[:, h, :] = vh
        tmp[pl.ds(h, BATCH, stride=2), :] = kh
        tmp[pl.ds(2 * BATCH + h, BATCH, stride=2), :] = vh
    new_out[0] = tmp[0:2 * BATCH, :].astype(BF)
    new_out[1] = tmp[2 * BATCH:4 * BATCH, :].astype(BF)
    low = lax.broadcasted_iota(jnp.int32, (4, HEAD_DIM), 1) < HALF
    part[:, 0] = jnp.zeros((4, BATCH, 4, HEAD_DIM), F32)
    part[:, 1] = jnp.broadcast_to(jnp.where(low, NEG_BIG, 0.0), (4, BATCH, 4, HEAD_DIM))
    q_copy = [remote(qall.at[0], qall.at[d], q_s.at[d - 1], q_r.at[d - 1], (rep, near[d])) for d in (1, 2, 3)]
    for c in q_copy:
        c.start()

    w_z.wait_recv()
    w_zs.start()
    w_zs.wait_recv()
    own_x_phase(znb, 2)
    own_x_phase(znb, 3)
    for c in q_copy:
        c.wait_recv()

    lane = lax.broadcasted_iota(jnp.int32, (4, ROWS), 1)
    same_head = lane % 2 == lax.broadcasted_iota(jnp.int32, (4, ROWS), 0) % 2

    def attend(s, b):
        blk = me if s == 0 else ynb
        seen = same_head & (blk * SEQ_LOC + lane // 2 < lens[b])
        for o in range(4):
            sc = lax.dot_general(qall[o, b].astype(BF), stage[s, b, o, 0], (((1,), (1,)), ((), ())), preferred_element_type=F32) * SCALE
            sc = jnp.where(seen, sc, NEG_BIG)
            old = part[o, 1, b]
            m_old, l_old = old[:, 0:1], old[:, HALF:HALF + 1]
            m_new = jnp.maximum(m_old, jnp.max(sc, axis=-1, keepdims=True))
            p = jnp.where(seen, jnp.exp(sc - m_new), 0.0)
            fade = jnp.exp(m_old - m_new)
            l_new = l_old * fade + jnp.sum(p, axis=-1, keepdims=True)
            part[o, 0, b] = part[o, 0, b] * fade + jnp.dot(p.astype(BF), stage[s, b, o, 1], preferred_element_type=F32)
            part[o, 1, b] = jnp.where(low, m_new, l_new)

    waiting = [(b, kv, o) for b in range(5, BATCH) for kv in range(2) for o in (2, 3)]

    def leave(b, kv, o):
        out_copy(1, b, o, kv).start()

    @pl.loop(0, BATCH)
    def _(b):
        attend(0, b)
        y_copy(b).wait_recv()

        @pl.when(b == BATCH - 1)
        def _():
            leave(*waiting[0])
        xrecv[b] = norm_rows(xrecv[b].astype(F32), gain_a[...])

        @pl.loop(0, 2)
        def _(kv):
            for o in (2, 3):
                project(xrecv, 1, b, o, kv)

                @pl.when(b < 5)
                def _():
                    out_copy(1, b, o, kv).start()

            for o in (1, 0):
                project(xrecv, 1, b, o, kv)
                out_copy(1, b, o, kv).start()

        attend(1, b)

    p_copy = [remote(part.at[d], precv.at[d - 1], p_s.at[d - 1], p_r.at[d - 1], (rep, near[d])) for d in (1, 2, 3)]
    for c in p_copy:
        c.start()
    for job in waiting[1:3]:
        leave(*job)
    for load in loads[4:]:
        load.wait()
    first = lax.broadcasted_iota(jnp.int32, (BATCH, 4, 1), 1) < 2
    s_self = jnp.where(first, jnp.sum(qall[0] * kself[...], axis=-1, keepdims=True) * SCALE, NEG_BIG)
    for c in p_copy:
        c.wait_recv()
    accs = [part[0, 0]] + [precv[i, 0] for i in range(3)]
    stats = [part[0, 1]] + [precv[i, 1] for i in range(3)]
    tops = [st[:, :, 0:1] for st in stats]
    top = s_self
    for t in tops:
        top = jnp.maximum(top, t)
    e_self = jnp.where(first, jnp.exp(s_self - top), 0.0)
    den = e_self
    num = e_self * vself[...]
    for t, st, ac in zip(tops, stats, accs):
        e = jnp.exp(t - top)
        den = den + e * st[:, :, HALF:HALF + 1]
        num = num + e * ac
    attn[...] = num / den
    for g in range(2):
        for h in range(2):
            flat[g * BATCH:(g + 1) * BATCH, h * HEAD_DIM:(h + 1) * HEAD_DIM] = attn[:, 2 * g + h, :]

    def reduce_columns(i, base, jobs):
        sends = [remote(psend.at[i, near[d]], rrecv.at[i, d - 1], r_s.at[i, d - 1], r_r.at[i, d - 1], (rep, near[d])) for d in range(1, 8)]
        for c in sends:
            c.start()
        for job in jobs[0]:
            leave(*job)
        total = psend[i, me]
        for d in range(1, 8):
            sends[d - 1].wait_recv()
            total = total + rrecv[i, d - 1]
        hid[i, me] = (base + total).astype(BF)
        gets = [remote(hid.at[i, me], hid.at[i, me], a_s.at[i, d - 1], a_r.at[i, d - 1], (rep, near[d])) for d in range(1, 8)]
        for c in gets:
            c.start()
        for job in jobs[1]:
            leave(*job)
        for d in range(1, 8):
            remote(hid.at[i, near[d]], hid.at[i, near[d]], a_s.at[i, d - 1], a_r.at[i, d - 1], (rep, near[d])).wait_recv()
        return sends + gets

    a16 = flat[...].astype(BF)
    for j in range(8):
        psend[0, j] = jnp.dot(a16, wob[:, j * SHARD:(j + 1) * SHARD], preferred_element_type=F32)
    mine = pl.ds(pl.multiple_of(me * SHARD, SHARD), SHARD)
    done = reduce_columns(0, rows[:, mine], (waiting[3:5], waiting[5:8]))

    sq = jnp.zeros((2 * BATCH, 1), F32)
    for j in range(8):
        hj = hid[0, j].astype(F32)
        sq = sq + jnp.sum(hj * hj, axis=-1, keepdims=True)
    inv = lax.rsqrt(sq / D_MODEL + 1e-5)
    for j in range(8):
        cols = slice(j * SHARD, (j + 1) * SHARD)
        norm2[:, cols] = (hid[0, j].astype(F32) * inv * gain_m[:, cols].astype(F32)).astype(BF)
    n2 = norm2[...]
    gate = jnp.dot(n2, wgb[...], preferred_element_type=F32)
    up = jnp.dot(n2, wub[...], preferred_element_type=F32)
    mid = (gate * jax.nn.sigmoid(gate) * up).astype(BF)
    for j in range(8):
        psend[1, j] = jnp.dot(mid, wdb[:, j * SHARD:(j + 1) * SHARD], preferred_element_type=F32)
    done += reduce_columns(1, hid[0, me].astype(F32), (waiting[8:10], waiting[10:12]))
    for j in range(8):
        cols = slice(j * SHARD, (j + 1) * SHARD)
        dec_out[:, cols] = hid[1, j][:BATCH]
        last_out[:, cols] = hid[1, j][BATCH:]

    for c in [w_x, w_s, w_z, w_xs, w_zs] + l_copy + q_copy + p_copy + done:
        c.wait_send()

    @pl.loop(0, BATCH)
    def _(b):
        y_copy(b).wait_send()
        for s in range(2):
            for kv in range(2):
                for o in range(4):
                    out_copy(s, b, o, kv).wait()


def layer(lens, prompt, new_tok, gain_a, gain_m, table, wq, wk, wv, wo, wg, wu, wd):
    vmem = pl.BlockSpec(memory_space=pltpu.VMEM)
    anym = pl.BlockSpec(memory_space=pl.ANY)
    dma = pltpu.SemaphoreType.DMA
    v = pltpu.VMEM
    return pl.pallas_call(
        layer_kernel,
        out_shape=(
            jax.ShapeDtypeStruct((2, BATCH, 8 * ROWS, HEAD_DIM), BF),
            jax.ShapeDtypeStruct((2, 2 * BATCH, HEAD_DIM), BF),
            jax.ShapeDtypeStruct((BATCH, D_MODEL), BF),
            jax.ShapeDtypeStruct((BATCH, D_MODEL), BF),
        ),
        in_specs=[pl.BlockSpec(memory_space=pltpu.SMEM), anym, vmem, vmem, vmem] + [anym] * 8,
        out_specs=(anym, vmem, vmem, vmem),
        scratch_shapes=[
            v((BATCH, SEQ_LOC, D_MODEL), BF), v((BATCH, SEQ_LOC, D_MODEL), BF), v((4, 2, D_MODEL, SHARD), BF),
            v((D_MODEL, SHARD), BF), v((SHARD, D_MODEL), BF), v((D_MODEL, FF_LOC), BF), v((D_MODEL, FF_LOC), BF), v((FF_LOC, D_MODEL), BF),
            v((TAB_ROWS, HEAD_DIM), F32), v((ROWS, HEAD_DIM), F32), v((2, BATCH, 4, 2, ROWS, HEAD_DIM), BF),
            v((BATCH, D_MODEL), F32), v((3, BATCH, D_MODEL), BF), v((3, BATCH, D_MODEL), BF), v((2 * BATCH, D_MODEL), F32),
            v((4, BATCH, 4, HEAD_DIM), F32), v((4, 2, BATCH, 4, HEAD_DIM), F32), v((3, 2, BATCH, 4, HEAD_DIM), F32),
            v((BATCH, 4, HEAD_DIM), F32), v((BATCH, 4, HEAD_DIM), F32), v((BATCH, 4, HEAD_DIM), F32), v((2 * BATCH, SHARD), F32),
            v((2, 8, 2 * BATCH, SHARD), F32), v((2, 7, 2 * BATCH, SHARD), F32), v((2, 8, 2 * BATCH, SHARD), BF), v((2 * BATCH, D_MODEL), BF),
            dma((8,)), dma((BATCH,)), dma((BATCH,)), dma((BATCH,)), dma((5,)), dma((5,)),
            dma((3, 2, BATCH, 2)), dma((3, 2, BATCH, 2)), dma((2, BATCH, 2)),
            dma((3,)), dma((3,)), dma((3,)), dma((3,)), dma((3,)), dma((3,)),
            dma((2, 7)), dma((2, 7)), dma((2, 7)), dma((2, 7)),
        ],
        compiler_params=pltpu.CompilerParams(collective_id=0, has_side_effects=True, vmem_limit_bytes=62 * 1024 * 1024),
        cost_estimate=pl.CostEstimate(flops=26_000_000_000, bytes_accessed=60_000_000, transcendentals=0),
        name='layer',
    )(lens, prompt, new_tok, gain_a, gain_m, table, wq, wk, wv, wo, wg, wu, wd)


def cache_kernel(kv, new, dec, last, key_out, val_out, dec_out, last_out, buf, row, load, store, row_sem):
    outs = (key_out, val_out)
    ins = [[pltpu.make_async_copy(kv.at[i, b], buf.at[i, b], load.at[i, b]) for b in range(BATCH)] for i in range(2)]
    rows_in = pltpu.make_async_copy(new, row, row_sem.at[0])
    rows_in.start()
    for i in range(2):
        for b in range(BATCH):
            ins[i][b].start()
    dec_out[...] = dec[...]
    last_out[...] = last[...]
    rows_in.wait()
    puts = [pltpu.make_async_copy(row.at[i], outs[i].at[0, :, pl.ds(SEQ_LEN, 1)], row_sem.at[1 + i]) for i in range(2)]
    for c in puts:
        c.start()
    for i in range(2):
        for b in range(BATCH):
            ins[i][b].wait()
            puts.append(pltpu.make_async_copy(buf.at[i, b], outs[i].at[0, b, pl.ds(0, SEQ_LEN)], store.at[i, b]))
            puts[-1].start()
    for c in puts:
        c.wait()


def caches(kv, new, dec, last):
    anym = pl.BlockSpec(memory_space=pl.ANY)
    dma = pltpu.SemaphoreType.DMA
    vmem = pl.BlockSpec(memory_space=pltpu.VMEM)
    shape = jax.ShapeDtypeStruct((1, BATCH, SEQ_LEN + 1, 2, HEAD_DIM), BF)
    row = jax.ShapeDtypeStruct((BATCH, D_MODEL), BF)
    return pl.pallas_call(
        cache_kernel,
        out_shape=(shape, shape, row, row),
        in_specs=[anym, anym, vmem, vmem],
        out_specs=(anym, anym, vmem, vmem),
        scratch_shapes=[
            pltpu.VMEM((2, BATCH, SEQ_LEN, 2, HEAD_DIM), BF), pltpu.VMEM((2, BATCH, 1, 2, HEAD_DIM), BF),
            dma((2, BATCH)), dma((2, BATCH)), dma((3,)),
        ],
        compiler_params=pltpu.CompilerParams(vmem_limit_bytes=62 * 1024 * 1024),
        cost_estimate=pl.CostEstimate(flops=0, bytes_accessed=50_000_000, transcendentals=0),
        name='caches',
    )(kv, new, dec, last)


def solution(mesh):
    seq_spec = P('replica', 'model', None)
    col_spec = P(None, None, 'model')
    row_spec = P(None, 'model', None)
    gain_spec = P(None, None)
    tok_spec = P('replica', None)
    cache_spec = P(None, 'replica', None, 'model', None)
    in_specs = (seq_spec, P('replica'), tok_spec, gain_spec, col_spec, col_spec, col_spec, row_spec, gain_spec, col_spec, col_spec, row_spec)
    out_specs = (tok_spec, tok_spec, cache_spec, cache_spec)
    table = rope_table()

    def per_device(prompt, lengths, new_tok, norm_attn, w_q, w_k, w_v, w_o, norm_mlp, w_gate, w_up, w_down):
        kv, new, dec, last = layer(lengths, prompt, new_tok, norm_attn, norm_mlp, jnp.asarray(table), w_q, w_k, w_v, w_o, w_gate, w_up, w_down)
        keys, vals, dec, last = caches(kv.reshape(2, BATCH, SEQ_LEN, 2, HEAD_DIM), new.reshape(2, BATCH, 1, 2, HEAD_DIM), dec, last)
        return dec, last, keys, vals

    return jax.shard_map(per_device, mesh=mesh, in_specs=in_specs, out_specs=out_specs, check_vma=False)
```

```python
import jax
import jax.numpy as jnp
import numpy as np
from jax import lax
from jax.experimental import pallas as pl
from jax.experimental.pallas import tpu as pltpu
from jax.sharding import PartitionSpec as P

HEAD_DIM = 128
HALF = HEAD_DIM // 2
NEG_BIG = -1e30
BATCH = 8
SEQ_LOC = 192
SEQ_LEN = 1536
D_MODEL = 2048
SHARD = 256
FF_LOC = 1024
ROWS = 2 * SEQ_LOC
TAB_ROWS = SEQ_LEN + 8
MESH = pl.DeviceIdType.MESH
BF = jnp.bfloat16
F32 = jnp.float32
SCALE = HEAD_DIM ** -0.5


def rope_table():
    inv_freq = np.float32(10000.0) ** (np.float32(-2.0) * np.arange(HALF, dtype=np.float32) / np.float32(HEAD_DIM))
    angles = np.arange(TAB_ROWS, dtype=np.float32)[:, None] * inv_freq.astype(np.float32)
    return np.concatenate([np.cos(angles), np.sin(angles)], axis=-1).astype(np.float32)


def norm_rows(x, gain):
    inv = lax.rsqrt(jnp.mean(x * x, axis=-1, keepdims=True) + 1e-5)
    return (x * inv * gain.astype(F32)).astype(BF)


def spread(tab):
    swapped = pltpu.roll(tab, HALF, 1)
    low = lax.broadcasted_iota(jnp.int32, tab.shape, 1) < HALF
    return jnp.where(low, tab, swapped), jnp.where(low, -swapped, tab)


def rotate(a, c, s):
    return a * c + pltpu.roll(a, HALF, 1) * s


def layer_kernel(lens, prompt, new_tok, gain_a, gain_m, table, wq, wk, wv, wo, wg, wu, wd,
                 kv_out, new_out, dec_out, last_out,
                 xbuf, xrecv, wbuf, wqb, wob, wgb, wub, wdb, tab, tmp, stage,
                 lastf, lsend, lrecv, rows, qall, part, precv, kself, vself, attn, flat,
                 psend, rrecv, hid, norm2,
                 lsem, xsem, ysend, yrecv, wsend, wrecv, osend, orecv, ssem,
                 l_s, l_r, q_s, q_r, p_s, p_r, r_s, r_r, a_s, a_r):
    rep = lax.axis_index('replica')
    me = lax.axis_index('model')
    core = lax.rem(me, 2)
    xpos = lax.rem(me // 2, 2)
    ypos = me // 4
    flips = (1 - 2 * core, 2 - 4 * xpos, 4 - 8 * ypos)
    near = [me + sum(f for i, f in enumerate(flips) if d >> i & 1) for d in range(8)]
    sib, xnb, xsb, ynb = near[1], near[2], near[3], near[4]
    znb = 1 - rep

    barrier = pltpu.get_barrier_semaphore()
    for peer in [(rep, near[d]) for d in range(1, 8)] + [(znb, me)]:
        pl.semaphore_signal(barrier, inc=1, device_id=peer, device_id_type=MESH)
    pl.semaphore_wait(barrier, 8)

    def remote(src, dst, send, recv, peer):
        return pltpu.make_async_remote_copy(src_ref=src, dst_ref=dst, send_sem=send, recv_sem=recv, device_id=peer, device_id_type=MESH)

    def y_copy(b):
        return remote(prompt.at[b], xrecv.at[b], ysend.at[b], yrecv.at[b], (rep, ynb))

    def x_load(b):
        return pltpu.make_async_copy(prompt.at[b], xbuf.at[b], xsem.at[b])

    loads = [pltpu.make_async_copy(a, b, lsem.at[i]) for i, (a, b) in enumerate((
        (wk.at[0], wbuf.at[0, 0]), (wv.at[0], wbuf.at[0, 1]), (table, tab), (wq.at[0], wqb), (wo.at[0], wob),
        (wg.at[0], wgb), (wu.at[0], wub), (wd.at[0], wdb)))]
    for i, w in enumerate((wk, wv)):
        @pl.when(rep == i)
        def _():
            remote(w.at[0], wbuf.at[2, rep], wsend.at[0], wrecv.at[0], (rep, xnb)).start()

    y_copy(0).start()
    loads[0].start()
    loads[1].start()

    @pl.loop(0, BATCH)
    def _(b):
        x_load(b).start()

    for load in loads[2:]:
        load.start()
    w_x = remote(wbuf.at[0, rep], wbuf.at[2, rep], wsend.at[0], wrecv.at[0], (rep, xnb))
    w_s = remote(wbuf.at[0], wbuf.at[1], wsend.at[1], wrecv.at[1], (rep, sib))
    w_z = remote(wbuf.at[2, rep], wbuf.at[2, rep], wsend.at[2], wrecv.at[2], (znb, me))
    w_xs = remote(wbuf.at[2, rep], wbuf.at[3, rep], wsend.at[3], wrecv.at[3], (rep, sib))
    w_zs = remote(wbuf.at[2, znb], wbuf.at[3, znb], wsend.at[4], wrecv.at[4], (rep, sib))
    loads[0].wait()
    loads[1].wait()
    w_s.start()

    def out_copy(s, b, o, kv):
        blk = me if s == 0 else ynb
        dst = kv_out.at[kv, b, pl.ds(pl.multiple_of(blk * ROWS, ROWS), ROWS), :]
        src = stage.at[s, b, o, kv]
        if o == 0:
            return pltpu.make_async_copy(src, dst, ssem.at[s, b, kv])
        return remote(src, dst, osend.at[o - 1, s, b, kv], orecv.at[o - 1, s, b, kv], (rep, near[o]))

    def own_two(b, o, kv):
        dst = kv_out.at[kv, pl.ds(b, 2), pl.ds(pl.multiple_of(me * ROWS, ROWS), ROWS), :]
        return remote(stage.at[0, pl.ds(b, 2), o, kv], dst, osend.at[o - 1, 0, b, kv], orecv.at[o - 1, 0, b, kv], (rep, near[o]))

    def chunk_kv(b, o):
        dst = kv_out.at[:, b, pl.ds(pl.multiple_of(ynb * ROWS, ROWS), ROWS), :]
        return remote(stage.at[1, b, o], dst, osend.at[o - 1, 1, b, 0], orecv.at[o - 1, 1, b, 0], (rep, near[o]))

    def project(buf, s, b, o, kv):
        acc = jnp.dot(buf[b], wbuf[o, kv], preferred_element_type=F32)
        blk = me if s == 0 else ynb
        c, sn = spread(tab[pl.ds(pl.multiple_of(blk * SEQ_LOC, SEQ_LOC), SEQ_LOC), :])
        is_k = kv == 0
        c = jnp.where(is_k, c, 1.0)
        sn = jnp.where(is_k, sn, 0.0)
        for h in range(2):
            tmp[pl.ds(h, SEQ_LOC, stride=2), :] = rotate(acc[:, h * HEAD_DIM:(h + 1) * HEAD_DIM], c, sn)
        stage[s, b, o, kv] = tmp[...].astype(BF)

    @pl.loop(0, BATCH)
    def _(b):
        x_load(b).wait()
        x = xbuf[b].astype(F32)
        here = me * SEQ_LOC + lax.broadcasted_iota(jnp.int32, (SEQ_LOC, 1), 0) == lens[b] - 1
        lastf[pl.ds(b, 1), :] = jnp.sum(jnp.where(here, x, 0.0), axis=0, keepdims=True)
        xbuf[b] = norm_rows(x, gain_a[...])

    l_copy = [remote(lsend.at[i], lrecv.at[i], l_s.at[i], l_r.at[i], (rep, near[d])) for i, d in enumerate((4, 1, 2))]
    lsend[0] = lastf[...].astype(BF)
    loads[2].wait()
    l_copy[0].start()

    @pl.loop(1, BATCH)
    def _(b):
        y_copy(b).start()

    @pl.loop(0, BATCH)
    def _(b):
        @pl.loop(0, 2)
        def _(kv):
            project(xbuf, 0, b, 0, kv)
            out_copy(0, b, 0, kv).start()

    def join_last(i):
        l_copy[i].wait_recv()
        return (lsend[i].astype(F32) + lrecv[i].astype(F32)).astype(BF)

    lsend[1] = join_last(0)
    w_s.wait_recv()
    l_copy[1].start()

    @pl.loop(0, BATCH)
    def _(b):
        @pl.loop(0, 2)
        def _(kv):
            project(xbuf, 0, b, 1, kv)
            out_copy(0, b, 1, kv).start()

    lsend[2] = join_last(1)

    w_x.wait_recv()
    w_z.start()
    w_xs.start()
    l_copy[2].start()

    def own_x_phase(kv, o):
        @pl.loop(0, BATCH, step=2)
        def _(b):
            project(xbuf, 0, b, o, kv)
            project(xbuf, 0, b + 1, o, kv)
            own_two(b, o, kv).start()

    own_x_phase(rep, 2)
    w_xs.wait_recv()
    own_x_phase(rep, 3)

    rows[0:BATCH, :] = new_tok[...].astype(F32)
    rows[BATCH:2 * BATCH, :] = join_last(2).astype(F32)
    loads[3].wait()
    n16 = norm_rows(rows[...], gain_a[...])
    q16 = jnp.dot(n16, wqb[...], preferred_element_type=F32)
    k16 = jnp.dot(n16, wbuf[0, 0], preferred_element_type=F32)
    v16 = jnp.dot(n16, wbuf[0, 1], preferred_element_type=F32)
    for b in range(BATCH):
        flat[pl.ds(b, 1), 0:HEAD_DIM] = tab[pl.ds(jnp.clip(lens[b], 0, SEQ_LEN), 1), :]
        flat[pl.ds(BATCH + b, 1), 0:HEAD_DIM] = tab[pl.ds(jnp.clip(lens[b] - 1, 0, SEQ_LEN), 1), :]
    c16, s16 = spread(flat[:, 0:HEAD_DIM])
    kself[...] = jnp.zeros_like(kself)
    vself[...] = jnp.zeros_like(vself)
    for h in range(2):
        lanes = slice(h * HEAD_DIM, (h + 1) * HEAD_DIM)
        qh = rotate(q16[:, lanes], c16, s16).astype(BF).astype(F32)
        kh = rotate(k16[:, lanes], c16, s16)[:BATCH].astype(BF).astype(F32)
        vh = v16[:BATCH, lanes].astype(BF).astype(F32)
        for g in range(2):
            qall[0, :, 2 * g + h, :] = qh[g * BATCH:(g + 1) * BATCH]
        kself[:, h, :] = kh
        vself[:, h, :] = vh
        tmp[pl.ds(h, BATCH, stride=2), :] = kh
        tmp[pl.ds(2 * BATCH + h, BATCH, stride=2), :] = vh
    new_out[0] = tmp[0:2 * BATCH, :].astype(BF)
    new_out[1] = tmp[2 * BATCH:4 * BATCH, :].astype(BF)
    low = lax.broadcasted_iota(jnp.int32, (4, HEAD_DIM), 1) < HALF
    part[:, 0] = jnp.zeros((4, BATCH, 4, HEAD_DIM), F32)
    part[:, 1] = jnp.broadcast_to(jnp.where(low, NEG_BIG, 0.0), (4, BATCH, 4, HEAD_DIM))
    q_copy = [remote(qall.at[0], qall.at[d], q_s.at[d - 1], q_r.at[d - 1], (rep, near[d])) for d in (1, 2, 3)]
    for c in q_copy:
        c.start()

    w_z.wait_recv()
    w_zs.start()
    w_zs.wait_recv()
    own_x_phase(znb, 2)
    own_x_phase(znb, 3)
    for c in q_copy:
        c.wait_recv()

    lane = lax.broadcasted_iota(jnp.int32, (4, ROWS), 1)
    same_head = lane % 2 == lax.broadcasted_iota(jnp.int32, (4, ROWS), 0) % 2

    def attend(s, b):
        blk = me if s == 0 else ynb
        seen = same_head & (blk * SEQ_LOC + lane // 2 < lens[b])
        for o in range(4):
            sc = lax.dot_general(qall[o, b].astype(BF), stage[s, b, o, 0], (((1,), (1,)), ((), ())), preferred_element_type=F32) * SCALE
            sc = jnp.where(seen, sc, NEG_BIG)
            old = part[o, 1, b]
            m_old, l_old = old[:, 0:1], old[:, HALF:HALF + 1]
            m_new = jnp.maximum(m_old, jnp.max(sc, axis=-1, keepdims=True))
            p = jnp.where(seen, jnp.exp(sc - m_new), 0.0)
            fade = jnp.exp(m_old - m_new)
            l_new = l_old * fade + jnp.sum(p, axis=-1, keepdims=True)
            part[o, 0, b] = part[o, 0, b] * fade + jnp.dot(p.astype(BF), stage[s, b, o, 1], preferred_element_type=F32)
            part[o, 1, b] = jnp.where(low, m_new, l_new)

    waiting = [(b, kv, o) for b in range(5, BATCH) for kv in range(2) for o in (2, 3)]

    def leave(b, kv, o):
        out_copy(1, b, o, kv).start()

    @pl.loop(0, BATCH)
    def _(b):
        attend(0, b)
        y_copy(b).wait_recv()

        @pl.when(b == BATCH - 1)
        def _():
            leave(*waiting[0])
        xrecv[b] = norm_rows(xrecv[b].astype(F32), gain_a[...])

        @pl.loop(0, 2)
        def _(kv):
            for o in (2, 3):
                project(xrecv, 1, b, o, kv)

                @pl.when((b < 5) & (kv == 1))
                def _():
                    chunk_kv(b, o).start()

            for o in (1, 0):
                project(xrecv, 1, b, o, kv)
                out_copy(1, b, o, kv).start()

        attend(1, b)

    p_copy = [remote(part.at[d], precv.at[d - 1], p_s.at[d - 1], p_r.at[d - 1], (rep, near[d])) for d in (1, 2, 3)]
    for c in p_copy:
        c.start()
    for job in waiting[1:3]:
        leave(*job)
    for load in loads[4:]:
        load.wait()
    first = lax.broadcasted_iota(jnp.int32, (BATCH, 4, 1), 1) < 2
    s_self = jnp.where(first, jnp.sum(qall[0] * kself[...], axis=-1, keepdims=True) * SCALE, NEG_BIG)
    for c in p_copy:
        c.wait_recv()
    accs = [part[0, 0]] + [precv[i, 0] for i in range(3)]
    stats = [part[0, 1]] + [precv[i, 1] for i in range(3)]
    tops = [st[:, :, 0:1] for st in stats]
    top = s_self
    for t in tops:
        top = jnp.maximum(top, t)
    e_self = jnp.where(first, jnp.exp(s_self - top), 0.0)
    den = e_self
    num = e_self * vself[...]
    for t, st, ac in zip(tops, stats, accs):
        e = jnp.exp(t - top)
        den = den + e * st[:, :, HALF:HALF + 1]
        num = num + e * ac
    attn[...] = num / den
    for g in range(2):
        for h in range(2):
            flat[g * BATCH:(g + 1) * BATCH, h * HEAD_DIM:(h + 1) * HEAD_DIM] = attn[:, 2 * g + h, :]

    def reduce_columns(i, base, jobs):
        sends = [remote(psend.at[i, near[d]], rrecv.at[i, d - 1], r_s.at[i, d - 1], r_r.at[i, d - 1], (rep, near[d])) for d in range(1, 8)]
        for c in sends:
            c.start()
        for job in jobs[0]:
            leave(*job)
        total = psend[i, me]
        for d in range(1, 8):
            sends[d - 1].wait_recv()
            total = total + rrecv[i, d - 1]
        hid[i, me] = (base + total).astype(BF)
        gets = [remote(hid.at[i, me], hid.at[i, me], a_s.at[i, d - 1], a_r.at[i, d - 1], (rep, near[d])) for d in range(1, 8)]
        for c in gets:
            c.start()
        for job in jobs[1]:
            leave(*job)
        for d in range(1, 8):
            remote(hid.at[i, near[d]], hid.at[i, near[d]], a_s.at[i, d - 1], a_r.at[i, d - 1], (rep, near[d])).wait_recv()
        return sends + gets

    a16 = flat[...].astype(BF)
    for j in range(8):
        psend[0, j] = jnp.dot(a16, wob[:, j * SHARD:(j + 1) * SHARD], preferred_element_type=F32)
    mine = pl.ds(pl.multiple_of(me * SHARD, SHARD), SHARD)
    done = reduce_columns(0, rows[:, mine], (waiting[3:5], waiting[5:8]))

    sq = jnp.zeros((2 * BATCH, 1), F32)
    for j in range(8):
        hj = hid[0, j].astype(F32)
        sq = sq + jnp.sum(hj * hj, axis=-1, keepdims=True)
    inv = lax.rsqrt(sq / D_MODEL + 1e-5)
    for j in range(8):
        cols = slice(j * SHARD, (j + 1) * SHARD)
        norm2[:, cols] = (hid[0, j].astype(F32) * inv * gain_m[:, cols].astype(F32)).astype(BF)
    n2 = norm2[...]
    gate = jnp.dot(n2, wgb[...], preferred_element_type=F32)
    up = jnp.dot(n2, wub[...], preferred_element_type=F32)
    mid = (gate * jax.nn.sigmoid(gate) * up).astype(BF)
    for j in range(8):
        psend[1, j] = jnp.dot(mid, wdb[:, j * SHARD:(j + 1) * SHARD], preferred_element_type=F32)
    done += reduce_columns(1, hid[0, me].astype(F32), (waiting[8:10], waiting[10:12]))
    for j in range(8):
        cols = slice(j * SHARD, (j + 1) * SHARD)
        dec_out[:, cols] = hid[1, j][:BATCH]
        last_out[:, cols] = hid[1, j][BATCH:]

    for c in [w_x, w_s, w_z, w_xs, w_zs] + l_copy + q_copy + p_copy + done:
        c.wait_send()

    @pl.loop(0, BATCH)
    def _(b):
        y_copy(b).wait_send()
        for kv in range(2):
            for s in range(2):
                for o in (0, 1):
                    out_copy(s, b, o, kv).wait()

    for o in (2, 3):
        @pl.loop(0, BATCH, step=2)
        def _(b):
            for kv in range(2):
                own_two(b, o, kv).wait()

        @pl.loop(0, 5)
        def _(b):
            chunk_kv(b, o).wait()

    for b, kv, o in waiting:
        out_copy(1, b, o, kv).wait()


def layer(lens, prompt, new_tok, gain_a, gain_m, table, wq, wk, wv, wo, wg, wu, wd):
    vmem = pl.BlockSpec(memory_space=pltpu.VMEM)
    anym = pl.BlockSpec(memory_space=pl.ANY)
    dma = pltpu.SemaphoreType.DMA
    v = pltpu.VMEM
    return pl.pallas_call(
        layer_kernel,
        out_shape=(
            jax.ShapeDtypeStruct((2, BATCH, 8 * ROWS, HEAD_DIM), BF),
            jax.ShapeDtypeStruct((2, 2 * BATCH, HEAD_DIM), BF),
            jax.ShapeDtypeStruct((BATCH, D_MODEL), BF),
            jax.ShapeDtypeStruct((BATCH, D_MODEL), BF),
        ),
        in_specs=[pl.BlockSpec(memory_space=pltpu.SMEM), anym, vmem, vmem, vmem] + [anym] * 8,
        out_specs=(anym, vmem, vmem, vmem),
        scratch_shapes=[
            v((BATCH, SEQ_LOC, D_MODEL), BF), v((BATCH, SEQ_LOC, D_MODEL), BF), v((4, 2, D_MODEL, SHARD), BF),
            v((D_MODEL, SHARD), BF), v((SHARD, D_MODEL), BF), v((D_MODEL, FF_LOC), BF), v((D_MODEL, FF_LOC), BF), v((FF_LOC, D_MODEL), BF),
            v((TAB_ROWS, HEAD_DIM), F32), v((ROWS, HEAD_DIM), F32), v((2, BATCH, 4, 2, ROWS, HEAD_DIM), BF),
            v((BATCH, D_MODEL), F32), v((3, BATCH, D_MODEL), BF), v((3, BATCH, D_MODEL), BF), v((2 * BATCH, D_MODEL), F32),
            v((4, BATCH, 4, HEAD_DIM), F32), v((4, 2, BATCH, 4, HEAD_DIM), F32), v((3, 2, BATCH, 4, HEAD_DIM), F32),
            v((BATCH, 4, HEAD_DIM), F32), v((BATCH, 4, HEAD_DIM), F32), v((BATCH, 4, HEAD_DIM), F32), v((2 * BATCH, SHARD), F32),
            v((2, 8, 2 * BATCH, SHARD), F32), v((2, 7, 2 * BATCH, SHARD), F32), v((2, 8, 2 * BATCH, SHARD), BF), v((2 * BATCH, D_MODEL), BF),
            dma((8,)), dma((BATCH,)), dma((BATCH,)), dma((BATCH,)), dma((5,)), dma((5,)),
            dma((3, 2, BATCH, 2)), dma((3, 2, BATCH, 2)), dma((2, BATCH, 2)),
            dma((3,)), dma((3,)), dma((3,)), dma((3,)), dma((3,)), dma((3,)),
            dma((2, 7)), dma((2, 7)), dma((2, 7)), dma((2, 7)),
        ],
        compiler_params=pltpu.CompilerParams(collective_id=0, has_side_effects=True, vmem_limit_bytes=62 * 1024 * 1024),
        cost_estimate=pl.CostEstimate(flops=26_000_000_000, bytes_accessed=60_000_000, transcendentals=0),
        name='layer',
    )(lens, prompt, new_tok, gain_a, gain_m, table, wq, wk, wv, wo, wg, wu, wd)


def cache_kernel(kv, new, dec, last, key_out, val_out, dec_out, last_out, buf, row, load, store, row_sem):
    outs = (key_out, val_out)
    ins = [[pltpu.make_async_copy(kv.at[i, b], buf.at[i, b], load.at[i, b]) for b in range(BATCH)] for i in range(2)]
    rows_in = pltpu.make_async_copy(new, row, row_sem.at[0])
    rows_in.start()
    for i in range(2):
        for b in range(BATCH):
            ins[i][b].start()
    dec_out[...] = dec[...]
    last_out[...] = last[...]
    rows_in.wait()
    puts = [pltpu.make_async_copy(row.at[i], outs[i].at[0, :, pl.ds(SEQ_LEN, 1)], row_sem.at[1 + i]) for i in range(2)]
    for c in puts:
        c.start()
    for i in range(2):
        for b in range(BATCH):
            ins[i][b].wait()
            puts.append(pltpu.make_async_copy(buf.at[i, b], outs[i].at[0, b, pl.ds(0, SEQ_LEN)], store.at[i, b]))
            puts[-1].start()
    for c in puts:
        c.wait()


def caches(kv, new, dec, last):
    anym = pl.BlockSpec(memory_space=pl.ANY)
    dma = pltpu.SemaphoreType.DMA
    vmem = pl.BlockSpec(memory_space=pltpu.VMEM)
    shape = jax.ShapeDtypeStruct((1, BATCH, SEQ_LEN + 1, 2, HEAD_DIM), BF)
    row = jax.ShapeDtypeStruct((BATCH, D_MODEL), BF)
    return pl.pallas_call(
        cache_kernel,
        out_shape=(shape, shape, row, row),
        in_specs=[anym, anym, vmem, vmem],
        out_specs=(anym, anym, vmem, vmem),
        scratch_shapes=[
            pltpu.VMEM((2, BATCH, SEQ_LEN, 2, HEAD_DIM), BF), pltpu.VMEM((2, BATCH, 1, 2, HEAD_DIM), BF),
            dma((2, BATCH)), dma((2, BATCH)), dma((3,)),
        ],
        compiler_params=pltpu.CompilerParams(vmem_limit_bytes=62 * 1024 * 1024),
        cost_estimate=pl.CostEstimate(flops=0, bytes_accessed=50_000_000, transcendentals=0),
        name='caches',
    )(kv, new, dec, last)


def solution(mesh):
    seq_spec = P('replica', 'model', None)
    col_spec = P(None, None, 'model')
    row_spec = P(None, 'model', None)
    gain_spec = P(None, None)
    tok_spec = P('replica', None)
    cache_spec = P(None, 'replica', None, 'model', None)
    in_specs = (seq_spec, P('replica'), tok_spec, gain_spec, col_spec, col_spec, col_spec, row_spec, gain_spec, col_spec, col_spec, row_spec)
    out_specs = (tok_spec, tok_spec, cache_spec, cache_spec)
    table = rope_table()

    def per_device(prompt, lengths, new_tok, norm_attn, w_q, w_k, w_v, w_o, norm_mlp, w_gate, w_up, w_down):
        kv, new, dec, last = layer(lengths, prompt, new_tok, norm_attn, norm_mlp, jnp.asarray(table), w_q, w_k, w_v, w_o, w_gate, w_up, w_down)
        keys, vals, dec, last = caches(kv.reshape(2, BATCH, SEQ_LEN, 2, HEAD_DIM), new.reshape(2, BATCH, 1, 2, HEAD_DIM), dec, last)
        return dec, last, keys, vals

    return jax.shard_map(per_device, mesh=mesh, in_specs=in_specs, out_specs=out_specs, check_vma=False)
```

```python
import jax
import jax.numpy as jnp
import numpy as np
from jax import lax
from jax.experimental import pallas as pl
from jax.experimental.pallas import tpu as pltpu
from jax.sharding import PartitionSpec as P

HEAD_DIM = 128
HALF = HEAD_DIM // 2
NEG_BIG = -1e30
BATCH = 8
SEQ_LOC = 192
SEQ_LEN = 1536
D_MODEL = 2048
SHARD = 256
FF_LOC = 1024
ROWS = 2 * SEQ_LOC
TAB_ROWS = SEQ_LEN + 8
MESH = pl.DeviceIdType.MESH
BF = jnp.bfloat16
F32 = jnp.float32
SCALE = HEAD_DIM ** -0.5


def rope_table():
    inv_freq = np.float32(10000.0) ** (np.float32(-2.0) * np.arange(HALF, dtype=np.float32) / np.float32(HEAD_DIM))
    angles = np.arange(TAB_ROWS, dtype=np.float32)[:, None] * inv_freq.astype(np.float32)
    return np.concatenate([np.cos(angles), np.sin(angles)], axis=-1).astype(np.float32)


def norm_rows(x, gain):
    inv = lax.rsqrt(jnp.mean(x * x, axis=-1, keepdims=True) + 1e-5)
    return (x * inv * gain.astype(F32)).astype(BF)


def spread(tab):
    swapped = pltpu.roll(tab, HALF, 1)
    low = lax.broadcasted_iota(jnp.int32, tab.shape, 1) < HALF
    return jnp.where(low, tab, swapped), jnp.where(low, -swapped, tab)


def rotate(a, c, s):
    return a * c + pltpu.roll(a, HALF, 1) * s


def layer_kernel(lens, prompt, new_tok, gain_a, gain_m, table, wq, wk, wv, wo, wg, wu, wd,
                 kv_out, new_out, dec_out, last_out,
                 xbuf, xrecv, wbuf, wqb, wob, wgb, wub, wdb, tab, tmp, stage,
                 lastf, lsend, lrecv, rows, qall, part, precv, kself, vself, attn, flat,
                 psend, rrecv, hid, norm2,
                 lsem, xsem, ysend, yrecv, wsend, wrecv, osend, orecv, ssem,
                 l_s, l_r, q_s, q_r, p_s, p_r, r_s, r_r, a_s, a_r):
    rep = lax.axis_index('replica')
    me = lax.axis_index('model')
    core = lax.rem(me, 2)
    xpos = lax.rem(me // 2, 2)
    ypos = me // 4
    flips = (1 - 2 * core, 2 - 4 * xpos, 4 - 8 * ypos)
    near = [me + sum(f for i, f in enumerate(flips) if d >> i & 1) for d in range(8)]
    sib, xnb, xsb, ynb = near[1], near[2], near[3], near[4]
    znb = 1 - rep

    barrier = pltpu.get_barrier_semaphore()
    for peer in [(rep, near[d]) for d in range(1, 8)] + [(znb, me)]:
        pl.semaphore_signal(barrier, inc=1, device_id=peer, device_id_type=MESH)
    pl.semaphore_wait(barrier, 8)

    def remote(src, dst, send, recv, peer):
        return pltpu.make_async_remote_copy(src_ref=src, dst_ref=dst, send_sem=send, recv_sem=recv, device_id=peer, device_id_type=MESH)

    def y_copy(b):
        return remote(prompt.at[b], xrecv.at[b], ysend.at[b], yrecv.at[b], (rep, ynb))

    def x_load(b):
        return pltpu.make_async_copy(prompt.at[b], xbuf.at[b], xsem.at[b])

    loads = [pltpu.make_async_copy(a, b, lsem.at[i]) for i, (a, b) in enumerate((
        (wk.at[0], wbuf.at[0, 0]), (wv.at[0], wbuf.at[0, 1]), (table, tab), (wq.at[0], wqb), (wo.at[0], wob),
        (wg.at[0], wgb), (wu.at[0], wub), (wd.at[0], wdb)))]
    for i, w in enumerate((wk, wv)):
        @pl.when(rep == i)
        def _():
            remote(w.at[0], wbuf.at[2, rep], wsend.at[0], wrecv.at[0], (rep, xnb)).start()

    y_copy(0).start()
    loads[0].start()
    loads[1].start()

    @pl.loop(0, BATCH)
    def _(b):
        x_load(b).start()

    for load in loads[2:]:
        load.start()
    w_x = remote(wbuf.at[0, rep], wbuf.at[2, rep], wsend.at[0], wrecv.at[0], (rep, xnb))
    w_s = remote(wbuf.at[0], wbuf.at[1], wsend.at[1], wrecv.at[1], (rep, sib))
    w_z = remote(wbuf.at[2, rep], wbuf.at[2, rep], wsend.at[2], wrecv.at[2], (znb, me))
    w_xs = remote(wbuf.at[2, rep], wbuf.at[3, rep], wsend.at[3], wrecv.at[3], (rep, sib))
    w_zs = remote(wbuf.at[2, znb], wbuf.at[3, znb], wsend.at[4], wrecv.at[4], (rep, sib))
    loads[0].wait()
    loads[1].wait()
    w_s.start()

    def out_copy(s, b, o, kv):
        blk = me if s == 0 else ynb
        dst = kv_out.at[kv, b, pl.ds(pl.multiple_of(blk * ROWS, ROWS), ROWS), :]
        src = stage.at[s, b, o, kv]
        if o == 0:
            return pltpu.make_async_copy(src, dst, ssem.at[s, b, kv])
        return remote(src, dst, osend.at[o - 1, s, b, kv], orecv.at[o - 1, s, b, kv], (rep, near[o]))

    def own_two(b, o, kv):
        dst = kv_out.at[kv, pl.ds(b, 2), pl.ds(pl.multiple_of(me * ROWS, ROWS), ROWS), :]
        return remote(stage.at[0, pl.ds(b, 2), o, kv], dst, osend.at[o - 1, 0, b, kv], orecv.at[o - 1, 0, b, kv], (rep, near[o]))

    def chunk_kv(b, o):
        dst = kv_out.at[:, b, pl.ds(pl.multiple_of(ynb * ROWS, ROWS), ROWS), :]
        return remote(stage.at[1, b, o], dst, osend.at[o - 1, 1, b, 0], orecv.at[o - 1, 1, b, 0], (rep, near[o]))

    def project(buf, s, b, o, kv):
        acc = jnp.dot(buf[b], wbuf[o, kv], preferred_element_type=F32)
        blk = me if s == 0 else ynb
        c, sn = spread(tab[pl.ds(pl.multiple_of(blk * SEQ_LOC, SEQ_LOC), SEQ_LOC), :])
        is_k = kv == 0
        c = jnp.where(is_k, c, 1.0)
        sn = jnp.where(is_k, sn, 0.0)
        for h in range(2):
            tmp[pl.ds(h, SEQ_LOC, stride=2), :] = rotate(acc[:, h * HEAD_DIM:(h + 1) * HEAD_DIM], c, sn)
        stage[s, b, o, kv] = tmp[...].astype(BF)

    @pl.loop(0, BATCH)
    def _(b):
        x_load(b).wait()
        x = xbuf[b].astype(F32)
        here = me * SEQ_LOC + lax.broadcasted_iota(jnp.int32, (SEQ_LOC, 1), 0) == lens[b] - 1
        lastf[pl.ds(b, 1), :] = jnp.sum(jnp.where(here, x, 0.0), axis=0, keepdims=True)
        xbuf[b] = norm_rows(x, gain_a[...])

    l_copy = [remote(lsend.at[i], lrecv.at[i], l_s.at[i], l_r.at[i], (rep, near[d])) for i, d in enumerate((4, 1, 2))]
    lsend[0] = lastf[...].astype(BF)
    loads[2].wait()
    l_copy[0].start()

    @pl.loop(1, BATCH)
    def _(b):
        y_copy(b).start()

    @pl.loop(0, BATCH)
    def _(b):
        @pl.loop(0, 2)
        def _(kv):
            project(xbuf, 0, b, 0, kv)
            out_copy(0, b, 0, kv).start()

    def join_last(i):
        l_copy[i].wait_recv()
        return (lsend[i].astype(F32) + lrecv[i].astype(F32)).astype(BF)

    lsend[1] = join_last(0)
    w_s.wait_recv()
    l_copy[1].start()

    @pl.loop(0, BATCH)
    def _(b):
        @pl.loop(0, 2)
        def _(kv):
            project(xbuf, 0, b, 1, kv)
            out_copy(0, b, 1, kv).start()

    lsend[2] = join_last(1)

    w_x.wait_recv()
    w_z.start()
    w_xs.start()
    l_copy[2].start()

    def own_x_phase(kv, o):
        @pl.loop(0, BATCH, step=2)
        def _(b):
            project(xbuf, 0, b, o, kv)
            project(xbuf, 0, b + 1, o, kv)
            own_two(b, o, kv).start()

    own_x_phase(rep, 2)
    w_xs.wait_recv()
    own_x_phase(rep, 3)

    rows[0:BATCH, :] = new_tok[...].astype(F32)
    rows[BATCH:2 * BATCH, :] = join_last(2).astype(F32)
    loads[3].wait()
    n16 = norm_rows(rows[...], gain_a[...])
    q16 = jnp.dot(n16, wqb[...], preferred_element_type=F32)
    k16 = jnp.dot(n16, wbuf[0, 0], preferred_element_type=F32)
    v16 = jnp.dot(n16, wbuf[0, 1], preferred_element_type=F32)
    for b in range(BATCH):
        flat[pl.ds(b, 1), 0:HEAD_DIM] = tab[pl.ds(jnp.clip(lens[b], 0, SEQ_LEN), 1), :]
        flat[pl.ds(BATCH + b, 1), 0:HEAD_DIM] = tab[pl.ds(jnp.clip(lens[b] - 1, 0, SEQ_LEN), 1), :]
    c16, s16 = spread(flat[:, 0:HEAD_DIM])
    kself[...] = jnp.zeros_like(kself)
    vself[...] = jnp.zeros_like(vself)
    for h in range(2):
        lanes = slice(h * HEAD_DIM, (h + 1) * HEAD_DIM)
        qh = rotate(q16[:, lanes], c16, s16).astype(BF).astype(F32)
        kh = rotate(k16[:, lanes], c16, s16)[:BATCH].astype(BF).astype(F32)
        vh = v16[:BATCH, lanes].astype(BF).astype(F32)
        for g in range(2):
            qall[0, :, 2 * g + h, :] = qh[g * BATCH:(g + 1) * BATCH]
        kself[:, h, :] = kh
        vself[:, h, :] = vh
        tmp[pl.ds(h, BATCH, stride=2), :] = kh
        tmp[pl.ds(2 * BATCH + h, BATCH, stride=2), :] = vh
    new_out[0] = tmp[0:2 * BATCH, :].astype(BF)
    new_out[1] = tmp[2 * BATCH:4 * BATCH, :].astype(BF)
    low = lax.broadcasted_iota(jnp.int32, (4, HEAD_DIM), 1) < HALF
    part[:, 0] = jnp.zeros((4, BATCH, 4, HEAD_DIM), F32)
    part[:, 1] = jnp.broadcast_to(jnp.where(low, NEG_BIG, 0.0), (4, BATCH, 4, HEAD_DIM))
    q_copy = [remote(qall.at[0], qall.at[d], q_s.at[d - 1], q_r.at[d - 1], (rep, near[d])) for d in (1, 2, 3)]
    for c in q_copy:
        c.start()

    w_z.wait_recv()
    w_zs.start()
    w_zs.wait_recv()
    own_x_phase(znb, 2)
    own_x_phase(znb, 3)
    for c in q_copy:
        c.wait_recv()

    lane = lax.broadcasted_iota(jnp.int32, (4, ROWS), 1)
    same_head = lane % 2 == lax.broadcasted_iota(jnp.int32, (4, ROWS), 0) % 2

    def attend(s, b):
        blk = me if s == 0 else ynb
        seen = same_head & (blk * SEQ_LOC + lane // 2 < lens[b])
        four = range(4)
        old = [part[o, 1, b] for o in four]
        acc = [part[o, 0, b] for o in four]
        sc = [lax.dot_general(qall[o, b].astype(BF), stage[s, b, o, 0], (((1,), (1,)), ((), ())), preferred_element_type=F32) for o in four]
        sc = [jnp.where(seen, x * SCALE, NEG_BIG) for x in sc]
        top = [jnp.maximum(old[o][:, 0:1], jnp.max(sc[o], axis=-1, keepdims=True)) for o in four]
        p = [jnp.where(seen, jnp.exp(sc[o] - top[o]), 0.0) for o in four]
        fade = [jnp.exp(old[o][:, 0:1] - top[o]) for o in four]
        den = [old[o][:, HALF:HALF + 1] * fade[o] + jnp.sum(p[o], axis=-1, keepdims=True) for o in four]
        add = [jnp.dot(p[o].astype(BF), stage[s, b, o, 1], preferred_element_type=F32) for o in four]
        for o in four:
            part[o, 0, b] = acc[o] * fade[o] + add[o]
            part[o, 1, b] = jnp.where(low, top[o], den[o])

    waiting = [(b, kv, o) for b in range(5, BATCH) for kv in range(2) for o in (2, 3)]

    def leave(b, kv, o):
        out_copy(1, b, o, kv).start()

    @pl.loop(0, BATCH)
    def _(b):
        attend(0, b)
        y_copy(b).wait_recv()

        @pl.when(b == BATCH - 1)
        def _():
            leave(*waiting[0])
            leave(*waiting[1])
        xrecv[b] = norm_rows(xrecv[b].astype(F32), gain_a[...])

        @pl.loop(0, 2)
        def _(kv):
            for o in (2, 3):
                project(xrecv, 1, b, o, kv)

                @pl.when((b < 5) & (kv == 1))
                def _():
                    chunk_kv(b, o).start()

            for o in (1, 0):
                project(xrecv, 1, b, o, kv)
                out_copy(1, b, o, kv).start()

        attend(1, b)

    p_copy = [remote(part.at[d], precv.at[d - 1], p_s.at[d - 1], p_r.at[d - 1], (rep, near[d])) for d in (1, 2, 3)]
    for c in p_copy:
        c.start()
    for job in waiting[2:4]:
        leave(*job)
    for load in loads[4:]:
        load.wait()
    first = lax.broadcasted_iota(jnp.int32, (BATCH, 4, 1), 1) < 2
    s_self = jnp.where(first, jnp.sum(qall[0] * kself[...], axis=-1, keepdims=True) * SCALE, NEG_BIG)
    for c in p_copy:
        c.wait_recv()
    accs = [part[0, 0]] + [precv[i, 0] for i in range(3)]
    stats = [part[0, 1]] + [precv[i, 1] for i in range(3)]
    tops = [st[:, :, 0:1] for st in stats]
    top = s_self
    for t in tops:
        top = jnp.maximum(top, t)
    e_self = jnp.where(first, jnp.exp(s_self - top), 0.0)
    den = e_self
    num = e_self * vself[...]
    for t, st, ac in zip(tops, stats, accs):
        e = jnp.exp(t - top)
        den = den + e * st[:, :, HALF:HALF + 1]
        num = num + e * ac
    attn[...] = num / den
    for g in range(2):
        for h in range(2):
            flat[g * BATCH:(g + 1) * BATCH, h * HEAD_DIM:(h + 1) * HEAD_DIM] = attn[:, 2 * g + h, :]

    def reduce_columns(i, base, jobs):
        sends = [remote(psend.at[i, near[d]], rrecv.at[i, d - 1], r_s.at[i, d - 1], r_r.at[i, d - 1], (rep, near[d])) for d in range(1, 8)]
        for c in sends:
            c.start()
        for job in jobs[0]:
            leave(*job)
        total = psend[i, me]
        for d in range(1, 8):
            sends[d - 1].wait_recv()
            total = total + rrecv[i, d - 1]
        hid[i, me] = (base + total).astype(BF)
        gets = [remote(hid.at[i, me], hid.at[i, me], a_s.at[i, d - 1], a_r.at[i, d - 1], (rep, near[d])) for d in range(1, 8)]
        for c in gets:
            c.start()
        for job in jobs[1]:
            leave(*job)
        for d in range(1, 8):
            remote(hid.at[i, near[d]], hid.at[i, near[d]], a_s.at[i, d - 1], a_r.at[i, d - 1], (rep, near[d])).wait_recv()
        return sends + gets

    a16 = flat[...].astype(BF)
    for j in range(8):
        psend[0, j] = jnp.dot(a16, wob[:, j * SHARD:(j + 1) * SHARD], preferred_element_type=F32)
    mine = pl.ds(pl.multiple_of(me * SHARD, SHARD), SHARD)
    done = reduce_columns(0, rows[:, mine], (waiting[4:6], waiting[6:8]))

    sq = jnp.zeros((2 * BATCH, 1), F32)
    for j in range(8):
        hj = hid[0, j].astype(F32)
        sq = sq + jnp.sum(hj * hj, axis=-1, keepdims=True)
    inv = lax.rsqrt(sq / D_MODEL + 1e-5)
    for j in range(8):
        cols = slice(j * SHARD, (j + 1) * SHARD)
        norm2[:, cols] = (hid[0, j].astype(F32) * inv * gain_m[:, cols].astype(F32)).astype(BF)
    n2 = norm2[...]
    gate = jnp.dot(n2, wgb[...], preferred_element_type=F32)
    up = jnp.dot(n2, wub[...], preferred_element_type=F32)
    mid = (gate * jax.nn.sigmoid(gate) * up).astype(BF)
    for j in range(8):
        psend[1, j] = jnp.dot(mid, wdb[:, j * SHARD:(j + 1) * SHARD], preferred_element_type=F32)
    done += reduce_columns(1, hid[0, me].astype(F32), (waiting[8:10], waiting[10:12]))
    for j in range(8):
        cols = slice(j * SHARD, (j + 1) * SHARD)
        dec_out[:, cols] = hid[1, j][:BATCH]
        last_out[:, cols] = hid[1, j][BATCH:]

    for c in [w_x, w_s, w_z, w_xs, w_zs] + l_copy + q_copy + p_copy + done:
        c.wait_send()

    @pl.loop(0, BATCH)
    def _(b):
        y_copy(b).wait_send()
        for kv in range(2):
            for s in range(2):
                for o in (0, 1):
                    out_copy(s, b, o, kv).wait()

    for o in (2, 3):
        @pl.loop(0, BATCH, step=2)
        def _(b):
            for kv in range(2):
                own_two(b, o, kv).wait()

        @pl.loop(0, 5)
        def _(b):
            chunk_kv(b, o).wait()

    for b, kv, o in waiting:
        out_copy(1, b, o, kv).wait()


def layer(lens, prompt, new_tok, gain_a, gain_m, table, wq, wk, wv, wo, wg, wu, wd):
    vmem = pl.BlockSpec(memory_space=pltpu.VMEM)
    anym = pl.BlockSpec(memory_space=pl.ANY)
    dma = pltpu.SemaphoreType.DMA
    v = pltpu.VMEM
    return pl.pallas_call(
        layer_kernel,
        out_shape=(
            jax.ShapeDtypeStruct((2, BATCH, 8 * ROWS, HEAD_DIM), BF),
            jax.ShapeDtypeStruct((2, 2 * BATCH, HEAD_DIM), BF),
            jax.ShapeDtypeStruct((BATCH, D_MODEL), BF),
            jax.ShapeDtypeStruct((BATCH, D_MODEL), BF),
        ),
        in_specs=[pl.BlockSpec(memory_space=pltpu.SMEM), anym, vmem, vmem, vmem] + [anym] * 8,
        out_specs=(anym, vmem, vmem, vmem),
        scratch_shapes=[
            v((BATCH, SEQ_LOC, D_MODEL), BF), v((BATCH, SEQ_LOC, D_MODEL), BF), v((4, 2, D_MODEL, SHARD), BF),
            v((D_MODEL, SHARD), BF), v((SHARD, D_MODEL), BF), v((D_MODEL, FF_LOC), BF), v((D_MODEL, FF_LOC), BF), v((FF_LOC, D_MODEL), BF),
            v((TAB_ROWS, HEAD_DIM), F32), v((ROWS, HEAD_DIM), F32), v((2, BATCH, 4, 2, ROWS, HEAD_DIM), BF),
            v((BATCH, D_MODEL), F32), v((3, BATCH, D_MODEL), BF), v((3, BATCH, D_MODEL), BF), v((2 * BATCH, D_MODEL), F32),
            v((4, BATCH, 4, HEAD_DIM), F32), v((4, 2, BATCH, 4, HEAD_DIM), F32), v((3, 2, BATCH, 4, HEAD_DIM), F32),
            v((BATCH, 4, HEAD_DIM), F32), v((BATCH, 4, HEAD_DIM), F32), v((BATCH, 4, HEAD_DIM), F32), v((2 * BATCH, SHARD), F32),
            v((2, 8, 2 * BATCH, SHARD), F32), v((2, 7, 2 * BATCH, SHARD), F32), v((2, 8, 2 * BATCH, SHARD), BF), v((2 * BATCH, D_MODEL), BF),
            dma((8,)), dma((BATCH,)), dma((BATCH,)), dma((BATCH,)), dma((5,)), dma((5,)),
            dma((3, 2, BATCH, 2)), dma((3, 2, BATCH, 2)), dma((2, BATCH, 2)),
            dma((3,)), dma((3,)), dma((3,)), dma((3,)), dma((3,)), dma((3,)),
            dma((2, 7)), dma((2, 7)), dma((2, 7)), dma((2, 7)),
        ],
        compiler_params=pltpu.CompilerParams(collective_id=0, has_side_effects=True, vmem_limit_bytes=62 * 1024 * 1024),
        cost_estimate=pl.CostEstimate(flops=26_000_000_000, bytes_accessed=60_000_000, transcendentals=0),
        name='layer',
    )(lens, prompt, new_tok, gain_a, gain_m, table, wq, wk, wv, wo, wg, wu, wd)


def cache_kernel(kv, new, dec, last, key_out, val_out, dec_out, last_out, buf, row, load, store, row_sem):
    outs = (key_out, val_out)
    ins = [[pltpu.make_async_copy(kv.at[i, b], buf.at[i, b], load.at[i, b]) for b in range(BATCH)] for i in range(2)]
    rows_in = pltpu.make_async_copy(new, row, row_sem.at[0])
    rows_in.start()
    for i in range(2):
        for b in range(BATCH):
            ins[i][b].start()
    dec_out[...] = dec[...]
    last_out[...] = last[...]
    rows_in.wait()
    puts = [pltpu.make_async_copy(row.at[i], outs[i].at[0, :, pl.ds(SEQ_LEN, 1)], row_sem.at[1 + i]) for i in range(2)]
    for c in puts:
        c.start()
    for i in range(2):
        for b in range(BATCH):
            ins[i][b].wait()
            puts.append(pltpu.make_async_copy(buf.at[i, b], outs[i].at[0, b, pl.ds(0, SEQ_LEN)], store.at[i, b]))
            puts[-1].start()
    for c in puts:
        c.wait()


def caches(kv, new, dec, last):
    anym = pl.BlockSpec(memory_space=pl.ANY)
    dma = pltpu.SemaphoreType.DMA
    vmem = pl.BlockSpec(memory_space=pltpu.VMEM)
    shape = jax.ShapeDtypeStruct((1, BATCH, SEQ_LEN + 1, 2, HEAD_DIM), BF)
    row = jax.ShapeDtypeStruct((BATCH, D_MODEL), BF)
    return pl.pallas_call(
        cache_kernel,
        out_shape=(shape, shape, row, row),
        in_specs=[anym, anym, vmem, vmem],
        out_specs=(anym, anym, vmem, vmem),
        scratch_shapes=[
            pltpu.VMEM((2, BATCH, SEQ_LEN, 2, HEAD_DIM), BF), pltpu.VMEM((2, BATCH, 1, 2, HEAD_DIM), BF),
            dma((2, BATCH)), dma((2, BATCH)), dma((3,)),
        ],
        compiler_params=pltpu.CompilerParams(vmem_limit_bytes=62 * 1024 * 1024),
        cost_estimate=pl.CostEstimate(flops=0, bytes_accessed=50_000_000, transcendentals=0),
        name='caches',
    )(kv, new, dec, last)


def solution(mesh):
    seq_spec = P('replica', 'model', None)
    col_spec = P(None, None, 'model')
    row_spec = P(None, 'model', None)
    gain_spec = P(None, None)
    tok_spec = P('replica', None)
    cache_spec = P(None, 'replica', None, 'model', None)
    in_specs = (seq_spec, P('replica'), tok_spec, gain_spec, col_spec, col_spec, col_spec, row_spec, gain_spec, col_spec, col_spec, row_spec)
    out_specs = (tok_spec, tok_spec, cache_spec, cache_spec)
    table = rope_table()

    def per_device(prompt, lengths, new_tok, norm_attn, w_q, w_k, w_v, w_o, norm_mlp, w_gate, w_up, w_down):
        kv, new, dec, last = layer(lengths, prompt, new_tok, norm_attn, norm_mlp, jnp.asarray(table), w_q, w_k, w_v, w_o, w_gate, w_up, w_down)
        keys, vals, dec, last = caches(kv.reshape(2, BATCH, SEQ_LEN, 2, HEAD_DIM), new.reshape(2, BATCH, 1, 2, HEAD_DIM), dec, last)
        return dec, last, keys, vals

    return jax.shard_map(per_device, mesh=mesh, in_specs=in_specs, out_specs=out_specs, check_vma=False)
```

```python
import jax
import jax.numpy as jnp
import numpy as np
from jax import lax
from jax.experimental import pallas as pl
from jax.experimental.pallas import tpu as pltpu
from jax.sharding import PartitionSpec as P

HEAD_DIM = 128
HALF = HEAD_DIM // 2
NEG_BIG = -1e30
BATCH = 8
SEQ_LOC = 192
SEQ_LEN = 1536
D_MODEL = 2048
SHARD = 256
FF_LOC = 1024
ROWS = 2 * SEQ_LOC
TAB_ROWS = SEQ_LEN + 8
MESH = pl.DeviceIdType.MESH
BF = jnp.bfloat16
F32 = jnp.float32
SCALE = HEAD_DIM ** -0.5


def rope_table():
    inv_freq = np.float32(10000.0) ** (np.float32(-2.0) * np.arange(HALF, dtype=np.float32) / np.float32(HEAD_DIM))
    angles = np.arange(TAB_ROWS, dtype=np.float32)[:, None] * inv_freq.astype(np.float32)
    return np.concatenate([np.cos(angles), np.sin(angles)], axis=-1).astype(np.float32)


def norm_rows(x, gain):
    inv = lax.rsqrt(jnp.mean(x * x, axis=-1, keepdims=True) + 1e-5)
    return (x * inv * gain.astype(F32)).astype(BF)


def spread(tab):
    swapped = pltpu.roll(tab, HALF, 1)
    low = lax.broadcasted_iota(jnp.int32, tab.shape, 1) < HALF
    return jnp.where(low, tab, swapped), jnp.where(low, -swapped, tab)


def rotate(a, c, s):
    return a * c + pltpu.roll(a, HALF, 1) * s


def layer_kernel(lens, prompt, new_tok, gain_a, gain_m, table, wq, wk, wv, wo, wg, wu, wd,
                 kv_out, new_out, dec_out, last_out,
                 xbuf, xrecv, wbuf, wqb, wob, wgb, wub, wdb, tab, tmp, stage,
                 lastf, lsend, lrecv, rows, qall, part, precv, kself, vself, attn, flat,
                 psend, rrecv, hid, norm2,
                 lsem, xsem, ysend, yrecv, wsend, wrecv, osend, orecv,
                 l_s, l_r, q_s, q_r, p_s, p_r, r_s, r_r, a_s, a_r):
    rep = lax.axis_index('replica')
    me = lax.axis_index('model')
    core = lax.rem(me, 2)
    xpos = lax.rem(me // 2, 2)
    ypos = me // 4
    flips = (1 - 2 * core, 2 - 4 * xpos, 4 - 8 * ypos)
    near = [me + sum(f for i, f in enumerate(flips) if d >> i & 1) for d in range(8)]
    sib, xnb, xsb, ynb = near[1], near[2], near[3], near[4]
    znb = 1 - rep

    barrier = pltpu.get_barrier_semaphore()
    for peer in [(rep, near[d]) for d in range(1, 8)] + [(znb, me)]:
        pl.semaphore_signal(barrier, inc=1, device_id=peer, device_id_type=MESH)
    pl.semaphore_wait(barrier, 8)

    def remote(src, dst, send, recv, peer):
        return pltpu.make_async_remote_copy(src_ref=src, dst_ref=dst, send_sem=send, recv_sem=recv, device_id=peer, device_id_type=MESH)

    def y_copy(b):
        return remote(prompt.at[b], xrecv.at[b], ysend.at[b], yrecv.at[b], (rep, ynb))

    def x_load(b):
        return pltpu.make_async_copy(prompt.at[b], xbuf.at[b], xsem.at[b])

    loads = [pltpu.make_async_copy(a, b, lsem.at[i]) for i, (a, b) in enumerate((
        (wk.at[0], wbuf.at[0, 0]), (wv.at[0], wbuf.at[0, 1]), (table, tab), (wq.at[0], wqb), (wo.at[0], wob),
        (wg.at[0], wgb), (wu.at[0], wub), (wd.at[0], wdb)))]
    for i, w in enumerate((wk, wv)):
        @pl.when(rep == i)
        def _():
            remote(w.at[0], wbuf.at[2, rep], wsend.at[0], wrecv.at[0], (rep, xnb)).start()

    y_copy(0).start()
    loads[0].start()
    loads[1].start()

    @pl.loop(0, BATCH)
    def _(b):
        x_load(b).start()

    for load in loads[2:]:
        load.start()
    w_x = remote(wbuf.at[0, rep], wbuf.at[2, rep], wsend.at[0], wrecv.at[0], (rep, xnb))
    w_s = remote(wbuf.at[0], wbuf.at[1], wsend.at[1], wrecv.at[1], (rep, sib))
    w_z = remote(wbuf.at[2, rep], wbuf.at[2, rep], wsend.at[2], wrecv.at[2], (znb, me))
    w_xs = remote(wbuf.at[2, rep], wbuf.at[3, rep], wsend.at[3], wrecv.at[3], (rep, sib))
    w_zs = remote(wbuf.at[2, znb], wbuf.at[3, znb], wsend.at[4], wrecv.at[4], (rep, sib))
    loads[0].wait()
    loads[1].wait()
    w_s.start()

    def out_copy(s, b, o, kv):
        blk = me if s == 0 else ynb
        dst = kv_out.at[kv, b, pl.ds(pl.multiple_of(blk * ROWS, ROWS), ROWS), :]
        src = stage.at[s, b, o - 1, kv]
        return remote(src, dst, osend.at[o - 1, s, b, kv], orecv.at[o - 1, s, b, kv], (rep, near[o]))

    def own_two(b, o, kv):
        dst = kv_out.at[kv, pl.ds(b, 2), pl.ds(pl.multiple_of(me * ROWS, ROWS), ROWS), :]
        return remote(stage.at[0, pl.ds(b, 2), o - 1, kv], dst, osend.at[o - 1, 0, b, kv], orecv.at[o - 1, 0, b, kv], (rep, near[o]))

    def chunk_kv(b, o):
        dst = kv_out.at[:, b, pl.ds(pl.multiple_of(ynb * ROWS, ROWS), ROWS), :]
        return remote(stage.at[1, b, o - 1], dst, osend.at[o - 1, 1, b, 0], orecv.at[o - 1, 1, b, 0], (rep, near[o]))

    def project(buf, s, b, o, kv):
        acc = jnp.dot(buf[b], wbuf[o, kv], preferred_element_type=F32)
        blk = me if s == 0 else ynb
        c, sn = spread(tab[pl.ds(pl.multiple_of(blk * SEQ_LOC, SEQ_LOC), SEQ_LOC), :])
        is_k = kv == 0
        c = jnp.where(is_k, c, 1.0)
        sn = jnp.where(is_k, sn, 0.0)
        for h in range(2):
            tmp[pl.ds(h, SEQ_LOC, stride=2), :] = rotate(acc[:, h * HEAD_DIM:(h + 1) * HEAD_DIM], c, sn)
        if o == 0:
            kv_out[kv, b, pl.ds(pl.multiple_of(blk * ROWS, ROWS), ROWS), :] = tmp[...].astype(BF)
        else:
            stage[s, b, o - 1, kv] = tmp[...].astype(BF)

    @pl.loop(0, BATCH)
    def _(b):
        x_load(b).wait()
        x = xbuf[b].astype(F32)
        here = me * SEQ_LOC + lax.broadcasted_iota(jnp.int32, (SEQ_LOC, 1), 0) == lens[b] - 1
        lastf[pl.ds(b, 1), :] = jnp.sum(jnp.where(here, x, 0.0), axis=0, keepdims=True)
        xbuf[b] = norm_rows(x, gain_a[...])

    l_copy = [remote(lsend.at[i], lrecv.at[i], l_s.at[i], l_r.at[i], (rep, near[d])) for i, d in enumerate((4, 1, 2))]
    lsend[0] = lastf[...].astype(BF)
    loads[2].wait()
    l_copy[0].start()

    @pl.loop(1, BATCH)
    def _(b):
        y_copy(b).start()

    @pl.loop(0, BATCH)
    def _(b):
        @pl.loop(0, 2)
        def _(kv):
            project(xbuf, 0, b, 0, kv)

    def join_last(i):
        l_copy[i].wait_recv()
        return (lsend[i].astype(F32) + lrecv[i].astype(F32)).astype(BF)

    lsend[1] = join_last(0)
    w_s.wait_recv()
    l_copy[1].start()

    @pl.loop(0, BATCH)
    def _(b):
        @pl.loop(0, 2)
        def _(kv):
            project(xbuf, 0, b, 1, kv)
            out_copy(0, b, 1, kv).start()

    lsend[2] = join_last(1)

    w_x.wait_recv()
    w_z.start()
    w_xs.start()
    l_copy[2].start()

    def own_x_phase(kv, o):
        @pl.loop(0, BATCH, step=2)
        def _(b):
            project(xbuf, 0, b, o, kv)
            project(xbuf, 0, b + 1, o, kv)
            own_two(b, o, kv).start()

    own_x_phase(rep, 2)
    w_xs.wait_recv()
    own_x_phase(rep, 3)

    rows[0:BATCH, :] = new_tok[...].astype(F32)
    rows[BATCH:2 * BATCH, :] = join_last(2).astype(F32)
    loads[3].wait()
    n16 = norm_rows(rows[...], gain_a[...])
    q16 = jnp.dot(n16, wqb[...], preferred_element_type=F32)
    k16 = jnp.dot(n16, wbuf[0, 0], preferred_element_type=F32)
    v16 = jnp.dot(n16, wbuf[0, 1], preferred_element_type=F32)
    for b in range(BATCH):
        flat[pl.ds(b, 1), 0:HEAD_DIM] = tab[pl.ds(jnp.clip(lens[b], 0, SEQ_LEN), 1), :]
        flat[pl.ds(BATCH + b, 1), 0:HEAD_DIM] = tab[pl.ds(jnp.clip(lens[b] - 1, 0, SEQ_LEN), 1), :]
    c16, s16 = spread(flat[:, 0:HEAD_DIM])
    kself[...] = jnp.zeros_like(kself)
    vself[...] = jnp.zeros_like(vself)
    for h in range(2):
        lanes = slice(h * HEAD_DIM, (h + 1) * HEAD_DIM)
        qh = rotate(q16[:, lanes], c16, s16).astype(BF).astype(F32)
        kh = rotate(k16[:, lanes], c16, s16)[:BATCH].astype(BF).astype(F32)
        vh = v16[:BATCH, lanes].astype(BF).astype(F32)
        for g in range(2):
            qall[0, :, 2 * g + h, :] = qh[g * BATCH:(g + 1) * BATCH]
        kself[:, h, :] = kh
        vself[:, h, :] = vh
        tmp[pl.ds(h, BATCH, stride=2), :] = kh
        tmp[pl.ds(2 * BATCH + h, BATCH, stride=2), :] = vh
    new_out[0] = tmp[0:2 * BATCH, :].astype(BF)
    new_out[1] = tmp[2 * BATCH:4 * BATCH, :].astype(BF)
    low = lax.broadcasted_iota(jnp.int32, (4, HEAD_DIM), 1) < HALF
    part[:, 0] = jnp.zeros((4, BATCH, 4, HEAD_DIM), F32)
    part[:, 1] = jnp.broadcast_to(jnp.where(low, NEG_BIG, 0.0), (4, BATCH, 4, HEAD_DIM))
    q_copy = [remote(qall.at[0], qall.at[d], q_s.at[d - 1], q_r.at[d - 1], (rep, near[d])) for d in (1, 2, 3)]
    for c in q_copy:
        c.start()

    w_z.wait_recv()
    w_zs.start()
    w_zs.wait_recv()
    own_x_phase(znb, 2)
    own_x_phase(znb, 3)
    for c in q_copy:
        c.wait_recv()

    lane = lax.broadcasted_iota(jnp.int32, (4, ROWS), 1)
    same_head = lane % 2 == lax.broadcasted_iota(jnp.int32, (4, ROWS), 0) % 2

    def attend(s, b):
        blk = me if s == 0 else ynb
        seen = same_head & (blk * SEQ_LOC + lane // 2 < lens[b])
        four = range(4)
        mine = pl.ds(pl.multiple_of(blk * ROWS, ROWS), ROWS)
        keys, vals = ([kv_out[kv, b, mine, :]] + [stage[s, b, o - 1, kv] for o in (1, 2, 3)] for kv in range(2))
        old = [part[o, 1, b] for o in four]
        acc = [part[o, 0, b] for o in four]
        sc = [lax.dot_general(qall[o, b].astype(BF), keys[o], (((1,), (1,)), ((), ())), preferred_element_type=F32) for o in four]
        sc = [jnp.where(seen, x * SCALE, NEG_BIG) for x in sc]
        top = [jnp.maximum(old[o][:, 0:1], jnp.max(sc[o], axis=-1, keepdims=True)) for o in four]
        p = [jnp.where(seen, jnp.exp(sc[o] - top[o]), 0.0) for o in four]
        fade = [jnp.exp(old[o][:, 0:1] - top[o]) for o in four]
        den = [old[o][:, HALF:HALF + 1] * fade[o] + jnp.sum(p[o], axis=-1, keepdims=True) for o in four]
        add = [jnp.dot(p[o].astype(BF), vals[o], preferred_element_type=F32) for o in four]
        for o in four:
            part[o, 0, b] = acc[o] * fade[o] + add[o]
            part[o, 1, b] = jnp.where(low, top[o], den[o])

    waiting = [(b, kv, o) for b in range(5, BATCH) for kv in range(2) for o in (2, 3)]

    def leave(b, kv, o):
        out_copy(1, b, o, kv).start()

    @pl.loop(0, BATCH)
    def _(b):
        attend(0, b)
        y_copy(b).wait_recv()

        @pl.when(b == BATCH - 1)
        def _():
            leave(*waiting[0])
            leave(*waiting[1])
        xrecv[b] = norm_rows(xrecv[b].astype(F32), gain_a[...])

        @pl.loop(0, 2)
        def _(kv):
            for o in (2, 3):
                project(xrecv, 1, b, o, kv)

                @pl.when((b < 5) & (kv == 1))
                def _():
                    chunk_kv(b, o).start()

            project(xrecv, 1, b, 1, kv)
            out_copy(1, b, 1, kv).start()
            project(xrecv, 1, b, 0, kv)

        attend(1, b)

    p_copy = [remote(part.at[d], precv.at[d - 1], p_s.at[d - 1], p_r.at[d - 1], (rep, near[d])) for d in (1, 2, 3)]
    for c in p_copy:
        c.start()
    for job in waiting[2:4]:
        leave(*job)
    for load in loads[4:]:
        load.wait()
    first = lax.broadcasted_iota(jnp.int32, (BATCH, 4, 1), 1) < 2
    s_self = jnp.where(first, jnp.sum(qall[0] * kself[...], axis=-1, keepdims=True) * SCALE, NEG_BIG)
    for c in p_copy:
        c.wait_recv()
    accs = [part[0, 0]] + [precv[i, 0] for i in range(3)]
    stats = [part[0, 1]] + [precv[i, 1] for i in range(3)]
    tops = [st[:, :, 0:1] for st in stats]
    top = s_self
    for t in tops:
        top = jnp.maximum(top, t)
    e_self = jnp.where(first, jnp.exp(s_self - top), 0.0)
    den = e_self
    num = e_self * vself[...]
    for t, st, ac in zip(tops, stats, accs):
        e = jnp.exp(t - top)
        den = den + e * st[:, :, HALF:HALF + 1]
        num = num + e * ac
    attn[...] = num / den
    for g in range(2):
        for h in range(2):
            flat[g * BATCH:(g + 1) * BATCH, h * HEAD_DIM:(h + 1) * HEAD_DIM] = attn[:, 2 * g + h, :]

    def reduce_columns(i, base, jobs):
        sends = [remote(psend.at[i, near[d]], rrecv.at[i, d - 1], r_s.at[i, d - 1], r_r.at[i, d - 1], (rep, near[d])) for d in range(1, 8)]
        for c in sends:
            c.start()
        for job in jobs[0]:
            leave(*job)
        total = psend[i, me]
        for d in range(1, 8):
            sends[d - 1].wait_recv()
            total = total + rrecv[i, d - 1]
        hid[i, me] = (base + total).astype(BF)
        gets = [remote(hid.at[i, me], hid.at[i, me], a_s.at[i, d - 1], a_r.at[i, d - 1], (rep, near[d])) for d in range(1, 8)]
        for c in gets:
            c.start()
        for job in jobs[1]:
            leave(*job)
        for d in range(1, 8):
            remote(hid.at[i, near[d]], hid.at[i, near[d]], a_s.at[i, d - 1], a_r.at[i, d - 1], (rep, near[d])).wait_recv()
        return sends + gets

    a16 = flat[...].astype(BF)
    for j in range(8):
        psend[0, j] = jnp.dot(a16, wob[:, j * SHARD:(j + 1) * SHARD], preferred_element_type=F32)
    mine = pl.ds(pl.multiple_of(me * SHARD, SHARD), SHARD)
    done = reduce_columns(0, rows[:, mine], (waiting[4:6], waiting[6:8]))

    sq = jnp.zeros((2 * BATCH, 1), F32)
    for j in range(8):
        hj = hid[0, j].astype(F32)
        sq = sq + jnp.sum(hj * hj, axis=-1, keepdims=True)
    inv = lax.rsqrt(sq / D_MODEL + 1e-5)
    for j in range(8):
        cols = slice(j * SHARD, (j + 1) * SHARD)
        norm2[:, cols] = (hid[0, j].astype(F32) * inv * gain_m[:, cols].astype(F32)).astype(BF)
    n2 = norm2[...]
    gate = jnp.dot(n2, wgb[...], preferred_element_type=F32)
    up = jnp.dot(n2, wub[...], preferred_element_type=F32)
    mid = (gate * jax.nn.sigmoid(gate) * up).astype(BF)
    for j in range(8):
        psend[1, j] = jnp.dot(mid, wdb[:, j * SHARD:(j + 1) * SHARD], preferred_element_type=F32)
    done += reduce_columns(1, hid[0, me].astype(F32), (waiting[8:10], waiting[10:12]))
    for j in range(8):
        cols = slice(j * SHARD, (j + 1) * SHARD)
        dec_out[:, cols] = hid[1, j][:BATCH]
        last_out[:, cols] = hid[1, j][BATCH:]

    for c in [w_x, w_s, w_z, w_xs, w_zs] + l_copy + q_copy + p_copy + done:
        c.wait_send()

    @pl.loop(0, BATCH)
    def _(b):
        y_copy(b).wait_send()
        for kv in range(2):
            for s in range(2):
                out_copy(s, b, 1, kv).wait()

    for o in (2, 3):
        @pl.loop(0, BATCH, step=2)
        def _(b):
            for kv in range(2):
                own_two(b, o, kv).wait()

        @pl.loop(0, 5)
        def _(b):
            chunk_kv(b, o).wait()

    for b, kv, o in waiting:
        out_copy(1, b, o, kv).wait()


def layer(lens, prompt, new_tok, gain_a, gain_m, table, wq, wk, wv, wo, wg, wu, wd):
    vmem = pl.BlockSpec(memory_space=pltpu.VMEM)
    anym = pl.BlockSpec(memory_space=pl.ANY)
    dma = pltpu.SemaphoreType.DMA
    v = pltpu.VMEM
    return pl.pallas_call(
        layer_kernel,
        out_shape=(
            pltpu.VMEM((2, BATCH, 8 * ROWS, HEAD_DIM), BF),
            pltpu.VMEM((2, 2 * BATCH, HEAD_DIM), BF),
            pltpu.VMEM((BATCH, D_MODEL), BF),
            pltpu.VMEM((BATCH, D_MODEL), BF),
        ),
        in_specs=[pl.BlockSpec(memory_space=pltpu.SMEM), anym, vmem, vmem, vmem] + [anym] * 8,
        out_specs=(vmem, vmem, vmem, vmem),
        scratch_shapes=[
            v((BATCH, SEQ_LOC, D_MODEL), BF), v((BATCH, SEQ_LOC, D_MODEL), BF), v((4, 2, D_MODEL, SHARD), BF),
            v((D_MODEL, SHARD), BF), v((SHARD, D_MODEL), BF), v((D_MODEL, FF_LOC), BF), v((D_MODEL, FF_LOC), BF), v((FF_LOC, D_MODEL), BF),
            v((TAB_ROWS, HEAD_DIM), F32), v((ROWS, HEAD_DIM), F32), v((2, BATCH, 3, 2, ROWS, HEAD_DIM), BF),
            v((BATCH, D_MODEL), F32), v((3, BATCH, D_MODEL), BF), v((3, BATCH, D_MODEL), BF), v((2 * BATCH, D_MODEL), F32),
            v((4, BATCH, 4, HEAD_DIM), F32), v((4, 2, BATCH, 4, HEAD_DIM), F32), v((3, 2, BATCH, 4, HEAD_DIM), F32),
            v((BATCH, 4, HEAD_DIM), F32), v((BATCH, 4, HEAD_DIM), F32), v((BATCH, 4, HEAD_DIM), F32), v((2 * BATCH, SHARD), F32),
            v((2, 8, 2 * BATCH, SHARD), F32), v((2, 7, 2 * BATCH, SHARD), F32), v((2, 8, 2 * BATCH, SHARD), BF), v((2 * BATCH, D_MODEL), BF),
            dma((8,)), dma((BATCH,)), dma((BATCH,)), dma((BATCH,)), dma((5,)), dma((5,)),
            dma((3, 2, BATCH, 2)), dma((3, 2, BATCH, 2)),
            dma((3,)), dma((3,)), dma((3,)), dma((3,)), dma((3,)), dma((3,)),
            dma((2, 7)), dma((2, 7)), dma((2, 7)), dma((2, 7)),
        ],
        compiler_params=pltpu.CompilerParams(collective_id=0, has_side_effects=True, vmem_limit_bytes=49 * 1024 * 1024),
        cost_estimate=pl.CostEstimate(flops=26_000_000_000, bytes_accessed=60_000_000, transcendentals=0),
        name='layer',
    )(lens, prompt, new_tok, gain_a, gain_m, table, wq, wk, wv, wo, wg, wu, wd)


def cache_kernel(kv, new, dec, last, key_out, val_out, dec_out, last_out, store, row_sem):
    outs = (key_out, val_out)
    puts = []
    for i in range(2):
        for b in range(BATCH):
            puts.append(pltpu.make_async_copy(kv.at[i, b], outs[i].at[0, b, pl.ds(0, SEQ_LEN)], store.at[i, b]))
            puts[-1].start()
    for i in range(2):
        puts.append(pltpu.make_async_copy(new.at[i], outs[i].at[0, :, pl.ds(SEQ_LEN, 1)], row_sem.at[i]))
        puts[-1].start()
    dec_out[...] = dec[...]
    last_out[...] = last[...]
    for c in puts:
        c.wait()


def caches(kv, new, dec, last):
    anym = pl.BlockSpec(memory_space=pl.ANY)
    dma = pltpu.SemaphoreType.DMA
    vmem = pl.BlockSpec(memory_space=pltpu.VMEM)
    shape = jax.ShapeDtypeStruct((1, BATCH, SEQ_LEN + 1, 2, HEAD_DIM), BF)
    row = jax.ShapeDtypeStruct((BATCH, D_MODEL), BF)
    return pl.pallas_call(
        cache_kernel,
        out_shape=(shape, shape, row, row),
        in_specs=[anym, anym, vmem, vmem],
        out_specs=(anym, anym, vmem, vmem),
        scratch_shapes=[dma((2, BATCH)), dma((2,))],
        compiler_params=pltpu.CompilerParams(vmem_limit_bytes=4 * 1024 * 1024),
        cost_estimate=pl.CostEstimate(flops=0, bytes_accessed=13_000_000, transcendentals=0),
        name='caches',
    )(kv, new, dec, last)


def solution(mesh):
    seq_spec = P('replica', 'model', None)
    col_spec = P(None, None, 'model')
    row_spec = P(None, 'model', None)
    gain_spec = P(None, None)
    tok_spec = P('replica', None)
    cache_spec = P(None, 'replica', None, 'model', None)
    in_specs = (seq_spec, P('replica'), tok_spec, gain_spec, col_spec, col_spec, col_spec, row_spec, gain_spec, col_spec, col_spec, row_spec)
    out_specs = (tok_spec, tok_spec, cache_spec, cache_spec)
    table = rope_table()

    def per_device(prompt, lengths, new_tok, norm_attn, w_q, w_k, w_v, w_o, norm_mlp, w_gate, w_up, w_down):
        kv, new, dec, last = layer(lengths, prompt, new_tok, norm_attn, norm_mlp, jnp.asarray(table), w_q, w_k, w_v, w_o, w_gate, w_up, w_down)
        keys, vals, dec, last = caches(kv.reshape(2, BATCH, SEQ_LEN, 2, HEAD_DIM), new.reshape(2, BATCH, 1, 2, HEAD_DIM), dec, last)
        return dec, last, keys, vals

    return jax.shard_map(per_device, mesh=mesh, in_specs=in_specs, out_specs=out_specs, check_vma=False)
```

```python
import jax
import jax.numpy as jnp
import numpy as np
from jax import lax
from jax.experimental import pallas as pl
from jax.experimental.pallas import tpu as pltpu
from jax.sharding import PartitionSpec as P

HEAD_DIM = 128
HALF = HEAD_DIM // 2
NEG_BIG = -1e30
BATCH = 8
SEQ_LOC = 192
SEQ_LEN = 1536
D_MODEL = 2048
SHARD = 256
FF_LOC = 1024
ROWS = 2 * SEQ_LOC
TAB_ROWS = SEQ_LEN + 8
MESH = pl.DeviceIdType.MESH
BF = jnp.bfloat16
F32 = jnp.float32
SCALE = HEAD_DIM ** -0.5


def rope_table():
    inv_freq = np.float32(10000.0) ** (np.float32(-2.0) * np.arange(HALF, dtype=np.float32) / np.float32(HEAD_DIM))
    angles = np.arange(TAB_ROWS, dtype=np.float32)[:, None] * inv_freq.astype(np.float32)
    return np.concatenate([np.cos(angles), np.sin(angles)], axis=-1).astype(np.float32)


def norm_rows(x, gain):
    inv = lax.rsqrt(jnp.mean(x * x, axis=-1, keepdims=True) + 1e-5)
    return (x * inv * gain.astype(F32)).astype(BF)


def spread(tab):
    swapped = pltpu.roll(tab, HALF, 1)
    low = lax.broadcasted_iota(jnp.int32, tab.shape, 1) < HALF
    return jnp.where(low, tab, swapped), jnp.where(low, -swapped, tab)


def rotate(a, c, s):
    return a * c + pltpu.roll(a, HALF, 1) * s


def layer_kernel(lens, prompt, new_tok, gain_a, gain_m, table, wq, wk, wv, wo, wg, wu, wd,
                 kv_out, new_out, dec_out, last_out,
                 xbuf, xrecv, wbuf, wqb, wob, wgb, wub, wdb, tab, tmp, stage,
                 lastf, lsend, lrecv, rows, qall, part, precv, kself, vself, attn, flat,
                 psend, rrecv, hid, norm2,
                 lsem, xsem, ysend, yrecv, wsend, wrecv, osend, orecv,
                 l_s, l_r, q_s, q_r, p_s, p_r, r_s, r_r, a_s, a_r):
    rep = lax.axis_index('replica')
    me = lax.axis_index('model')
    core = lax.rem(me, 2)
    xpos = lax.rem(me // 2, 2)
    ypos = me // 4
    flips = (1 - 2 * core, 2 - 4 * xpos, 4 - 8 * ypos)
    near = [me + sum(f for i, f in enumerate(flips) if d >> i & 1) for d in range(8)]
    sib, xnb, xsb, ynb = near[1], near[2], near[3], near[4]
    znb = 1 - rep

    barrier = pltpu.get_barrier_semaphore()
    for peer in [(rep, near[d]) for d in range(1, 8)] + [(znb, me)]:
        pl.semaphore_signal(barrier, inc=1, device_id=peer, device_id_type=MESH)
    pl.semaphore_wait(barrier, 8)

    def remote(src, dst, send, recv, peer):
        return pltpu.make_async_remote_copy(src_ref=src, dst_ref=dst, send_sem=send, recv_sem=recv, device_id=peer, device_id_type=MESH)

    def y_copy(b):
        return remote(prompt.at[b], xrecv.at[b], ysend.at[b], yrecv.at[b], (rep, ynb))

    def x_load(b):
        return pltpu.make_async_copy(prompt.at[b], xbuf.at[b], xsem.at[b])

    loads = [pltpu.make_async_copy(a, b, lsem.at[i]) for i, (a, b) in enumerate((
        (wk.at[0], wbuf.at[0, 0]), (wv.at[0], wbuf.at[0, 1]), (table, tab), (wq.at[0], wqb), (wo.at[0], wob),
        (wg.at[0], wgb), (wu.at[0], wub), (wd.at[0], wdb)))]
    for i, w in enumerate((wk, wv)):
        @pl.when(rep == i)
        def _():
            remote(w.at[0], wbuf.at[2, rep], wsend.at[0], wrecv.at[0], (rep, xnb)).start()

    y_copy(0).start()
    loads[0].start()
    loads[1].start()

    @pl.loop(0, BATCH)
    def _(b):
        x_load(b).start()

    for load in loads[2:]:
        load.start()
    w_x = remote(wbuf.at[0, rep], wbuf.at[2, rep], wsend.at[0], wrecv.at[0], (rep, xnb))
    w_s = remote(wbuf.at[0], wbuf.at[1], wsend.at[1], wrecv.at[1], (rep, sib))
    w_z = remote(wbuf.at[2, rep], wbuf.at[2, rep], wsend.at[2], wrecv.at[2], (znb, me))
    w_xs = remote(wbuf.at[2, rep], wbuf.at[3, rep], wsend.at[3], wrecv.at[3], (rep, sib))
    w_zs = remote(wbuf.at[2, znb], wbuf.at[3, znb], wsend.at[4], wrecv.at[4], (rep, sib))
    loads[0].wait()
    loads[1].wait()
    w_s.start()

    def out_copy(s, b, o, kv):
        blk = me if s == 0 else ynb
        dst = kv_out.at[kv, b, pl.ds(pl.multiple_of(blk * ROWS, ROWS), ROWS), :]
        src = stage.at[s, b, o - 1, kv]
        return remote(src, dst, osend.at[o - 1, s, b, kv], orecv.at[o - 1, s, b, kv], (rep, near[o]))

    def own_two(b, o, kv):
        dst = kv_out.at[kv, pl.ds(b, 2), pl.ds(pl.multiple_of(me * ROWS, ROWS), ROWS), :]
        return remote(stage.at[0, pl.ds(b, 2), o - 1, kv], dst, osend.at[o - 1, 0, b, kv], orecv.at[o - 1, 0, b, kv], (rep, near[o]))

    def chunk_kv(b, o):
        dst = kv_out.at[:, b, pl.ds(pl.multiple_of(ynb * ROWS, ROWS), ROWS), :]
        return remote(stage.at[1, b, o - 1], dst, osend.at[o - 1, 1, b, 0], orecv.at[o - 1, 1, b, 0], (rep, near[o]))

    def project(buf, s, b, o, kv):
        acc = jnp.dot(buf[b], wbuf[o, kv], preferred_element_type=F32)
        blk = me if s == 0 else ynb
        c, sn = spread(tab[pl.ds(pl.multiple_of(blk * SEQ_LOC, SEQ_LOC), SEQ_LOC), :])
        is_k = kv == 0
        c = jnp.where(is_k, c, 1.0)
        sn = jnp.where(is_k, sn, 0.0)
        for h in range(2):
            tmp[pl.ds(h, SEQ_LOC, stride=2), :] = rotate(acc[:, h * HEAD_DIM:(h + 1) * HEAD_DIM], c, sn)
        if o == 0:
            kv_out[kv, b, pl.ds(pl.multiple_of(blk * ROWS, ROWS), ROWS), :] = tmp[...].astype(BF)
        else:
            stage[s, b, o - 1, kv] = tmp[...].astype(BF)

    @pl.loop(0, BATCH)
    def _(b):
        x_load(b).wait()
        x = xbuf[b].astype(F32)
        here = me * SEQ_LOC + lax.broadcasted_iota(jnp.int32, (SEQ_LOC, 1), 0) == lens[b] - 1
        lastf[pl.ds(b, 1), :] = jnp.sum(jnp.where(here, x, 0.0), axis=0, keepdims=True)
        xbuf[b] = norm_rows(x, gain_a[...])

    l_copy = [remote(lsend.at[i], lrecv.at[i], l_s.at[i], l_r.at[i], (rep, near[d])) for i, d in enumerate((4, 1, 2))]
    lsend[0] = lastf[...].astype(BF)
    loads[2].wait()
    l_copy[0].start()

    @pl.loop(1, BATCH)
    def _(b):
        y_copy(b).start()

    @pl.loop(0, BATCH)
    def _(b):
        @pl.loop(0, 2)
        def _(kv):
            project(xbuf, 0, b, 0, kv)

    def join_last(i):
        l_copy[i].wait_recv()
        return (lsend[i].astype(F32) + lrecv[i].astype(F32)).astype(BF)

    lsend[1] = join_last(0)
    w_s.wait_recv()
    l_copy[1].start()

    @pl.loop(0, BATCH)
    def _(b):
        @pl.loop(0, 2)
        def _(kv):
            project(xbuf, 0, b, 1, kv)
            out_copy(0, b, 1, kv).start()

    lsend[2] = join_last(1)

    w_x.wait_recv()
    w_z.start()
    w_xs.start()
    l_copy[2].start()

    def own_x_phase(kv, o):
        @pl.loop(0, BATCH, step=2)
        def _(b):
            project(xbuf, 0, b, o, kv)
            project(xbuf, 0, b + 1, o, kv)
            own_two(b, o, kv).start()

    own_x_phase(rep, 2)
    w_xs.wait_recv()
    own_x_phase(rep, 3)

    rows[0:BATCH, :] = new_tok[...].astype(F32)
    rows[BATCH:2 * BATCH, :] = join_last(2).astype(F32)
    loads[3].wait()
    n16 = norm_rows(rows[...], gain_a[...])
    q16 = jnp.dot(n16, wqb[...], preferred_element_type=F32)
    k16 = jnp.dot(n16, wbuf[0, 0], preferred_element_type=F32)
    v16 = jnp.dot(n16, wbuf[0, 1], preferred_element_type=F32)
    for b in range(BATCH):
        flat[pl.ds(b, 1), 0:HEAD_DIM] = tab[pl.ds(jnp.clip(lens[b], 0, SEQ_LEN), 1), :]
        flat[pl.ds(BATCH + b, 1), 0:HEAD_DIM] = tab[pl.ds(jnp.clip(lens[b] - 1, 0, SEQ_LEN), 1), :]
    c16, s16 = spread(flat[:, 0:HEAD_DIM])
    kself[...] = jnp.zeros_like(kself)
    vself[...] = jnp.zeros_like(vself)
    for h in range(2):
        lanes = slice(h * HEAD_DIM, (h + 1) * HEAD_DIM)
        qh = rotate(q16[:, lanes], c16, s16).astype(BF).astype(F32)
        kh = rotate(k16[:, lanes], c16, s16)[:BATCH].astype(BF).astype(F32)
        vh = v16[:BATCH, lanes].astype(BF).astype(F32)
        for g in range(2):
            qall[0, :, 2 * g + h, :] = qh[g * BATCH:(g + 1) * BATCH]
        kself[:, h, :] = kh
        vself[:, h, :] = vh
        tmp[pl.ds(h, BATCH, stride=2), :] = kh
        tmp[pl.ds(2 * BATCH + h, BATCH, stride=2), :] = vh
    new_out[0] = tmp[0:2 * BATCH, :].astype(BF)
    new_out[1] = tmp[2 * BATCH:4 * BATCH, :].astype(BF)
    low = lax.broadcasted_iota(jnp.int32, (4, HEAD_DIM), 1) < HALF
    part[:, 0] = jnp.zeros((4, BATCH, 4, HEAD_DIM), F32)
    part[:, 1] = jnp.broadcast_to(jnp.where(low, NEG_BIG, 0.0), (4, BATCH, 4, HEAD_DIM))
    q_copy = [remote(qall.at[0], qall.at[d], q_s.at[d - 1], q_r.at[d - 1], (rep, near[d])) for d in (1, 2, 3)]
    for c in q_copy:
        c.start()

    w_z.wait_recv()
    w_zs.start()
    w_zs.wait_recv()
    own_x_phase(znb, 2)
    own_x_phase(znb, 3)
    for c in q_copy:
        c.wait_recv()

    lane = lax.broadcasted_iota(jnp.int32, (4, ROWS), 1)
    same_head = lane % 2 == lax.broadcasted_iota(jnp.int32, (4, ROWS), 0) % 2

    def attend(s, b):
        blk = me if s == 0 else ynb
        seen = same_head & (blk * SEQ_LOC + lane // 2 < lens[b])
        four = range(4)
        mine = pl.ds(pl.multiple_of(blk * ROWS, ROWS), ROWS)
        keys, vals = ([kv_out[kv, b, mine, :]] + [stage[s, b, o - 1, kv] for o in (1, 2, 3)] for kv in range(2))
        old = [part[o, 1, b] for o in four]
        acc = [part[o, 0, b] for o in four]
        sc = [lax.dot_general(qall[o, b].astype(BF), keys[o], (((1,), (1,)), ((), ())), preferred_element_type=F32) for o in four]
        sc = [jnp.where(seen, x * SCALE, NEG_BIG) for x in sc]
        top = [jnp.maximum(old[o][:, 0:1], jnp.max(sc[o], axis=-1, keepdims=True)) for o in four]
        p = [jnp.where(seen, jnp.exp(sc[o] - top[o]), 0.0) for o in four]
        fade = [jnp.exp(old[o][:, 0:1] - top[o]) for o in four]
        den = [old[o][:, HALF:HALF + 1] * fade[o] + jnp.sum(p[o], axis=-1, keepdims=True) for o in four]
        add = [jnp.dot(p[o].astype(BF), vals[o], preferred_element_type=F32) for o in four]
        for o in four:
            part[o, 0, b] = acc[o] * fade[o] + add[o]
            part[o, 1, b] = jnp.where(low, top[o], den[o])

    waiting = [(b, kv, o) for b in range(6, BATCH) for kv in range(2) for o in (2, 3)]

    def leave(b, kv, o):
        out_copy(1, b, o, kv).start()

    @pl.loop(0, BATCH)
    def _(b):
        attend(0, b)
        y_copy(b).wait_recv()

        xrecv[b] = norm_rows(xrecv[b].astype(F32), gain_a[...])

        @pl.loop(0, 2)
        def _(kv):
            for o in (2, 3):
                project(xrecv, 1, b, o, kv)

                @pl.when((b < 6) & (kv == 1))
                def _():
                    chunk_kv(b, o).start()

            project(xrecv, 1, b, 1, kv)
            out_copy(1, b, 1, kv).start()
            project(xrecv, 1, b, 0, kv)

        attend(1, b)

    p_copy = [remote(part.at[d], precv.at[d - 1], p_s.at[d - 1], p_r.at[d - 1], (rep, near[d])) for d in (1, 2, 3)]
    for c in p_copy:
        c.start()
    for job in waiting[0:2]:
        leave(*job)
    for load in loads[4:]:
        load.wait()
    first = lax.broadcasted_iota(jnp.int32, (BATCH, 4, 1), 1) < 2
    s_self = jnp.where(first, jnp.sum(qall[0] * kself[...], axis=-1, keepdims=True) * SCALE, NEG_BIG)
    for c in p_copy:
        c.wait_recv()
    accs = [part[0, 0]] + [precv[i, 0] for i in range(3)]
    stats = [part[0, 1]] + [precv[i, 1] for i in range(3)]
    tops = [st[:, :, 0:1] for st in stats]
    top = s_self
    for t in tops:
        top = jnp.maximum(top, t)
    e_self = jnp.where(first, jnp.exp(s_self - top), 0.0)
    den = e_self
    num = e_self * vself[...]
    for t, st, ac in zip(tops, stats, accs):
        e = jnp.exp(t - top)
        den = den + e * st[:, :, HALF:HALF + 1]
        num = num + e * ac
    attn[...] = num / den
    for g in range(2):
        for h in range(2):
            flat[g * BATCH:(g + 1) * BATCH, h * HEAD_DIM:(h + 1) * HEAD_DIM] = attn[:, 2 * g + h, :]

    def reduce_columns(i, base, jobs):
        sends = [remote(psend.at[i, near[d]], rrecv.at[i, d - 1], r_s.at[i, d - 1], r_r.at[i, d - 1], (rep, near[d])) for d in range(1, 8)]
        for c in sends:
            c.start()
        for job in jobs[0]:
            leave(*job)
        total = psend[i, me]
        for d in range(1, 8):
            sends[d - 1].wait_recv()
            total = total + rrecv[i, d - 1]
        hid[i, me] = (base + total).astype(BF)
        gets = [remote(hid.at[i, me], hid.at[i, me], a_s.at[i, d - 1], a_r.at[i, d - 1], (rep, near[d])) for d in range(1, 8)]
        for c in gets:
            c.start()
        for job in jobs[1]:
            leave(*job)
        for d in range(1, 8):
            remote(hid.at[i, near[d]], hid.at[i, near[d]], a_s.at[i, d - 1], a_r.at[i, d - 1], (rep, near[d])).wait_recv()
        return sends + gets

    a16 = flat[...].astype(BF)
    for j in range(8):
        psend[0, j] = jnp.dot(a16, wob[:, j * SHARD:(j + 1) * SHARD], preferred_element_type=F32)
    mine = pl.ds(pl.multiple_of(me * SHARD, SHARD), SHARD)
    done = reduce_columns(0, rows[:, mine], (waiting[2:3], waiting[3:6]))

    sq = jnp.zeros((2 * BATCH, 1), F32)
    for j in range(8):
        hj = hid[0, j].astype(F32)
        sq = sq + jnp.sum(hj * hj, axis=-1, keepdims=True)
    inv = lax.rsqrt(sq / D_MODEL + 1e-5)
    for j in range(8):
        cols = slice(j * SHARD, (j + 1) * SHARD)
        norm2[:, cols] = (hid[0, j].astype(F32) * inv * gain_m[:, cols].astype(F32)).astype(BF)
    n2 = norm2[...]
    gate = jnp.dot(n2, wgb[...], preferred_element_type=F32)
    up = jnp.dot(n2, wub[...], preferred_element_type=F32)
    mid = (gate * jax.nn.sigmoid(gate) * up).astype(BF)
    for j in range(8):
        psend[1, j] = jnp.dot(mid, wdb[:, j * SHARD:(j + 1) * SHARD], preferred_element_type=F32)
    done += reduce_columns(1, hid[0, me].astype(F32), (waiting[6:7], waiting[7:8]))
    for j in range(8):
        cols = slice(j * SHARD, (j + 1) * SHARD)
        dec_out[:, cols] = hid[1, j][:BATCH]
        last_out[:, cols] = hid[1, j][BATCH:]

    for c in [w_x, w_s, w_z, w_xs, w_zs] + l_copy + q_copy + p_copy + done:
        c.wait_send()

    @pl.loop(0, BATCH)
    def _(b):
        y_copy(b).wait_send()
        for kv in range(2):
            for s in range(2):
                out_copy(s, b, 1, kv).wait()

    for o in (2, 3):
        @pl.loop(0, BATCH, step=2)
        def _(b):
            for kv in range(2):
                own_two(b, o, kv).wait()

        @pl.loop(0, 6)
        def _(b):
            chunk_kv(b, o).wait()

    for b, kv, o in waiting:
        out_copy(1, b, o, kv).wait()


def layer(lens, prompt, new_tok, gain_a, gain_m, table, wq, wk, wv, wo, wg, wu, wd):
    vmem = pl.BlockSpec(memory_space=pltpu.VMEM)
    anym = pl.BlockSpec(memory_space=pl.ANY)
    dma = pltpu.SemaphoreType.DMA
    v = pltpu.VMEM
    return pl.pallas_call(
        layer_kernel,
        out_shape=(
            pltpu.VMEM((2, BATCH, 8 * ROWS, HEAD_DIM), BF),
            pltpu.VMEM((2, 2 * BATCH, HEAD_DIM), BF),
            pltpu.VMEM((BATCH, D_MODEL), BF),
            pltpu.VMEM((BATCH, D_MODEL), BF),
        ),
        in_specs=[pl.BlockSpec(memory_space=pltpu.SMEM), anym, vmem, vmem, vmem] + [anym] * 8,
        out_specs=(vmem, vmem, vmem, vmem),
        scratch_shapes=[
            v((BATCH, SEQ_LOC, D_MODEL), BF), v((BATCH, SEQ_LOC, D_MODEL), BF), v((4, 2, D_MODEL, SHARD), BF),
            v((D_MODEL, SHARD), BF), v((SHARD, D_MODEL), BF), v((D_MODEL, FF_LOC), BF), v((D_MODEL, FF_LOC), BF), v((FF_LOC, D_MODEL), BF),
            v((TAB_ROWS, HEAD_DIM), F32), v((ROWS, HEAD_DIM), F32), v((2, BATCH, 3, 2, ROWS, HEAD_DIM), BF),
            v((BATCH, D_MODEL), F32), v((3, BATCH, D_MODEL), BF), v((3, BATCH, D_MODEL), BF), v((2 * BATCH, D_MODEL), F32),
            v((4, BATCH, 4, HEAD_DIM), F32), v((4, 2, BATCH, 4, HEAD_DIM), F32), v((3, 2, BATCH, 4, HEAD_DIM), F32),
            v((BATCH, 4, HEAD_DIM), F32), v((BATCH, 4, HEAD_DIM), F32), v((BATCH, 4, HEAD_DIM), F32), v((2 * BATCH, SHARD), F32),
            v((2, 8, 2 * BATCH, SHARD), F32), v((2, 7, 2 * BATCH, SHARD), F32), v((2, 8, 2 * BATCH, SHARD), BF), v((2 * BATCH, D_MODEL), BF),
            dma((8,)), dma((BATCH,)), dma((BATCH,)), dma((BATCH,)), dma((5,)), dma((5,)),
            dma((3, 2, BATCH, 2)), dma((3, 2, BATCH, 2)),
            dma((3,)), dma((3,)), dma((3,)), dma((3,)), dma((3,)), dma((3,)),
            dma((2, 7)), dma((2, 7)), dma((2, 7)), dma((2, 7)),
        ],
        compiler_params=pltpu.CompilerParams(collective_id=0, has_side_effects=True, vmem_limit_bytes=49 * 1024 * 1024),
        cost_estimate=pl.CostEstimate(flops=26_000_000_000, bytes_accessed=60_000_000, transcendentals=0),
        name='layer',
    )(lens, prompt, new_tok, gain_a, gain_m, table, wq, wk, wv, wo, wg, wu, wd)


def cache_kernel(kv, new, dec, last, key_out, val_out, dec_out, last_out, store, row_sem):
    outs = (key_out, val_out)
    puts = []
    for i in range(2):
        for b in range(BATCH):
            puts.append(pltpu.make_async_copy(kv.at[i, b], outs[i].at[0, b, pl.ds(0, SEQ_LEN)], store.at[i, b]))
            puts[-1].start()
    for i in range(2):
        puts.append(pltpu.make_async_copy(new.at[i], outs[i].at[0, :, pl.ds(SEQ_LEN, 1)], row_sem.at[i]))
        puts[-1].start()
    dec_out[...] = dec[...]
    last_out[...] = last[...]
    for c in puts:
        c.wait()


def caches(kv, new, dec, last):
    anym = pl.BlockSpec(memory_space=pl.ANY)
    dma = pltpu.SemaphoreType.DMA
    vmem = pl.BlockSpec(memory_space=pltpu.VMEM)
    shape = jax.ShapeDtypeStruct((1, BATCH, SEQ_LEN + 1, 2, HEAD_DIM), BF)
    row = jax.ShapeDtypeStruct((BATCH, D_MODEL), BF)
    return pl.pallas_call(
        cache_kernel,
        out_shape=(shape, shape, row, row),
        in_specs=[anym, anym, vmem, vmem],
        out_specs=(anym, anym, vmem, vmem),
        scratch_shapes=[dma((2, BATCH)), dma((2,))],
        compiler_params=pltpu.CompilerParams(vmem_limit_bytes=4 * 1024 * 1024),
        cost_estimate=pl.CostEstimate(flops=0, bytes_accessed=13_000_000, transcendentals=0),
        name='caches',
    )(kv, new, dec, last)


def solution(mesh):
    seq_spec = P('replica', 'model', None)
    col_spec = P(None, None, 'model')
    row_spec = P(None, 'model', None)
    gain_spec = P(None, None)
    tok_spec = P('replica', None)
    cache_spec = P(None, 'replica', None, 'model', None)
    in_specs = (seq_spec, P('replica'), tok_spec, gain_spec, col_spec, col_spec, col_spec, row_spec, gain_spec, col_spec, col_spec, row_spec)
    out_specs = (tok_spec, tok_spec, cache_spec, cache_spec)
    table = rope_table()

    def per_device(prompt, lengths, new_tok, norm_attn, w_q, w_k, w_v, w_o, norm_mlp, w_gate, w_up, w_down):
        kv, new, dec, last = layer(lengths, prompt, new_tok, norm_attn, norm_mlp, jnp.asarray(table), w_q, w_k, w_v, w_o, w_gate, w_up, w_down)
        keys, vals, dec, last = caches(kv.reshape(2, BATCH, SEQ_LEN, 2, HEAD_DIM), new.reshape(2, BATCH, 1, 2, HEAD_DIM), dec, last)
        return dec, last, keys, vals

    return jax.shard_map(per_device, mesh=mesh, in_specs=in_specs, out_specs=out_specs, check_vma=False)
```

```python
import jax
import jax.numpy as jnp
import numpy as np
from jax import lax
from jax.experimental import pallas as pl
from jax.experimental.pallas import tpu as pltpu
from jax.sharding import PartitionSpec as P

HEAD_DIM = 128
HALF = HEAD_DIM // 2
NEG_BIG = -1e30
BATCH = 8
SEQ_LOC = 192
SEQ_LEN = 1536
D_MODEL = 2048
SHARD = 256
FF_LOC = 1024
ROWS = 2 * SEQ_LOC
TAB_ROWS = SEQ_LEN + 8
MESH = pl.DeviceIdType.MESH
BF = jnp.bfloat16
F32 = jnp.float32
SCALE = HEAD_DIM ** -0.5


def rope_table():
    inv_freq = np.float32(10000.0) ** (np.float32(-2.0) * np.arange(HALF, dtype=np.float32) / np.float32(HEAD_DIM))
    angles = np.arange(TAB_ROWS, dtype=np.float32)[:, None] * inv_freq.astype(np.float32)
    return np.concatenate([np.cos(angles), np.sin(angles)], axis=-1).astype(np.float32)


def norm_rows(x, gain):
    inv = lax.rsqrt(jnp.mean(x * x, axis=-1, keepdims=True) + 1e-5)
    return (x * inv * gain.astype(F32)).astype(BF)


def spread(tab):
    swapped = pltpu.roll(tab, HALF, 1)
    low = lax.broadcasted_iota(jnp.int32, tab.shape, 1) < HALF
    return jnp.where(low, tab, swapped), jnp.where(low, -swapped, tab)


def rotate(a, c, s):
    return a * c + pltpu.roll(a, HALF, 1) * s


def layer_kernel(lens, prompt, new_tok, gain_a, gain_m, table, wq, wk, wv, wo, wg, wu, wd,
                 kv_out, new_out, dec_out, last_out,
                 xbuf, xrecv, wbuf, wqb, wob, wgb, wub, wdb, tab, tmp, stage,
                 lastf, lsend, lrecv, rows, qall, part, precv, kself, vself, attn, flat,
                 psend, rrecv, hid, norm2,
                 lsem, xsem, ysend, yrecv, wsend, wrecv, osend, orecv,
                 l_s, l_r, q_s, q_r, p_s, p_r, r_s, r_r, a_s, a_r):
    rep = lax.axis_index('replica')
    me = lax.axis_index('model')
    core = lax.rem(me, 2)
    xpos = lax.rem(me // 2, 2)
    ypos = me // 4
    flips = (1 - 2 * core, 2 - 4 * xpos, 4 - 8 * ypos)
    near = [me + sum(f for i, f in enumerate(flips) if d >> i & 1) for d in range(8)]
    sib, xnb, xsb, ynb = near[1], near[2], near[3], near[4]
    znb = 1 - rep

    barrier = pltpu.get_barrier_semaphore()
    for peer in [(rep, near[d]) for d in range(1, 8)] + [(znb, me)]:
        pl.semaphore_signal(barrier, inc=1, device_id=peer, device_id_type=MESH)
    pl.semaphore_wait(barrier, 8)

    def remote(src, dst, send, recv, peer):
        return pltpu.make_async_remote_copy(src_ref=src, dst_ref=dst, send_sem=send, recv_sem=recv, device_id=peer, device_id_type=MESH)

    def y_copy(b):
        return remote(prompt.at[b], xrecv.at[b], ysend.at[b], yrecv.at[b], (rep, ynb))

    def x_load(b):
        return pltpu.make_async_copy(prompt.at[b], xbuf.at[b], xsem.at[b])

    loads = [pltpu.make_async_copy(a, b, lsem.at[i]) for i, (a, b) in enumerate((
        (wk.at[0], wbuf.at[0, 0]), (wv.at[0], wbuf.at[0, 1]), (table, tab), (wq.at[0], wqb), (wo.at[0], wob),
        (wg.at[0], wgb), (wu.at[0], wub), (wd.at[0], wdb)))]
    for i, w in enumerate((wk, wv)):
        @pl.when(rep == i)
        def _():
            remote(w.at[0], wbuf.at[2, rep], wsend.at[0], wrecv.at[0], (rep, xnb)).start()

    y_copy(0).start()
    loads[0].start()
    loads[1].start()

    @pl.loop(0, BATCH)
    def _(b):
        x_load(b).start()

    for load in loads[2:]:
        load.start()
    w_x = remote(wbuf.at[0, rep], wbuf.at[2, rep], wsend.at[0], wrecv.at[0], (rep, xnb))
    w_s = remote(wbuf.at[0], wbuf.at[1], wsend.at[1], wrecv.at[1], (rep, sib))
    w_z = remote(wbuf.at[2, rep], wbuf.at[2, rep], wsend.at[2], wrecv.at[2], (znb, me))
    w_xs = remote(wbuf.at[2, rep], wbuf.at[3, rep], wsend.at[3], wrecv.at[3], (rep, sib))
    w_zs = remote(wbuf.at[2, znb], wbuf.at[3, znb], wsend.at[4], wrecv.at[4], (rep, sib))
    loads[0].wait()
    loads[1].wait()
    w_s.start()

    def out_copy(s, b, o, kv):
        blk = me if s == 0 else ynb
        dst = kv_out.at[kv, b, pl.ds(pl.multiple_of(blk * ROWS, ROWS), ROWS), :]
        src = stage.at[s, b, o - 1, kv]
        return remote(src, dst, osend.at[o - 1, s, b, kv], orecv.at[o - 1, s, b, kv], (rep, near[o]))

    def own_two(b, o, kv):
        dst = kv_out.at[kv, pl.ds(b, 2), pl.ds(pl.multiple_of(me * ROWS, ROWS), ROWS), :]
        return remote(stage.at[0, pl.ds(b, 2), o - 1, kv], dst, osend.at[o - 1, 0, b, kv], orecv.at[o - 1, 0, b, kv], (rep, near[o]))

    def chunk_kv(b, o):
        dst = kv_out.at[:, b, pl.ds(pl.multiple_of(ynb * ROWS, ROWS), ROWS), :]
        return remote(stage.at[1, b, o - 1], dst, osend.at[o - 1, 1, b, 0], orecv.at[o - 1, 1, b, 0], (rep, near[o]))

    def project(buf, s, b, o, kv):
        acc = jnp.dot(buf[b], wbuf[o, kv], preferred_element_type=F32)
        blk = me if s == 0 else ynb
        c, sn = spread(tab[pl.ds(pl.multiple_of(blk * SEQ_LOC, SEQ_LOC), SEQ_LOC), :])
        is_k = kv == 0
        c = jnp.where(is_k, c, 1.0)
        sn = jnp.where(is_k, sn, 0.0)
        for h in range(2):
            tmp[pl.ds(h, SEQ_LOC, stride=2), :] = rotate(acc[:, h * HEAD_DIM:(h + 1) * HEAD_DIM], c, sn)
        if o == 0:
            kv_out[kv, b, pl.ds(pl.multiple_of(blk * ROWS, ROWS), ROWS), :] = tmp[...].astype(BF)
        else:
            stage[s, b, o - 1, kv] = tmp[...].astype(BF)

    @pl.loop(0, BATCH)
    def _(b):
        x_load(b).wait()
        x = xbuf[b].astype(F32)
        here = me * SEQ_LOC + lax.broadcasted_iota(jnp.int32, (SEQ_LOC, 1), 0) == lens[b] - 1
        lastf[pl.ds(b, 1), :] = jnp.sum(jnp.where(here, x, 0.0), axis=0, keepdims=True)
        xbuf[b] = norm_rows(x, gain_a[...])

    l_copy = [remote(lsend.at[i], lrecv.at[i], l_s.at[i], l_r.at[i], (rep, near[d])) for i, d in enumerate((4, 1, 2))]
    lsend[0] = lastf[...].astype(BF)
    loads[2].wait()
    l_copy[0].start()

    @pl.loop(1, BATCH)
    def _(b):
        y_copy(b).start()

    @pl.loop(0, BATCH)
    def _(b):
        @pl.loop(0, 2)
        def _(kv):
            project(xbuf, 0, b, 0, kv)

    def join_last(i):
        l_copy[i].wait_recv()
        return (lsend[i].astype(F32) + lrecv[i].astype(F32)).astype(BF)

    lsend[1] = join_last(0)
    w_s.wait_recv()
    l_copy[1].start()

    @pl.loop(0, BATCH)
    def _(b):
        @pl.loop(0, 2)
        def _(kv):
            project(xbuf, 0, b, 1, kv)
            out_copy(0, b, 1, kv).start()

    lsend[2] = join_last(1)

    w_x.wait_recv()
    w_z.start()
    w_xs.start()
    l_copy[2].start()

    def own_x_phase(kv, o):
        @pl.loop(0, BATCH, step=2)
        def _(b):
            project(xbuf, 0, b, o, kv)
            project(xbuf, 0, b + 1, o, kv)
            own_two(b, o, kv).start()

    own_x_phase(rep, 2)
    w_xs.wait_recv()
    own_x_phase(rep, 3)

    rows[0:BATCH, :] = new_tok[...].astype(F32)
    rows[BATCH:2 * BATCH, :] = join_last(2).astype(F32)
    loads[3].wait()
    n16 = norm_rows(rows[...], gain_a[...])
    q16 = jnp.dot(n16, wqb[...], preferred_element_type=F32)
    k16 = jnp.dot(n16, wbuf[0, 0], preferred_element_type=F32)
    v16 = jnp.dot(n16, wbuf[0, 1], preferred_element_type=F32)
    for b in range(BATCH):
        flat[pl.ds(b, 1), 0:HEAD_DIM] = tab[pl.ds(jnp.clip(lens[b], 0, SEQ_LEN), 1), :]
        flat[pl.ds(BATCH + b, 1), 0:HEAD_DIM] = tab[pl.ds(jnp.clip(lens[b] - 1, 0, SEQ_LEN), 1), :]
    c16, s16 = spread(flat[:, 0:HEAD_DIM])
    kself[...] = jnp.zeros_like(kself)
    vself[...] = jnp.zeros_like(vself)
    for h in range(2):
        lanes = slice(h * HEAD_DIM, (h + 1) * HEAD_DIM)
        qh = rotate(q16[:, lanes], c16, s16).astype(BF).astype(F32)
        kh = rotate(k16[:, lanes], c16, s16)[:BATCH].astype(BF).astype(F32)
        vh = v16[:BATCH, lanes].astype(BF).astype(F32)
        for g in range(2):
            qall[0, :, 2 * g + h, :] = qh[g * BATCH:(g + 1) * BATCH]
        kself[:, h, :] = kh
        vself[:, h, :] = vh
        tmp[pl.ds(h, BATCH, stride=2), :] = kh
        tmp[pl.ds(2 * BATCH + h, BATCH, stride=2), :] = vh
    new_out[0] = tmp[0:2 * BATCH, :].astype(BF)
    new_out[1] = tmp[2 * BATCH:4 * BATCH, :].astype(BF)
    low = lax.broadcasted_iota(jnp.int32, (4, HEAD_DIM), 1) < HALF
    part[:, 0] = jnp.zeros((4, BATCH, 4, HEAD_DIM), F32)
    part[:, 1] = jnp.broadcast_to(jnp.where(low, NEG_BIG, 0.0), (4, BATCH, 4, HEAD_DIM))
    q_copy = [remote(qall.at[0], qall.at[d], q_s.at[d - 1], q_r.at[d - 1], (rep, near[d])) for d in (1, 2, 3)]
    for c in q_copy:
        c.start()

    w_z.wait_recv()
    w_zs.start()
    w_zs.wait_recv()
    own_x_phase(znb, 2)
    own_x_phase(znb, 3)
    for c in q_copy:
        c.wait_recv()

    lane = lax.broadcasted_iota(jnp.int32, (4, ROWS), 1)
    same_head = lane % 2 == lax.broadcasted_iota(jnp.int32, (4, ROWS), 0) % 2

    def attend(s, b):
        blk = me if s == 0 else ynb
        seen = same_head & (blk * SEQ_LOC + lane // 2 < lens[b])
        four = range(4)
        mine = pl.ds(pl.multiple_of(blk * ROWS, ROWS), ROWS)
        keys, vals = ([kv_out[kv, b, mine, :]] + [stage[s, b, o - 1, kv] for o in (1, 2, 3)] for kv in range(2))
        old = [part[o, 1, b] for o in four]
        acc = [part[o, 0, b] for o in four]
        sc = [lax.dot_general(qall[o, b].astype(BF), keys[o], (((1,), (1,)), ((), ())), preferred_element_type=F32) for o in four]
        sc = [jnp.where(seen, x * SCALE, NEG_BIG) for x in sc]
        top = [jnp.maximum(old[o][:, 0:1], jnp.max(sc[o], axis=-1, keepdims=True)) for o in four]
        p = [jnp.where(seen, jnp.exp(sc[o] - top[o]), 0.0) for o in four]
        fade = [jnp.exp(old[o][:, 0:1] - top[o]) for o in four]
        den = [old[o][:, HALF:HALF + 1] * fade[o] + jnp.sum(p[o], axis=-1, keepdims=True) for o in four]
        add = [jnp.dot(p[o].astype(BF), vals[o], preferred_element_type=F32) for o in four]
        for o in four:
            part[o, 0, b] = acc[o] * fade[o] + add[o]
            part[o, 1, b] = jnp.where(low, top[o], den[o])

    waiting = [(b, kv, o) for b in range(6, BATCH) for kv in range(2) for o in (2, 3)]

    def leave(b, kv, o):
        out_copy(1, b, o, kv).start()

    @pl.loop(0, BATCH)
    def _(b):
        attend(0, b)
        y_copy(b).wait_recv()

        xrecv[b] = norm_rows(xrecv[b].astype(F32), gain_a[...])

        @pl.loop(0, 2)
        def _(kv):
            for o in (2, 3):
                project(xrecv, 1, b, o, kv)

                @pl.when((b < 6) & (kv == 1))
                def _():
                    chunk_kv(b, o).start()

            project(xrecv, 1, b, 1, kv)
            out_copy(1, b, 1, kv).start()
            project(xrecv, 1, b, 0, kv)

        attend(1, b)

    p_copy = [remote(part.at[d], precv.at[d - 1], p_s.at[d - 1], p_r.at[d - 1], (rep, near[d])) for d in (1, 2, 3)]
    for c in p_copy:
        c.start()
    for c in p_copy:
        c.wait_send()
    for job in waiting[0:2]:
        leave(*job)
    for load in loads[4:]:
        load.wait()
    first = lax.broadcasted_iota(jnp.int32, (BATCH, 4, 1), 1) < 2
    s_self = jnp.where(first, jnp.sum(qall[0] * kself[...], axis=-1, keepdims=True) * SCALE, NEG_BIG)
    for c in p_copy:
        c.wait_recv()
    accs = [part[0, 0]] + [precv[i, 0] for i in range(3)]
    stats = [part[0, 1]] + [precv[i, 1] for i in range(3)]
    tops = [st[:, :, 0:1] for st in stats]
    top = s_self
    for t in tops:
        top = jnp.maximum(top, t)
    e_self = jnp.where(first, jnp.exp(s_self - top), 0.0)
    den = e_self
    num = e_self * vself[...]
    for t, st, ac in zip(tops, stats, accs):
        e = jnp.exp(t - top)
        den = den + e * st[:, :, HALF:HALF + 1]
        num = num + e * ac
    attn[...] = num / den
    for g in range(2):
        for h in range(2):
            flat[g * BATCH:(g + 1) * BATCH, h * HEAD_DIM:(h + 1) * HEAD_DIM] = attn[:, 2 * g + h, :]

    def reduce_columns(i, base, jobs):
        sends = [remote(psend.at[i, near[d]], rrecv.at[i, d - 1], r_s.at[i, d - 1], r_r.at[i, d - 1], (rep, near[d])) for d in range(1, 8)]
        for c in sends:
            c.start()
        for c in sends:
            c.wait_send()
        for job in jobs[0]:
            leave(*job)
        total = psend[i, me]
        for d in range(1, 8):
            sends[d - 1].wait_recv()
            total = total + rrecv[i, d - 1]
        hid[i, me] = (base + total).astype(BF)
        gets = [remote(hid.at[i, me], hid.at[i, me], a_s.at[i, d - 1], a_r.at[i, d - 1], (rep, near[d])) for d in range(1, 8)]
        for c in gets:
            c.start()
        for c in gets:
            c.wait_send()
        for job in jobs[1]:
            leave(*job)
        for d in range(1, 8):
            remote(hid.at[i, near[d]], hid.at[i, near[d]], a_s.at[i, d - 1], a_r.at[i, d - 1], (rep, near[d])).wait_recv()

    a16 = flat[...].astype(BF)
    for j in range(8):
        psend[0, j] = jnp.dot(a16, wob[:, j * SHARD:(j + 1) * SHARD], preferred_element_type=F32)
    mine = pl.ds(pl.multiple_of(me * SHARD, SHARD), SHARD)
    reduce_columns(0, rows[:, mine], (waiting[2:3], waiting[3:6]))

    sq = jnp.zeros((2 * BATCH, 1), F32)
    for j in range(8):
        hj = hid[0, j].astype(F32)
        sq = sq + jnp.sum(hj * hj, axis=-1, keepdims=True)
    inv = lax.rsqrt(sq / D_MODEL + 1e-5)
    for j in range(8):
        cols = slice(j * SHARD, (j + 1) * SHARD)
        norm2[:, cols] = (hid[0, j].astype(F32) * inv * gain_m[:, cols].astype(F32)).astype(BF)
    n2 = norm2[...]
    gate = jnp.dot(n2, wgb[...], preferred_element_type=F32)
    up = jnp.dot(n2, wub[...], preferred_element_type=F32)
    mid = (gate * jax.nn.sigmoid(gate) * up).astype(BF)
    for j in range(8):
        psend[1, j] = jnp.dot(mid, wdb[:, j * SHARD:(j + 1) * SHARD], preferred_element_type=F32)
    reduce_columns(1, hid[0, me].astype(F32), (waiting[6:7], waiting[7:8]))
    for j in range(8):
        cols = slice(j * SHARD, (j + 1) * SHARD)
        dec_out[:, cols] = hid[1, j][:BATCH]
        last_out[:, cols] = hid[1, j][BATCH:]

    for c in [w_x, w_s, w_z, w_xs, w_zs] + l_copy + q_copy:
        c.wait_send()

    @pl.loop(0, BATCH)
    def _(b):
        y_copy(b).wait_send()
        for kv in range(2):
            for s in range(2):
                out_copy(s, b, 1, kv).wait()

    for o in (2, 3):
        @pl.loop(0, BATCH, step=2)
        def _(b):
            for kv in range(2):
                own_two(b, o, kv).wait()

        @pl.loop(0, 6)
        def _(b):
            chunk_kv(b, o).wait()

    for b, kv, o in waiting:
        out_copy(1, b, o, kv).wait()


def layer(lens, prompt, new_tok, gain_a, gain_m, table, wq, wk, wv, wo, wg, wu, wd):
    vmem = pl.BlockSpec(memory_space=pltpu.VMEM)
    anym = pl.BlockSpec(memory_space=pl.ANY)
    dma = pltpu.SemaphoreType.DMA
    v = pltpu.VMEM
    return pl.pallas_call(
        layer_kernel,
        out_shape=(
            pltpu.VMEM((2, BATCH, 8 * ROWS, HEAD_DIM), BF),
            pltpu.VMEM((2, 2 * BATCH, HEAD_DIM), BF),
            pltpu.VMEM((BATCH, D_MODEL), BF),
            pltpu.VMEM((BATCH, D_MODEL), BF),
        ),
        in_specs=[pl.BlockSpec(memory_space=pltpu.SMEM), anym, vmem, vmem, vmem] + [anym] * 8,
        out_specs=(vmem, vmem, vmem, vmem),
        scratch_shapes=[
            v((BATCH, SEQ_LOC, D_MODEL), BF), v((BATCH, SEQ_LOC, D_MODEL), BF), v((4, 2, D_MODEL, SHARD), BF),
            v((D_MODEL, SHARD), BF), v((SHARD, D_MODEL), BF), v((D_MODEL, FF_LOC), BF), v((D_MODEL, FF_LOC), BF), v((FF_LOC, D_MODEL), BF),
            v((TAB_ROWS, HEAD_DIM), F32), v((ROWS, HEAD_DIM), F32), v((2, BATCH, 3, 2, ROWS, HEAD_DIM), BF),
            v((BATCH, D_MODEL), F32), v((3, BATCH, D_MODEL), BF), v((3, BATCH, D_MODEL), BF), v((2 * BATCH, D_MODEL), F32),
            v((4, BATCH, 4, HEAD_DIM), F32), v((4, 2, BATCH, 4, HEAD_DIM), F32), v((3, 2, BATCH, 4, HEAD_DIM), F32),
            v((BATCH, 4, HEAD_DIM), F32), v((BATCH, 4, HEAD_DIM), F32), v((BATCH, 4, HEAD_DIM), F32), v((2 * BATCH, SHARD), F32),
            v((2, 8, 2 * BATCH, SHARD), F32), v((2, 7, 2 * BATCH, SHARD), F32), v((2, 8, 2 * BATCH, SHARD), BF), v((2 * BATCH, D_MODEL), BF),
            dma((8,)), dma((BATCH,)), dma((BATCH,)), dma((BATCH,)), dma((5,)), dma((5,)),
            dma((3, 2, BATCH, 2)), dma((3, 2, BATCH, 2)),
            dma((3,)), dma((3,)), dma((3,)), dma((3,)), dma((3,)), dma((3,)),
            dma((2, 7)), dma((2, 7)), dma((2, 7)), dma((2, 7)),
        ],
        compiler_params=pltpu.CompilerParams(collective_id=0, has_side_effects=True, vmem_limit_bytes=49 * 1024 * 1024),
        cost_estimate=pl.CostEstimate(flops=26_000_000_000, bytes_accessed=60_000_000, transcendentals=0),
        name='layer',
    )(lens, prompt, new_tok, gain_a, gain_m, table, wq, wk, wv, wo, wg, wu, wd)


def cache_kernel(kv, new, dec, last, key_out, val_out, dec_out, last_out, store, row_sem):
    outs = (key_out, val_out)
    puts = []
    for i in range(2):
        for b in range(BATCH):
            puts.append(pltpu.make_async_copy(kv.at[i, b], outs[i].at[0, b, pl.ds(0, SEQ_LEN)], store.at[i, b]))
            puts[-1].start()
    for i in range(2):
        puts.append(pltpu.make_async_copy(new.at[i], outs[i].at[0, :, pl.ds(SEQ_LEN, 1)], row_sem.at[i]))
        puts[-1].start()
    dec_out[...] = dec[...]
    last_out[...] = last[...]
    for c in puts:
        c.wait()


def caches(kv, new, dec, last):
    anym = pl.BlockSpec(memory_space=pl.ANY)
    dma = pltpu.SemaphoreType.DMA
    vmem = pl.BlockSpec(memory_space=pltpu.VMEM)
    shape = jax.ShapeDtypeStruct((1, BATCH, SEQ_LEN + 1, 2, HEAD_DIM), BF)
    row = jax.ShapeDtypeStruct((BATCH, D_MODEL), BF)
    return pl.pallas_call(
        cache_kernel,
        out_shape=(shape, shape, row, row),
        in_specs=[anym, anym, vmem, vmem],
        out_specs=(anym, anym, vmem, vmem),
        scratch_shapes=[dma((2, BATCH)), dma((2,))],
        compiler_params=pltpu.CompilerParams(vmem_limit_bytes=4 * 1024 * 1024),
        cost_estimate=pl.CostEstimate(flops=0, bytes_accessed=13_000_000, transcendentals=0),
        name='caches',
    )(kv, new, dec, last)


def solution(mesh):
    seq_spec = P('replica', 'model', None)
    col_spec = P(None, None, 'model')
    row_spec = P(None, 'model', None)
    gain_spec = P(None, None)
    tok_spec = P('replica', None)
    cache_spec = P(None, 'replica', None, 'model', None)
    in_specs = (seq_spec, P('replica'), tok_spec, gain_spec, col_spec, col_spec, col_spec, row_spec, gain_spec, col_spec, col_spec, row_spec)
    out_specs = (tok_spec, tok_spec, cache_spec, cache_spec)
    table = rope_table()

    def per_device(prompt, lengths, new_tok, norm_attn, w_q, w_k, w_v, w_o, norm_mlp, w_gate, w_up, w_down):
        kv, new, dec, last = layer(lengths, prompt, new_tok, norm_attn, norm_mlp, jnp.asarray(table), w_q, w_k, w_v, w_o, w_gate, w_up, w_down)
        keys, vals, dec, last = caches(kv.reshape(2, BATCH, SEQ_LEN, 2, HEAD_DIM), new.reshape(2, BATCH, 1, 2, HEAD_DIM), dec, last)
        return dec, last, keys, vals

    return jax.shard_map(per_device, mesh=mesh, in_specs=in_specs, out_specs=out_specs, check_vma=False)
```

```python
import jax
import jax.numpy as jnp
import numpy as np
from jax import lax
from jax.experimental import pallas as pl
from jax.experimental.pallas import tpu as pltpu
from jax.sharding import PartitionSpec as P

HEAD_DIM = 128
HALF = HEAD_DIM // 2
NEG_BIG = -1e30
BATCH = 8
SEQ_LOC = 192
SEQ_LEN = 1536
D_MODEL = 2048
SHARD = 256
FF_LOC = 1024
ROWS = 2 * SEQ_LOC
TAB_ROWS = SEQ_LEN + 8
MESH = pl.DeviceIdType.MESH
BF = jnp.bfloat16
F32 = jnp.float32
SCALE = HEAD_DIM ** -0.5


def rope_table():
    inv_freq = np.float32(10000.0) ** (np.float32(-2.0) * np.arange(HALF, dtype=np.float32) / np.float32(HEAD_DIM))
    angles = np.arange(TAB_ROWS, dtype=np.float32)[:, None] * inv_freq.astype(np.float32)
    return np.concatenate([np.cos(angles), np.sin(angles)], axis=-1).astype(np.float32)


def norm_rows(x, gain):
    inv = lax.rsqrt(jnp.mean(x * x, axis=-1, keepdims=True) + 1e-5)
    return (x * inv * gain.astype(F32)).astype(BF)


def spread(tab):
    swapped = pltpu.roll(tab, HALF, 1)
    low = lax.broadcasted_iota(jnp.int32, tab.shape, 1) < HALF
    return jnp.where(low, tab, swapped), jnp.where(low, -swapped, tab)


def rotate(a, c, s):
    return a * c + pltpu.roll(a, HALF, 1) * s


def layer_kernel(lens, prompt, new_tok, gain_a, gain_m, table, wq, wk, wv, wo, wg, wu, wd,
                 kv_out, new_out, dec_out, last_out,
                 xbuf, xrecv, wbuf, wqb, wob, wgb, wub, wdb, tab, tmp, stage,
                 lastf, lsend, lrecv, rows, qall, part, precv, kself, vself, attn, flat,
                 psend, rrecv, rsum, base2, hid, norm2,
                 lsem, xsem, ysend, yrecv, wsend, wrecv, osend, orecv,
                 l_s, l_r, q_s, q_r, p_s, p_r, r_s, r_r, a_s, a_r):
    rep = lax.axis_index('replica')
    me = lax.axis_index('model')
    core = lax.rem(me, 2)
    xpos = lax.rem(me // 2, 2)
    ypos = me // 4
    flips = (1 - 2 * core, 2 - 4 * xpos, 4 - 8 * ypos)
    near = [me + sum(f for i, f in enumerate(flips) if d >> i & 1) for d in range(8)]
    sib, xnb, xsb, ynb = near[1], near[2], near[3], near[4]
    znb = 1 - rep

    barrier = pltpu.get_barrier_semaphore()
    for peer in [(rep, near[d]) for d in range(1, 8)] + [(znb, me)]:
        pl.semaphore_signal(barrier, inc=1, device_id=peer, device_id_type=MESH)
    pl.semaphore_wait(barrier, 8)

    def remote(src, dst, send, recv, peer):
        return pltpu.make_async_remote_copy(src_ref=src, dst_ref=dst, send_sem=send, recv_sem=recv, device_id=peer, device_id_type=MESH)

    def y_copy(b):
        return remote(prompt.at[b], xrecv.at[b], ysend.at[b], yrecv.at[b], (rep, ynb))

    def x_load(b):
        return pltpu.make_async_copy(prompt.at[b], xbuf.at[b], xsem.at[b])

    loads = [pltpu.make_async_copy(a, b, lsem.at[i]) for i, (a, b) in enumerate((
        (wk.at[0], wbuf.at[0, 0]), (wv.at[0], wbuf.at[0, 1]), (table, tab), (wq.at[0], wqb), (wo.at[0], wob),
        (wg.at[0], wgb), (wu.at[0], wub), (wd.at[0], wdb)))]
    for i, w in enumerate((wk, wv)):
        @pl.when(rep == i)
        def _():
            remote(w.at[0], wbuf.at[2, rep], wsend.at[0], wrecv.at[0], (rep, xnb)).start()

    y_copy(0).start()
    loads[0].start()
    loads[1].start()

    @pl.loop(0, BATCH)
    def _(b):
        x_load(b).start()

    for load in loads[2:]:
        load.start()
    w_x = remote(wbuf.at[0, rep], wbuf.at[2, rep], wsend.at[0], wrecv.at[0], (rep, xnb))
    w_s = remote(wbuf.at[0], wbuf.at[1], wsend.at[1], wrecv.at[1], (rep, sib))
    w_z = remote(wbuf.at[2, rep], wbuf.at[2, rep], wsend.at[2], wrecv.at[2], (znb, me))
    w_xs = remote(wbuf.at[2, rep], wbuf.at[3, rep], wsend.at[3], wrecv.at[3], (rep, sib))
    w_zs = remote(wbuf.at[2, znb], wbuf.at[3, znb], wsend.at[4], wrecv.at[4], (rep, sib))
    loads[0].wait()
    loads[1].wait()
    w_s.start()

    def out_copy(s, b, o, kv):
        blk = me if s == 0 else ynb
        dst = kv_out.at[kv, b, pl.ds(pl.multiple_of(blk * ROWS, ROWS), ROWS), :]
        src = stage.at[s, b, o - 1, kv]
        return remote(src, dst, osend.at[o - 1, s, b, kv], orecv.at[o - 1, s, b, kv], (rep, near[o]))

    def own_two(b, o, kv):
        dst = kv_out.at[kv, pl.ds(b, 2), pl.ds(pl.multiple_of(me * ROWS, ROWS), ROWS), :]
        return remote(stage.at[0, pl.ds(b, 2), o - 1, kv], dst, osend.at[o - 1, 0, b, kv], orecv.at[o - 1, 0, b, kv], (rep, near[o]))

    def chunk_kv(b, o):
        dst = kv_out.at[:, b, pl.ds(pl.multiple_of(ynb * ROWS, ROWS), ROWS), :]
        return remote(stage.at[1, b, o - 1], dst, osend.at[o - 1, 1, b, 0], orecv.at[o - 1, 1, b, 0], (rep, near[o]))

    def project(buf, s, b, o, kv):
        acc = jnp.dot(buf[b], wbuf[o, kv], preferred_element_type=F32)
        blk = me if s == 0 else ynb
        c, sn = spread(tab[pl.ds(pl.multiple_of(blk * SEQ_LOC, SEQ_LOC), SEQ_LOC), :])
        is_k = kv == 0
        c = jnp.where(is_k, c, 1.0)
        sn = jnp.where(is_k, sn, 0.0)
        for h in range(2):
            tmp[pl.ds(h, SEQ_LOC, stride=2), :] = rotate(acc[:, h * HEAD_DIM:(h + 1) * HEAD_DIM], c, sn)
        if o == 0:
            kv_out[kv, b, pl.ds(pl.multiple_of(blk * ROWS, ROWS), ROWS), :] = tmp[...].astype(BF)
        else:
            stage[s, b, o - 1, kv] = tmp[...].astype(BF)

    @pl.loop(0, BATCH)
    def _(b):
        x_load(b).wait()
        x = xbuf[b].astype(F32)
        here = me * SEQ_LOC + lax.broadcasted_iota(jnp.int32, (SEQ_LOC, 1), 0) == lens[b] - 1
        lastf[pl.ds(b, 1), :] = jnp.sum(jnp.where(here, x, 0.0), axis=0, keepdims=True)
        xbuf[b] = norm_rows(x, gain_a[...])

    l_copy = [remote(lsend.at[i], lrecv.at[i], l_s.at[i], l_r.at[i], (rep, near[d])) for i, d in enumerate((4, 1, 2))]
    lsend[0] = lastf[...].astype(BF)
    loads[2].wait()
    l_copy[0].start()

    @pl.loop(1, BATCH)
    def _(b):
        y_copy(b).start()

    @pl.loop(0, BATCH)
    def _(b):
        @pl.loop(0, 2)
        def _(kv):
            project(xbuf, 0, b, 0, kv)

    def join_last(i):
        l_copy[i].wait_recv()
        return (lsend[i].astype(F32) + lrecv[i].astype(F32)).astype(BF)

    lsend[1] = join_last(0)
    w_s.wait_recv()
    l_copy[1].start()

    @pl.loop(0, BATCH)
    def _(b):
        @pl.loop(0, 2)
        def _(kv):
            project(xbuf, 0, b, 1, kv)
            out_copy(0, b, 1, kv).start()

    lsend[2] = join_last(1)

    w_x.wait_recv()
    w_z.start()
    w_xs.start()
    l_copy[2].start()

    def own_x_phase(kv, o):
        @pl.loop(0, BATCH, step=2)
        def _(b):
            project(xbuf, 0, b, o, kv)
            project(xbuf, 0, b + 1, o, kv)
            own_two(b, o, kv).start()

    own_x_phase(rep, 2)
    w_xs.wait_recv()
    own_x_phase(rep, 3)

    rows[0:BATCH, :] = new_tok[...].astype(F32)
    rows[BATCH:2 * BATCH, :] = join_last(2).astype(F32)
    loads[3].wait()
    n16 = norm_rows(rows[...], gain_a[...])
    q16 = jnp.dot(n16, wqb[...], preferred_element_type=F32)
    k16 = jnp.dot(n16, wbuf[0, 0], preferred_element_type=F32)
    v16 = jnp.dot(n16, wbuf[0, 1], preferred_element_type=F32)
    for b in range(BATCH):
        flat[pl.ds(b, 1), 0:HEAD_DIM] = tab[pl.ds(jnp.clip(lens[b], 0, SEQ_LEN), 1), :]
        flat[pl.ds(BATCH + b, 1), 0:HEAD_DIM] = tab[pl.ds(jnp.clip(lens[b] - 1, 0, SEQ_LEN), 1), :]
    c16, s16 = spread(flat[:, 0:HEAD_DIM])
    kself[...] = jnp.zeros_like(kself)
    vself[...] = jnp.zeros_like(vself)
    for h in range(2):
        lanes = slice(h * HEAD_DIM, (h + 1) * HEAD_DIM)
        qh = rotate(q16[:, lanes], c16, s16).astype(BF).astype(F32)
        kh = rotate(k16[:, lanes], c16, s16)[:BATCH].astype(BF).astype(F32)
        vh = v16[:BATCH, lanes].astype(BF).astype(F32)
        for g in range(2):
            qall[0, :, 2 * g + h, :] = qh[g * BATCH:(g + 1) * BATCH]
        kself[:, h, :] = kh
        vself[:, h, :] = vh
        tmp[pl.ds(h, BATCH, stride=2), :] = kh
        tmp[pl.ds(2 * BATCH + h, BATCH, stride=2), :] = vh
    new_out[0] = tmp[0:2 * BATCH, :].astype(BF)
    new_out[1] = tmp[2 * BATCH:4 * BATCH, :].astype(BF)
    low = lax.broadcasted_iota(jnp.int32, (4, HEAD_DIM), 1) < HALF
    part[:, 0] = jnp.zeros((4, BATCH, 4, HEAD_DIM), F32)
    part[:, 1] = jnp.broadcast_to(jnp.where(low, NEG_BIG, 0.0), (4, BATCH, 4, HEAD_DIM))
    q_copy = [remote(qall.at[0], qall.at[d], q_s.at[d - 1], q_r.at[d - 1], (rep, near[d])) for d in (1, 2, 3)]
    for c in q_copy:
        c.start()

    w_z.wait_recv()
    w_zs.start()
    w_zs.wait_recv()
    own_x_phase(znb, 2)
    own_x_phase(znb, 3)
    for c in q_copy:
        c.wait_recv()

    lane = lax.broadcasted_iota(jnp.int32, (4, ROWS), 1)
    same_head = lane % 2 == lax.broadcasted_iota(jnp.int32, (4, ROWS), 0) % 2

    def attend(s, b):
        blk = me if s == 0 else ynb
        seen = same_head & (blk * SEQ_LOC + lane // 2 < lens[b])
        four = range(4)
        mine = pl.ds(pl.multiple_of(blk * ROWS, ROWS), ROWS)
        keys, vals = ([kv_out[kv, b, mine, :]] + [stage[s, b, o - 1, kv] for o in (1, 2, 3)] for kv in range(2))
        old = [part[o, 1, b] for o in four]
        acc = [part[o, 0, b] for o in four]
        sc = [lax.dot_general(qall[o, b].astype(BF), keys[o], (((1,), (1,)), ((), ())), preferred_element_type=F32) for o in four]
        sc = [jnp.where(seen, x * SCALE, NEG_BIG) for x in sc]
        top = [jnp.maximum(old[o][:, 0:1], jnp.max(sc[o], axis=-1, keepdims=True)) for o in four]
        p = [jnp.where(seen, jnp.exp(sc[o] - top[o]), 0.0) for o in four]
        fade = [jnp.exp(old[o][:, 0:1] - top[o]) for o in four]
        den = [old[o][:, HALF:HALF + 1] * fade[o] + jnp.sum(p[o], axis=-1, keepdims=True) for o in four]
        add = [jnp.dot(p[o].astype(BF), vals[o], preferred_element_type=F32) for o in four]
        for o in four:
            part[o, 0, b] = acc[o] * fade[o] + add[o]
            part[o, 1, b] = jnp.where(low, top[o], den[o])

    waiting = [(b, kv, o) for b in range(6, BATCH) for kv in range(2) for o in (2, 3)]

    def leave(b, kv, o):
        out_copy(1, b, o, kv).start()

    @pl.loop(0, BATCH)
    def _(b):
        attend(0, b)
        y_copy(b).wait_recv()

        xrecv[b] = norm_rows(xrecv[b].astype(F32), gain_a[...])

        @pl.loop(0, 2)
        def _(kv):
            for o in (2, 3):
                project(xrecv, 1, b, o, kv)

                @pl.when((b < 6) & (kv == 1))
                def _():
                    chunk_kv(b, o).start()

            project(xrecv, 1, b, 1, kv)
            out_copy(1, b, 1, kv).start()
            project(xrecv, 1, b, 0, kv)

        attend(1, b)

    p_copy = [remote(part.at[d], precv.at[d - 1], p_s.at[d - 1], p_r.at[d - 1], (rep, near[d])) for d in (1, 2, 3)]
    for c in p_copy:
        c.start()
    for job in waiting[0:4]:
        leave(*job)
    for load in loads[4:]:
        load.wait()
    first = lax.broadcasted_iota(jnp.int32, (BATCH, 4, 1), 1) < 2
    s_self = jnp.where(first, jnp.sum(qall[0] * kself[...], axis=-1, keepdims=True) * SCALE, NEG_BIG)
    for c in p_copy:
        c.wait_recv()
    accs = [part[0, 0]] + [precv[i, 0] for i in range(3)]
    stats = [part[0, 1]] + [precv[i, 1] for i in range(3)]
    tops = [st[:, :, 0:1] for st in stats]
    top = s_self
    for t in tops:
        top = jnp.maximum(top, t)
    e_self = jnp.where(first, jnp.exp(s_self - top), 0.0)
    den = e_self
    num = e_self * vself[...]
    for t, st, ac in zip(tops, stats, accs):
        e = jnp.exp(t - top)
        den = den + e * st[:, :, HALF:HALF + 1]
        num = num + e * ac
    attn[...] = num / den
    for g in range(2):
        for h in range(2):
            flat[g * BATCH:(g + 1) * BATCH, h * HEAD_DIM:(h + 1) * HEAD_DIM] = attn[:, 2 * g + h, :]

    def quarter(flip):
        yy, cc = (ypos, 1 - ypos)[flip >> 2], (core, 1 - core)[flip & 1]
        return pl.ds(4 * yy + 2 * cc, 2)

    side = (1, 4, 5)

    def reduce_columns(i, base, jobs):
        sends = [remote(psend.at[i, quarter(d)], rrecv.at[i, k], r_s.at[i, k], r_r.at[i, k], (rep, near[d])) for k, d in enumerate(side)]
        for c in sends:
            c.start()
        total = psend[i, quarter(0)]
        for k in range(3):
            sends[k].wait_recv()
            total = total + rrecv[i, k]
        rsum[i] = total
        cross = remote(rsum.at[i], rrecv.at[i, 3], r_s.at[i, 3], r_r.at[i, 3], (rep, xnb))
        cross.start()
        for job in jobs:
            leave(*job)
        cross.wait_recv()
        total = total + rrecv[i, 3]
        hid[i, quarter(0)] = (base + total).astype(BF)
        gets = [remote(hid.at[i, quarter(0)], hid.at[i, quarter(0)], a_s.at[i, k], a_r.at[i, k], (rep, near[d])) for k, d in enumerate(side)]
        for c in gets:
            c.start()
        for k, d in enumerate(side):
            remote(hid.at[i, quarter(d)], hid.at[i, quarter(d)], a_s.at[i, k], a_r.at[i, k], (rep, near[d])).wait_recv()
        return sends + [cross] + gets

    a16 = flat[...].astype(BF)
    for j in range(8):
        psend[0, j] = jnp.dot(a16, wob[:, j * SHARD:(j + 1) * SHARD], preferred_element_type=F32)
    for k in range(2):
        cols = pl.ds(pl.multiple_of((4 * ypos + 2 * core + k) * SHARD, SHARD), SHARD)
        base2[k] = rows[:, cols]
    done = reduce_columns(0, base2[...], waiting[4:8])

    sq = jnp.zeros((2 * BATCH, 1), F32)
    for j in range(8):
        hj = hid[0, j].astype(F32)
        sq = sq + jnp.sum(hj * hj, axis=-1, keepdims=True)
    inv = lax.rsqrt(sq / D_MODEL + 1e-5)
    for j in range(8):
        cols = slice(j * SHARD, (j + 1) * SHARD)
        norm2[:, cols] = (hid[0, j].astype(F32) * inv * gain_m[:, cols].astype(F32)).astype(BF)
    n2 = norm2[...]
    gate = jnp.dot(n2, wgb[...], preferred_element_type=F32)
    up = jnp.dot(n2, wub[...], preferred_element_type=F32)
    mid = (gate * jax.nn.sigmoid(gate) * up).astype(BF)
    for j in range(8):
        psend[1, j] = jnp.dot(mid, wdb[:, j * SHARD:(j + 1) * SHARD], preferred_element_type=F32)
    done += reduce_columns(1, hid[0, quarter(0)].astype(F32), ())
    for j in range(8):
        cols = slice(j * SHARD, (j + 1) * SHARD)
        dec_out[:, cols] = hid[1, j][:BATCH]
        last_out[:, cols] = hid[1, j][BATCH:]

    for c in [w_x, w_s, w_z, w_xs, w_zs] + l_copy + q_copy + p_copy + done:
        c.wait_send()

    @pl.loop(0, BATCH)
    def _(b):
        y_copy(b).wait_send()
        for kv in range(2):
            for s in range(2):
                out_copy(s, b, 1, kv).wait()

    for o in (2, 3):
        @pl.loop(0, BATCH, step=2)
        def _(b):
            for kv in range(2):
                own_two(b, o, kv).wait()

        @pl.loop(0, 6)
        def _(b):
            chunk_kv(b, o).wait()

    for b, kv, o in waiting:
        out_copy(1, b, o, kv).wait()


def layer(lens, prompt, new_tok, gain_a, gain_m, table, wq, wk, wv, wo, wg, wu, wd):
    vmem = pl.BlockSpec(memory_space=pltpu.VMEM)
    anym = pl.BlockSpec(memory_space=pl.ANY)
    dma = pltpu.SemaphoreType.DMA
    v = pltpu.VMEM
    return pl.pallas_call(
        layer_kernel,
        out_shape=(
            pltpu.VMEM((2, BATCH, 8 * ROWS, HEAD_DIM), BF),
            pltpu.VMEM((2, 2 * BATCH, HEAD_DIM), BF),
            pltpu.VMEM((BATCH, D_MODEL), BF),
            pltpu.VMEM((BATCH, D_MODEL), BF),
        ),
        in_specs=[pl.BlockSpec(memory_space=pltpu.SMEM), anym, vmem, vmem, vmem] + [anym] * 8,
        out_specs=(vmem, vmem, vmem, vmem),
        scratch_shapes=[
            v((BATCH, SEQ_LOC, D_MODEL), BF), v((BATCH, SEQ_LOC, D_MODEL), BF), v((4, 2, D_MODEL, SHARD), BF),
            v((D_MODEL, SHARD), BF), v((SHARD, D_MODEL), BF), v((D_MODEL, FF_LOC), BF), v((D_MODEL, FF_LOC), BF), v((FF_LOC, D_MODEL), BF),
            v((TAB_ROWS, HEAD_DIM), F32), v((ROWS, HEAD_DIM), F32), v((2, BATCH, 3, 2, ROWS, HEAD_DIM), BF),
            v((BATCH, D_MODEL), F32), v((3, BATCH, D_MODEL), BF), v((3, BATCH, D_MODEL), BF), v((2 * BATCH, D_MODEL), F32),
            v((4, BATCH, 4, HEAD_DIM), F32), v((4, 2, BATCH, 4, HEAD_DIM), F32), v((3, 2, BATCH, 4, HEAD_DIM), F32),
            v((BATCH, 4, HEAD_DIM), F32), v((BATCH, 4, HEAD_DIM), F32), v((BATCH, 4, HEAD_DIM), F32), v((2 * BATCH, SHARD), F32),
            v((2, 8, 2 * BATCH, SHARD), F32), v((2, 4, 2, 2 * BATCH, SHARD), F32), v((2, 2, 2 * BATCH, SHARD), F32), v((2, 2 * BATCH, SHARD), F32), v((2, 8, 2 * BATCH, SHARD), BF), v((2 * BATCH, D_MODEL), BF),
            dma((8,)), dma((BATCH,)), dma((BATCH,)), dma((BATCH,)), dma((5,)), dma((5,)),
            dma((3, 2, BATCH, 2)), dma((3, 2, BATCH, 2)),
            dma((3,)), dma((3,)), dma((3,)), dma((3,)), dma((3,)), dma((3,)),
            dma((2, 4)), dma((2, 4)), dma((2, 3)), dma((2, 3)),
        ],
        compiler_params=pltpu.CompilerParams(collective_id=0, has_side_effects=True, vmem_limit_bytes=49 * 1024 * 1024),
        cost_estimate=pl.CostEstimate(flops=26_000_000_000, bytes_accessed=60_000_000, transcendentals=0),
        name='layer',
    )(lens, prompt, new_tok, gain_a, gain_m, table, wq, wk, wv, wo, wg, wu, wd)


def cache_kernel(kv, new, dec, last, key_out, val_out, dec_out, last_out, store, row_sem):
    outs = (key_out, val_out)
    puts = []
    for i in range(2):
        for b in range(BATCH):
            puts.append(pltpu.make_async_copy(kv.at[i, b], outs[i].at[0, b, pl.ds(0, SEQ_LEN)], store.at[i, b]))
            puts[-1].start()
    for i in range(2):
        puts.append(pltpu.make_async_copy(new.at[i], outs[i].at[0, :, pl.ds(SEQ_LEN, 1)], row_sem.at[i]))
        puts[-1].start()
    dec_out[...] = dec[...]
    last_out[...] = last[...]
    for c in puts:
        c.wait()


def caches(kv, new, dec, last):
    anym = pl.BlockSpec(memory_space=pl.ANY)
    dma = pltpu.SemaphoreType.DMA
    vmem = pl.BlockSpec(memory_space=pltpu.VMEM)
    shape = jax.ShapeDtypeStruct((1, BATCH, SEQ_LEN + 1, 2, HEAD_DIM), BF)
    row = jax.ShapeDtypeStruct((BATCH, D_MODEL), BF)
    return pl.pallas_call(
        cache_kernel,
        out_shape=(shape, shape, row, row),
        in_specs=[anym, anym, vmem, vmem],
        out_specs=(anym, anym, vmem, vmem),
        scratch_shapes=[dma((2, BATCH)), dma((2,))],
        compiler_params=pltpu.CompilerParams(vmem_limit_bytes=4 * 1024 * 1024),
        cost_estimate=pl.CostEstimate(flops=0, bytes_accessed=13_000_000, transcendentals=0),
        name='caches',
    )(kv, new, dec, last)


def solution(mesh):
    seq_spec = P('replica', 'model', None)
    col_spec = P(None, None, 'model')
    row_spec = P(None, 'model', None)
    gain_spec = P(None, None)
    tok_spec = P('replica', None)
    cache_spec = P(None, 'replica', None, 'model', None)
    in_specs = (seq_spec, P('replica'), tok_spec, gain_spec, col_spec, col_spec, col_spec, row_spec, gain_spec, col_spec, col_spec, row_spec)
    out_specs = (tok_spec, tok_spec, cache_spec, cache_spec)
    table = rope_table()

    def per_device(prompt, lengths, new_tok, norm_attn, w_q, w_k, w_v, w_o, norm_mlp, w_gate, w_up, w_down):
        kv, new, dec, last = layer(lengths, prompt, new_tok, norm_attn, norm_mlp, jnp.asarray(table), w_q, w_k, w_v, w_o, w_gate, w_up, w_down)
        keys, vals, dec, last = caches(kv.reshape(2, BATCH, SEQ_LEN, 2, HEAD_DIM), new.reshape(2, BATCH, 1, 2, HEAD_DIM), dec, last)
        return dec, last, keys, vals

    return jax.shard_map(per_device, mesh=mesh, in_specs=in_specs, out_specs=out_specs, check_vma=False)
```

```python
import jax
import jax.numpy as jnp
import numpy as np
from jax import lax
from jax.experimental import pallas as pl
from jax.experimental.pallas import tpu as pltpu
from jax.sharding import PartitionSpec as P

HEAD_DIM = 128
HALF = HEAD_DIM // 2
NEG_BIG = -1e30
BATCH = 8
SEQ_LOC = 192
SEQ_LEN = 1536
D_MODEL = 2048
SHARD = 256
FF_LOC = 1024
ROWS = 2 * SEQ_LOC
TAB_ROWS = SEQ_LEN + 8
MESH = pl.DeviceIdType.MESH
BF = jnp.bfloat16
F32 = jnp.float32
SCALE = HEAD_DIM ** -0.5


def rope_table():
    inv_freq = np.float32(10000.0) ** (np.float32(-2.0) * np.arange(HALF, dtype=np.float32) / np.float32(HEAD_DIM))
    angles = np.arange(TAB_ROWS, dtype=np.float32)[:, None] * inv_freq.astype(np.float32)
    return np.concatenate([np.cos(angles), np.sin(angles)], axis=-1).astype(np.float32)


def norm_rows(x, gain):
    inv = lax.rsqrt(jnp.mean(x * x, axis=-1, keepdims=True) + 1e-5)
    return (x * inv * gain.astype(F32)).astype(BF)


def spread(tab):
    swapped = pltpu.roll(tab, HALF, 1)
    low = lax.broadcasted_iota(jnp.int32, tab.shape, 1) < HALF
    return jnp.where(low, tab, swapped), jnp.where(low, -swapped, tab)


def rotate(a, c, s):
    return a * c + pltpu.roll(a, HALF, 1) * s


def layer_kernel(lens, prompt, new_tok, gain_a, gain_m, table, wq, wk, wv, wo, wg, wu, wd,
                 kv_out, new_out, dec_out, last_out,
                 xbuf, xrecv, wbuf, wqb, wob, wgb, wub, wdb, tab, tmp, stage,
                 lastf, lsend, lrecv, rows, qall, part, precv, kself, vself, attn, flat,
                 psend, rrecv, hid, norm2,
                 lsem, xsem, ysend, yrecv, wsend, wrecv, osend, orecv,
                 l_s, l_r, q_s, q_r, p_s, p_r, r_s, r_r, a_s, a_r):
    rep = lax.axis_index('replica')
    me = lax.axis_index('model')
    core = lax.rem(me, 2)
    xpos = lax.rem(me // 2, 2)
    ypos = me // 4
    flips = (1 - 2 * core, 2 - 4 * xpos, 4 - 8 * ypos)
    near = [me + sum(f for i, f in enumerate(flips) if d >> i & 1) for d in range(8)]
    sib, xnb, xsb, ynb = near[1], near[2], near[3], near[4]
    znb = 1 - rep

    barrier = pltpu.get_barrier_semaphore()
    for peer in [(rep, near[d]) for d in range(1, 8)] + [(znb, me)]:
        pl.semaphore_signal(barrier, inc=1, device_id=peer, device_id_type=MESH)
    pl.semaphore_wait(barrier, 8)

    def remote(src, dst, send, recv, peer):
        return pltpu.make_async_remote_copy(src_ref=src, dst_ref=dst, send_sem=send, recv_sem=recv, device_id=peer, device_id_type=MESH)

    def y_copy(b):
        return remote(prompt.at[b], xrecv.at[b], ysend.at[b], yrecv.at[b], (rep, ynb))

    def x_load(b):
        return pltpu.make_async_copy(prompt.at[b], xbuf.at[b], xsem.at[b])

    loads = [pltpu.make_async_copy(a, b, lsem.at[i]) for i, (a, b) in enumerate((
        (wk.at[0], wbuf.at[0, 0]), (wv.at[0], wbuf.at[0, 1]), (table, tab), (wq.at[0], wqb), (wo.at[0], wob),
        (wg.at[0], wgb), (wu.at[0], wub), (wd.at[0], wdb)))]
    for i, w in enumerate((wk, wv)):
        @pl.when(rep == i)
        def _():
            remote(w.at[0], wbuf.at[2, rep], wsend.at[0], wrecv.at[0], (rep, xnb)).start()

    y_copy(0).start()
    loads[0].start()
    loads[1].start()

    @pl.loop(0, BATCH)
    def _(b):
        x_load(b).start()

    for load in loads[2:]:
        load.start()
    w_x = remote(wbuf.at[0, rep], wbuf.at[2, rep], wsend.at[0], wrecv.at[0], (rep, xnb))
    w_s = remote(wbuf.at[0], wbuf.at[1], wsend.at[1], wrecv.at[1], (rep, sib))
    w_z = remote(wbuf.at[2, rep], wbuf.at[2, rep], wsend.at[2], wrecv.at[2], (znb, me))
    w_xs = remote(wbuf.at[2, rep], wbuf.at[3, rep], wsend.at[3], wrecv.at[3], (rep, sib))
    w_zs = remote(wbuf.at[2, znb], wbuf.at[3, znb], wsend.at[4], wrecv.at[4], (rep, sib))
    loads[0].wait()
    loads[1].wait()
    w_s.start()

    def out_copy(s, b, o, kv):
        blk = me if s == 0 else ynb
        dst = kv_out.at[kv, b, pl.ds(pl.multiple_of(blk * ROWS, ROWS), ROWS), :]
        src = stage.at[s, b, o - 1, kv]
        return remote(src, dst, osend.at[o - 1, s, b, kv], orecv.at[o - 1, s, b, kv], (rep, near[o]))

    def own_two(b, o, kv):
        dst = kv_out.at[kv, pl.ds(b, 2), pl.ds(pl.multiple_of(me * ROWS, ROWS), ROWS), :]
        return remote(stage.at[0, pl.ds(b, 2), o - 1, kv], dst, osend.at[o - 1, 0, b, kv], orecv.at[o - 1, 0, b, kv], (rep, near[o]))

    def chunk_kv(b, o):
        dst = kv_out.at[:, b, pl.ds(pl.multiple_of(ynb * ROWS, ROWS), ROWS), :]
        return remote(stage.at[1, b, o - 1], dst, osend.at[o - 1, 1, b, 0], orecv.at[o - 1, 1, b, 0], (rep, near[o]))

    def project(buf, s, b, o, kv):
        acc = jnp.dot(buf[b], wbuf[o, kv], preferred_element_type=F32)
        blk = me if s == 0 else ynb
        c, sn = spread(tab[pl.ds(pl.multiple_of(blk * SEQ_LOC, SEQ_LOC), SEQ_LOC), :])
        is_k = kv == 0
        c = jnp.where(is_k, c, 1.0)
        sn = jnp.where(is_k, sn, 0.0)
        for h in range(2):
            tmp[pl.ds(h, SEQ_LOC, stride=2), :] = rotate(acc[:, h * HEAD_DIM:(h + 1) * HEAD_DIM], c, sn)
        if o == 0:
            kv_out[kv, b, pl.ds(pl.multiple_of(blk * ROWS, ROWS), ROWS), :] = tmp[...].astype(BF)
        else:
            stage[s, b, o - 1, kv] = tmp[...].astype(BF)

    @pl.loop(0, BATCH)
    def _(b):
        x_load(b).wait()
        here = me * SEQ_LOC + lax.broadcasted_iota(jnp.int32, (SEQ_LOC, 1), 0) == lens[b] - 1
        lastf[pl.ds(b, 1), :] = jnp.sum(jnp.where(here, xbuf[b].astype(F32), 0.0), axis=0, keepdims=True)

    l_copy = [remote(lsend.at[i], lrecv.at[i], l_s.at[i], l_r.at[i], (rep, near[d])) for i, d in enumerate((4, 1, 2))]
    lsend[0] = lastf[...].astype(BF)
    l_copy[0].start()

    @pl.loop(1, BATCH)
    def _(b):
        y_copy(b).start()

    @pl.loop(0, BATCH)
    def _(b):
        xbuf[b] = norm_rows(xbuf[b].astype(F32), gain_a[...])

    def join_last(i):
        l_copy[i].wait_recv()
        return (lsend[i].astype(F32) + lrecv[i].astype(F32)).astype(BF)

    lsend[1] = join_last(0)
    l_copy[1].start()
    loads[2].wait()

    w_x.wait_recv()
    w_z.start()
    w_xs.start()
    lsend[2] = join_last(1)
    l_copy[2].start()

    def own_x_phase(kv, o):
        @pl.loop(0, BATCH, step=2)
        def _(b):
            project(xbuf, 0, b, o, kv)
            project(xbuf, 0, b + 1, o, kv)
            own_two(b, o, kv).start()

    own_x_phase(rep, 2)
    w_xs.wait_recv()
    own_x_phase(rep, 3)

    rows[0:BATCH, :] = new_tok[...].astype(F32)
    rows[BATCH:2 * BATCH, :] = join_last(2).astype(F32)
    loads[3].wait()
    n16 = norm_rows(rows[...], gain_a[...])
    q16 = jnp.dot(n16, wqb[...], preferred_element_type=F32)
    k16 = jnp.dot(n16, wbuf[0, 0], preferred_element_type=F32)
    v16 = jnp.dot(n16, wbuf[0, 1], preferred_element_type=F32)
    for b in range(BATCH):
        flat[pl.ds(b, 1), 0:HEAD_DIM] = tab[pl.ds(jnp.clip(lens[b], 0, SEQ_LEN), 1), :]
        flat[pl.ds(BATCH + b, 1), 0:HEAD_DIM] = tab[pl.ds(jnp.clip(lens[b] - 1, 0, SEQ_LEN), 1), :]
    c16, s16 = spread(flat[:, 0:HEAD_DIM])
    kself[...] = jnp.zeros_like(kself)
    vself[...] = jnp.zeros_like(vself)
    for h in range(2):
        lanes = slice(h * HEAD_DIM, (h + 1) * HEAD_DIM)
        qh = rotate(q16[:, lanes], c16, s16).astype(BF).astype(F32)
        kh = rotate(k16[:, lanes], c16, s16)[:BATCH].astype(BF).astype(F32)
        vh = v16[:BATCH, lanes].astype(BF).astype(F32)
        for g in range(2):
            qall[0, :, 2 * g + h, :] = qh[g * BATCH:(g + 1) * BATCH]
        kself[:, h, :] = kh
        vself[:, h, :] = vh
        tmp[pl.ds(h, BATCH, stride=2), :] = kh
        tmp[pl.ds(2 * BATCH + h, BATCH, stride=2), :] = vh
    new_out[0] = tmp[0:2 * BATCH, :].astype(BF)
    new_out[1] = tmp[2 * BATCH:4 * BATCH, :].astype(BF)
    low = lax.broadcasted_iota(jnp.int32, (4, HEAD_DIM), 1) < HALF
    part[:, 0] = jnp.zeros((4, BATCH, 4, HEAD_DIM), F32)
    part[:, 1] = jnp.broadcast_to(jnp.where(low, NEG_BIG, 0.0), (4, BATCH, 4, HEAD_DIM))
    q_copy = [remote(qall.at[0], qall.at[d], q_s.at[d - 1], q_r.at[d - 1], (rep, near[d])) for d in (1, 2, 3)]
    for c in q_copy:
        c.start()

    w_s.wait_recv()

    @pl.loop(0, BATCH)
    def _(b):
        @pl.loop(0, 2)
        def _(kv):
            project(xbuf, 0, b, 0, kv)
            project(xbuf, 0, b, 1, kv)
            out_copy(0, b, 1, kv).start()

    w_z.wait_recv()
    w_zs.start()
    w_zs.wait_recv()
    own_x_phase(znb, 2)
    own_x_phase(znb, 3)
    for c in q_copy:
        c.wait_recv()

    lane = lax.broadcasted_iota(jnp.int32, (4, ROWS), 1)
    same_head = lane % 2 == lax.broadcasted_iota(jnp.int32, (4, ROWS), 0) % 2

    def attend(s, b):
        blk = me if s == 0 else ynb
        seen = same_head & (blk * SEQ_LOC + lane // 2 < lens[b])
        four = range(4)
        mine = pl.ds(pl.multiple_of(blk * ROWS, ROWS), ROWS)
        keys, vals = ([kv_out[kv, b, mine, :]] + [stage[s, b, o - 1, kv] for o in (1, 2, 3)] for kv in range(2))
        old = [part[o, 1, b] for o in four]
        acc = [part[o, 0, b] for o in four]
        sc = [lax.dot_general(qall[o, b].astype(BF), keys[o], (((1,), (1,)), ((), ())), preferred_element_type=F32) for o in four]
        sc = [jnp.where(seen, x * SCALE, NEG_BIG) for x in sc]
        top = [jnp.maximum(old[o][:, 0:1], jnp.max(sc[o], axis=-1, keepdims=True)) for o in four]
        p = [jnp.where(seen, jnp.exp(sc[o] - top[o]), 0.0) for o in four]
        fade = [jnp.exp(old[o][:, 0:1] - top[o]) for o in four]
        den = [old[o][:, HALF:HALF + 1] * fade[o] + jnp.sum(p[o], axis=-1, keepdims=True) for o in four]
        add = [jnp.dot(p[o].astype(BF), vals[o], preferred_element_type=F32) for o in four]
        for o in four:
            part[o, 0, b] = acc[o] * fade[o] + add[o]
            part[o, 1, b] = jnp.where(low, top[o], den[o])

    waiting = [(b, kv, o) for b in range(6, BATCH) for kv in range(2) for o in (2, 3)]

    def leave(b, kv, o):
        out_copy(1, b, o, kv).start()

    @pl.loop(0, BATCH)
    def _(b):
        attend(0, b)
        y_copy(b).wait_recv()

        xrecv[b] = norm_rows(xrecv[b].astype(F32), gain_a[...])

        @pl.loop(0, 2)
        def _(kv):
            for o in (2, 3):
                project(xrecv, 1, b, o, kv)

                @pl.when((b < 6) & (kv == 1))
                def _():
                    chunk_kv(b, o).start()

            project(xrecv, 1, b, 1, kv)
            out_copy(1, b, 1, kv).start()
            project(xrecv, 1, b, 0, kv)

        attend(1, b)

    p_copy = [remote(part.at[d], precv.at[d - 1], p_s.at[d - 1], p_r.at[d - 1], (rep, near[d])) for d in (1, 2, 3)]
    for c in p_copy:
        c.start()
    for job in waiting[0:2]:
        leave(*job)
    for load in loads[4:]:
        load.wait()
    first = lax.broadcasted_iota(jnp.int32, (BATCH, 4, 1), 1) < 2
    s_self = jnp.where(first, jnp.sum(qall[0] * kself[...], axis=-1, keepdims=True) * SCALE, NEG_BIG)
    for c in p_copy:
        c.wait_recv()
    accs = [part[0, 0]] + [precv[i, 0] for i in range(3)]
    stats = [part[0, 1]] + [precv[i, 1] for i in range(3)]
    tops = [st[:, :, 0:1] for st in stats]
    top = s_self
    for t in tops:
        top = jnp.maximum(top, t)
    e_self = jnp.where(first, jnp.exp(s_self - top), 0.0)
    den = e_self
    num = e_self * vself[...]
    for t, st, ac in zip(tops, stats, accs):
        e = jnp.exp(t - top)
        den = den + e * st[:, :, HALF:HALF + 1]
        num = num + e * ac
    attn[...] = num / den
    for g in range(2):
        for h in range(2):
            flat[g * BATCH:(g + 1) * BATCH, h * HEAD_DIM:(h + 1) * HEAD_DIM] = attn[:, 2 * g + h, :]

    def reduce_columns(i, base, jobs):
        sends = [remote(psend.at[i, near[d]], rrecv.at[i, d - 1], r_s.at[i, d - 1], r_r.at[i, d - 1], (rep, near[d])) for d in range(1, 8)]
        for c in sends:
            c.start()
        for job in jobs[0]:
            leave(*job)
        total = psend[i, me]
        for d in range(1, 8):
            sends[d - 1].wait_recv()
            total = total + rrecv[i, d - 1]
        hid[i, me] = (base + total).astype(BF)
        gets = [remote(hid.at[i, me], hid.at[i, me], a_s.at[i, d - 1], a_r.at[i, d - 1], (rep, near[d])) for d in range(1, 8)]
        for c in gets:
            c.start()
        for job in jobs[1]:
            leave(*job)
        for d in range(1, 8):
            remote(hid.at[i, near[d]], hid.at[i, near[d]], a_s.at[i, d - 1], a_r.at[i, d - 1], (rep, near[d])).wait_recv()
        return sends + gets

    a16 = flat[...].astype(BF)
    for j in range(8):
        psend[0, j] = jnp.dot(a16, wob[:, j * SHARD:(j + 1) * SHARD], preferred_element_type=F32)
    mine = pl.ds(pl.multiple_of(me * SHARD, SHARD), SHARD)
    done = reduce_columns(0, rows[:, mine], (waiting[2:3], waiting[3:6]))

    sq = jnp.zeros((2 * BATCH, 1), F32)
    for j in range(8):
        hj = hid[0, j].astype(F32)
        sq = sq + jnp.sum(hj * hj, axis=-1, keepdims=True)
    inv = lax.rsqrt(sq / D_MODEL + 1e-5)
    for j in range(8):
        cols = slice(j * SHARD, (j + 1) * SHARD)
        norm2[:, cols] = (hid[0, j].astype(F32) * inv * gain_m[:, cols].astype(F32)).astype(BF)
    n2 = norm2[...]
    gate = jnp.dot(n2, wgb[...], preferred_element_type=F32)
    up = jnp.dot(n2, wub[...], preferred_element_type=F32)
    mid = (gate * jax.nn.sigmoid(gate) * up).astype(BF)
    for j in range(8):
        psend[1, j] = jnp.dot(mid, wdb[:, j * SHARD:(j + 1) * SHARD], preferred_element_type=F32)
    done += reduce_columns(1, hid[0, me].astype(F32), (waiting[6:7], waiting[7:8]))
    for j in range(8):
        cols = slice(j * SHARD, (j + 1) * SHARD)
        dec_out[:, cols] = hid[1, j][:BATCH]
        last_out[:, cols] = hid[1, j][BATCH:]

    for c in [w_x, w_s, w_z, w_xs, w_zs] + l_copy + q_copy + p_copy + done:
        c.wait_send()

    @pl.loop(0, BATCH)
    def _(b):
        y_copy(b).wait_send()
        for kv in range(2):
            for s in range(2):
                out_copy(s, b, 1, kv).wait()

    for o in (2, 3):
        @pl.loop(0, BATCH, step=2)
        def _(b):
            for kv in range(2):
                own_two(b, o, kv).wait()

        @pl.loop(0, 6)
        def _(b):
            chunk_kv(b, o).wait()

    for b, kv, o in waiting:
        out_copy(1, b, o, kv).wait()


def layer(lens, prompt, new_tok, gain_a, gain_m, table, wq, wk, wv, wo, wg, wu, wd):
    vmem = pl.BlockSpec(memory_space=pltpu.VMEM)
    anym = pl.BlockSpec(memory_space=pl.ANY)
    dma = pltpu.SemaphoreType.DMA
    v = pltpu.VMEM
    return pl.pallas_call(
        layer_kernel,
        out_shape=(
            pltpu.VMEM((2, BATCH, 8 * ROWS, HEAD_DIM), BF),
            pltpu.VMEM((2, 2 * BATCH, HEAD_DIM), BF),
            pltpu.VMEM((BATCH, D_MODEL), BF),
            pltpu.VMEM((BATCH, D_MODEL), BF),
        ),
        in_specs=[pl.BlockSpec(memory_space=pltpu.SMEM), anym, vmem, vmem, vmem] + [anym] * 8,
        out_specs=(vmem, vmem, vmem, vmem),
        scratch_shapes=[
            v((BATCH, SEQ_LOC, D_MODEL), BF), v((BATCH, SEQ_LOC, D_MODEL), BF), v((4, 2, D_MODEL, SHARD), BF),
            v((D_MODEL, SHARD), BF), v((SHARD, D_MODEL), BF), v((D_MODEL, FF_LOC), BF), v((D_MODEL, FF_LOC), BF), v((FF_LOC, D_MODEL), BF),
            v((TAB_ROWS, HEAD_DIM), F32), v((ROWS, HEAD_DIM), F32), v((2, BATCH, 3, 2, ROWS, HEAD_DIM), BF),
            v((BATCH, D_MODEL), F32), v((3, BATCH, D_MODEL), BF), v((3, BATCH, D_MODEL), BF), v((2 * BATCH, D_MODEL), F32),
            v((4, BATCH, 4, HEAD_DIM), F32), v((4, 2, BATCH, 4, HEAD_DIM), F32), v((3, 2, BATCH, 4, HEAD_DIM), F32),
            v((BATCH, 4, HEAD_DIM), F32), v((BATCH, 4, HEAD_DIM), F32), v((BATCH, 4, HEAD_DIM), F32), v((2 * BATCH, SHARD), F32),
            v((2, 8, 2 * BATCH, SHARD), F32), v((2, 7, 2 * BATCH, SHARD), F32), v((2, 8, 2 * BATCH, SHARD), BF), v((2 * BATCH, D_MODEL), BF),
            dma((8,)), dma((BATCH,)), dma((BATCH,)), dma((BATCH,)), dma((5,)), dma((5,)),
            dma((3, 2, BATCH, 2)), dma((3, 2, BATCH, 2)),
            dma((3,)), dma((3,)), dma((3,)), dma((3,)), dma((3,)), dma((3,)),
            dma((2, 7)), dma((2, 7)), dma((2, 7)), dma((2, 7)),
        ],
        compiler_params=pltpu.CompilerParams(collective_id=0, has_side_effects=True, vmem_limit_bytes=49 * 1024 * 1024),
        cost_estimate=pl.CostEstimate(flops=26_000_000_000, bytes_accessed=60_000_000, transcendentals=0),
        name='layer',
    )(lens, prompt, new_tok, gain_a, gain_m, table, wq, wk, wv, wo, wg, wu, wd)


def cache_kernel(kv, new, dec, last, key_out, val_out, dec_out, last_out, store, row_sem):
    outs = (key_out, val_out)
    puts = []
    for i in range(2):
        for b in range(BATCH):
            puts.append(pltpu.make_async_copy(kv.at[i, b], outs[i].at[0, b, pl.ds(0, SEQ_LEN)], store.at[i, b]))
            puts[-1].start()
    for i in range(2):
        puts.append(pltpu.make_async_copy(new.at[i], outs[i].at[0, :, pl.ds(SEQ_LEN, 1)], row_sem.at[i]))
        puts[-1].start()
    dec_out[...] = dec[...]
    last_out[...] = last[...]
    for c in puts:
        c.wait()


def caches(kv, new, dec, last):
    anym = pl.BlockSpec(memory_space=pl.ANY)
    dma = pltpu.SemaphoreType.DMA
    vmem = pl.BlockSpec(memory_space=pltpu.VMEM)
    shape = jax.ShapeDtypeStruct((1, BATCH, SEQ_LEN + 1, 2, HEAD_DIM), BF)
    row = jax.ShapeDtypeStruct((BATCH, D_MODEL), BF)
    return pl.pallas_call(
        cache_kernel,
        out_shape=(shape, shape, row, row),
        in_specs=[anym, anym, vmem, vmem],
        out_specs=(anym, anym, vmem, vmem),
        scratch_shapes=[dma((2, BATCH)), dma((2,))],
        compiler_params=pltpu.CompilerParams(vmem_limit_bytes=4 * 1024 * 1024),
        cost_estimate=pl.CostEstimate(flops=0, bytes_accessed=13_000_000, transcendentals=0),
        name='caches',
    )(kv, new, dec, last)


def solution(mesh):
    seq_spec = P('replica', 'model', None)
    col_spec = P(None, None, 'model')
    row_spec = P(None, 'model', None)
    gain_spec = P(None, None)
    tok_spec = P('replica', None)
    cache_spec = P(None, 'replica', None, 'model', None)
    in_specs = (seq_spec, P('replica'), tok_spec, gain_spec, col_spec, col_spec, col_spec, row_spec, gain_spec, col_spec, col_spec, row_spec)
    out_specs = (tok_spec, tok_spec, cache_spec, cache_spec)
    table = rope_table()

    def per_device(prompt, lengths, new_tok, norm_attn, w_q, w_k, w_v, w_o, norm_mlp, w_gate, w_up, w_down):
        kv, new, dec, last = layer(lengths, prompt, new_tok, norm_attn, norm_mlp, jnp.asarray(table), w_q, w_k, w_v, w_o, w_gate, w_up, w_down)
        keys, vals, dec, last = caches(kv.reshape(2, BATCH, SEQ_LEN, 2, HEAD_DIM), new.reshape(2, BATCH, 1, 2, HEAD_DIM), dec, last)
        return dec, last, keys, vals

    return jax.shard_map(per_device, mesh=mesh, in_specs=in_specs, out_specs=out_specs, check_vma=False)
```

```python
import jax
import jax.numpy as jnp
import numpy as np
from jax import lax
from jax.experimental import pallas as pl
from jax.experimental.pallas import tpu as pltpu
from jax.sharding import PartitionSpec as P

HEAD_DIM = 128
HALF = HEAD_DIM // 2
NEG_BIG = -1e30
BATCH = 8
SEQ_LOC = 192
SEQ_LEN = 1536
D_MODEL = 2048
SHARD = 256
FF_LOC = 1024
ROWS = 2 * SEQ_LOC
TAB_ROWS = SEQ_LEN + 8
MESH = pl.DeviceIdType.MESH
BF = jnp.bfloat16
F32 = jnp.float32
SCALE = HEAD_DIM ** -0.5


def rope_table():
    inv_freq = np.float32(10000.0) ** (np.float32(-2.0) * np.arange(HALF, dtype=np.float32) / np.float32(HEAD_DIM))
    angles = np.arange(TAB_ROWS, dtype=np.float32)[:, None] * inv_freq.astype(np.float32)
    return np.concatenate([np.cos(angles), np.sin(angles)], axis=-1).astype(np.float32)


def norm_rows(x, gain):
    inv = lax.rsqrt(jnp.mean(x * x, axis=-1, keepdims=True) + 1e-5)
    return (x * inv * gain.astype(F32)).astype(BF)


def spread(tab):
    swapped = pltpu.roll(tab, HALF, 1)
    low = lax.broadcasted_iota(jnp.int32, tab.shape, 1) < HALF
    return jnp.where(low, tab, swapped), jnp.where(low, -swapped, tab)


def rotate(a, c, s):
    return a * c + pltpu.roll(a, HALF, 1) * s


def layer_kernel(lens, prompt, new_tok, gain_a, gain_m, table, wq, wk, wv, wo, wg, wu, wd,
                 kv_out, new_out, dec_out, last_out,
                 xbuf, xrecv, wbuf, wqb, wob, wgb, wub, wdb, tab, tmp, stage,
                 lastf, lsend, lrecv, rows, qall, part, precv, kself, vself, attn, flat,
                 psend, rrecv, hid, norm2,
                 lsem, xsem, ysend, yrecv, wsend, wrecv, osend, orecv,
                 l_s, l_r, q_s, q_r, p_s, p_r, r_s, r_r, a_s, a_r):
    rep = lax.axis_index('replica')
    me = lax.axis_index('model')
    core = lax.rem(me, 2)
    xpos = lax.rem(me // 2, 2)
    ypos = me // 4
    flips = (1 - 2 * core, 2 - 4 * xpos, 4 - 8 * ypos)
    near = [me + sum(f for i, f in enumerate(flips) if d >> i & 1) for d in range(8)]
    sib, xnb, xsb, ynb = near[1], near[2], near[3], near[4]
    znb = 1 - rep

    barrier = pltpu.get_barrier_semaphore()
    for peer in [(rep, near[d]) for d in range(1, 8)] + [(znb, me)]:
        pl.semaphore_signal(barrier, inc=1, device_id=peer, device_id_type=MESH)
    pl.semaphore_wait(barrier, 8)

    def remote(src, dst, send, recv, peer):
        return pltpu.make_async_remote_copy(src_ref=src, dst_ref=dst, send_sem=send, recv_sem=recv, device_id=peer, device_id_type=MESH)

    def y_copy(b):
        return remote(prompt.at[b], xrecv.at[b], ysend.at[b], yrecv.at[b], (rep, ynb))

    def x_load(b):
        return pltpu.make_async_copy(prompt.at[b], xbuf.at[b], xsem.at[b])

    loads = [pltpu.make_async_copy(a, b, lsem.at[i]) for i, (a, b) in enumerate((
        (wk.at[0], wbuf.at[0, 0]), (wv.at[0], wbuf.at[0, 1]), (table, tab), (wq.at[0], wqb), (wo.at[0], wob),
        (wg.at[0], wgb), (wu.at[0], wub), (wd.at[0], wdb)))]
    for i, w in enumerate((wk, wv)):
        @pl.when(rep == i)
        def _():
            remote(w.at[0], wbuf.at[2, rep], wsend.at[0], wrecv.at[0], (rep, xnb)).start()

    y_copy(0).start()
    loads[0].start()
    loads[1].start()

    @pl.loop(0, BATCH)
    def _(b):
        x_load(b).start()

    for load in loads[2:]:
        load.start()
    w_x = remote(wbuf.at[0, rep], wbuf.at[2, rep], wsend.at[0], wrecv.at[0], (rep, xnb))
    w_s = remote(wbuf.at[0], wbuf.at[1], wsend.at[1], wrecv.at[1], (rep, sib))
    w_z = remote(wbuf.at[2, rep], wbuf.at[2, rep], wsend.at[2], wrecv.at[2], (znb, me))
    w_xs = remote(wbuf.at[2, rep], wbuf.at[3, rep], wsend.at[3], wrecv.at[3], (rep, sib))
    w_zs = remote(wbuf.at[2, znb], wbuf.at[3, znb], wsend.at[4], wrecv.at[4], (rep, sib))
    loads[0].wait()
    loads[1].wait()
    w_s.start()

    def out_copy(s, b, o, kv):
        blk = me if s == 0 else ynb
        dst = kv_out.at[kv, b, pl.ds(pl.multiple_of(blk * ROWS, ROWS), ROWS), :]
        src = stage.at[s, b, o - 1, kv]
        return remote(src, dst, osend.at[o - 1, s, b, kv], orecv.at[o - 1, s, b, kv], (rep, near[o]))

    def own_two(b, o, kv):
        dst = kv_out.at[kv, pl.ds(b, 2), pl.ds(pl.multiple_of(me * ROWS, ROWS), ROWS), :]
        return remote(stage.at[0, pl.ds(b, 2), o - 1, kv], dst, osend.at[o - 1, 0, b, kv], orecv.at[o - 1, 0, b, kv], (rep, near[o]))

    def chunk_kv(b, o):
        dst = kv_out.at[:, b, pl.ds(pl.multiple_of(ynb * ROWS, ROWS), ROWS), :]
        return remote(stage.at[1, b, o - 1], dst, osend.at[o - 1, 1, b, 0], orecv.at[o - 1, 1, b, 0], (rep, near[o]))

    def project(buf, s, b, o, kv):
        acc = jnp.dot(buf[b], wbuf[o, kv], preferred_element_type=F32)
        blk = me if s == 0 else ynb
        c, sn = spread(tab[pl.ds(pl.multiple_of(blk * SEQ_LOC, SEQ_LOC), SEQ_LOC), :])
        is_k = kv == 0
        c = jnp.where(is_k, c, 1.0)
        sn = jnp.where(is_k, sn, 0.0)
        for h in range(2):
            tmp[pl.ds(h, SEQ_LOC, stride=2), :] = rotate(acc[:, h * HEAD_DIM:(h + 1) * HEAD_DIM], c, sn)
        if o == 0:
            kv_out[kv, b, pl.ds(pl.multiple_of(blk * ROWS, ROWS), ROWS), :] = tmp[...].astype(BF)
        else:
            stage[s, b, o - 1, kv] = tmp[...].astype(BF)

    @pl.loop(0, BATCH)
    def _(b):
        x_load(b).wait()
        here = me * SEQ_LOC + lax.broadcasted_iota(jnp.int32, (SEQ_LOC, 1), 0) == lens[b] - 1
        lastf[pl.ds(b, 1), :] = jnp.sum(jnp.where(here, xbuf[b].astype(F32), 0.0), axis=0, keepdims=True)

    l_copy = [remote(lsend.at[i], lrecv.at[i], l_s.at[i], l_r.at[i], (rep, near[d])) for i, d in enumerate((4, 1, 2))]
    lsend[0] = lastf[...].astype(BF)
    l_copy[0].start()
    y_copy(1).start()

    @pl.loop(0, BATCH)
    def _(b):
        xbuf[b] = norm_rows(xbuf[b].astype(F32), gain_a[...])

    @pl.loop(2, BATCH)
    def _(b):
        remote(xbuf.at[b], xrecv.at[b], ysend.at[b], yrecv.at[b], (rep, ynb)).start()

    def join_last(i):
        l_copy[i].wait_recv()
        return (lsend[i].astype(F32) + lrecv[i].astype(F32)).astype(BF)

    lsend[1] = join_last(0)
    l_copy[1].start()
    loads[2].wait()

    w_x.wait_recv()
    w_z.start()
    w_xs.start()
    lsend[2] = join_last(1)
    l_copy[2].start()

    def own_x_phase(kv, o):
        @pl.loop(0, BATCH, step=2)
        def _(b):
            project(xbuf, 0, b, o, kv)
            project(xbuf, 0, b + 1, o, kv)
            own_two(b, o, kv).start()

    own_x_phase(rep, 2)
    w_xs.wait_recv()
    own_x_phase(rep, 3)

    rows[0:BATCH, :] = new_tok[...].astype(F32)
    rows[BATCH:2 * BATCH, :] = join_last(2).astype(F32)
    loads[3].wait()
    n16 = norm_rows(rows[...], gain_a[...])
    q16 = jnp.dot(n16, wqb[...], preferred_element_type=F32)
    k16 = jnp.dot(n16, wbuf[0, 0], preferred_element_type=F32)
    v16 = jnp.dot(n16, wbuf[0, 1], preferred_element_type=F32)
    for b in range(BATCH):
        flat[pl.ds(b, 1), 0:HEAD_DIM] = tab[pl.ds(jnp.clip(lens[b], 0, SEQ_LEN), 1), :]
        flat[pl.ds(BATCH + b, 1), 0:HEAD_DIM] = tab[pl.ds(jnp.clip(lens[b] - 1, 0, SEQ_LEN), 1), :]
    c16, s16 = spread(flat[:, 0:HEAD_DIM])
    kself[...] = jnp.zeros_like(kself)
    vself[...] = jnp.zeros_like(vself)
    for h in range(2):
        lanes = slice(h * HEAD_DIM, (h + 1) * HEAD_DIM)
        qh = rotate(q16[:, lanes], c16, s16).astype(BF).astype(F32)
        kh = rotate(k16[:, lanes], c16, s16)[:BATCH].astype(BF).astype(F32)
        vh = v16[:BATCH, lanes].astype(BF).astype(F32)
        for g in range(2):
            qall[0, :, 2 * g + h, :] = qh[g * BATCH:(g + 1) * BATCH]
        kself[:, h, :] = kh
        vself[:, h, :] = vh
        tmp[pl.ds(h, BATCH, stride=2), :] = kh
        tmp[pl.ds(2 * BATCH + h, BATCH, stride=2), :] = vh
    new_out[0] = tmp[0:2 * BATCH, :].astype(BF)
    new_out[1] = tmp[2 * BATCH:4 * BATCH, :].astype(BF)
    low = lax.broadcasted_iota(jnp.int32, (4, HEAD_DIM), 1) < HALF
    part[:, 0] = jnp.zeros((4, BATCH, 4, HEAD_DIM), F32)
    part[:, 1] = jnp.broadcast_to(jnp.where(low, NEG_BIG, 0.0), (4, BATCH, 4, HEAD_DIM))
    q_copy = [remote(qall.at[0], qall.at[d], q_s.at[d - 1], q_r.at[d - 1], (rep, near[d])) for d in (1, 2, 3)]
    for c in q_copy:
        c.start()

    w_s.wait_recv()

    @pl.loop(0, BATCH)
    def _(b):
        @pl.loop(0, 2)
        def _(kv):
            project(xbuf, 0, b, 0, kv)
            project(xbuf, 0, b, 1, kv)
            out_copy(0, b, 1, kv).start()

    w_z.wait_recv()
    w_zs.start()
    w_zs.wait_recv()
    own_x_phase(znb, 2)
    own_x_phase(znb, 3)
    for c in q_copy:
        c.wait_recv()

    lane = lax.broadcasted_iota(jnp.int32, (4, ROWS), 1)
    same_head = lane % 2 == lax.broadcasted_iota(jnp.int32, (4, ROWS), 0) % 2

    def attend(s, b):
        blk = me if s == 0 else ynb
        seen = same_head & (blk * SEQ_LOC + lane // 2 < lens[b])
        four = range(4)
        mine = pl.ds(pl.multiple_of(blk * ROWS, ROWS), ROWS)
        keys, vals = ([kv_out[kv, b, mine, :]] + [stage[s, b, o - 1, kv] for o in (1, 2, 3)] for kv in range(2))
        old = [part[o, 1, b] for o in four]
        acc = [part[o, 0, b] for o in four]
        sc = [lax.dot_general(qall[o, b].astype(BF), keys[o], (((1,), (1,)), ((), ())), preferred_element_type=F32) for o in four]
        sc = [jnp.where(seen, x * SCALE, NEG_BIG) for x in sc]
        top = [jnp.maximum(old[o][:, 0:1], jnp.max(sc[o], axis=-1, keepdims=True)) for o in four]
        p = [jnp.where(seen, jnp.exp(sc[o] - top[o]), 0.0) for o in four]
        fade = [jnp.exp(old[o][:, 0:1] - top[o]) for o in four]
        den = [old[o][:, HALF:HALF + 1] * fade[o] + jnp.sum(p[o], axis=-1, keepdims=True) for o in four]
        add = [jnp.dot(p[o].astype(BF), vals[o], preferred_element_type=F32) for o in four]
        for o in four:
            part[o, 0, b] = acc[o] * fade[o] + add[o]
            part[o, 1, b] = jnp.where(low, top[o], den[o])

    waiting = [(b, kv, o) for b in range(6, BATCH) for kv in range(2) for o in (2, 3)]

    def leave(b, kv, o):
        out_copy(1, b, o, kv).start()

    @pl.loop(0, BATCH)
    def _(b):
        attend(0, b)
        y_copy(b).wait_recv()

        @pl.when(b < 2)
        def _():
            xrecv[b] = norm_rows(xrecv[b].astype(F32), gain_a[...])

        @pl.loop(0, 2)
        def _(kv):
            for o in (2, 3):
                project(xrecv, 1, b, o, kv)

                @pl.when((b < 6) & (kv == 1))
                def _():
                    chunk_kv(b, o).start()

            project(xrecv, 1, b, 1, kv)
            out_copy(1, b, 1, kv).start()
            project(xrecv, 1, b, 0, kv)

        attend(1, b)

    p_copy = [remote(part.at[d], precv.at[d - 1], p_s.at[d - 1], p_r.at[d - 1], (rep, near[d])) for d in (1, 2, 3)]
    for c in p_copy:
        c.start()
    for job in waiting[0:2]:
        leave(*job)
    for load in loads[4:]:
        load.wait()
    first = lax.broadcasted_iota(jnp.int32, (BATCH, 4, 1), 1) < 2
    s_self = jnp.where(first, jnp.sum(qall[0] * kself[...], axis=-1, keepdims=True) * SCALE, NEG_BIG)
    for c in p_copy:
        c.wait_recv()
    accs = [part[0, 0]] + [precv[i, 0] for i in range(3)]
    stats = [part[0, 1]] + [precv[i, 1] for i in range(3)]
    tops = [st[:, :, 0:1] for st in stats]
    top = s_self
    for t in tops:
        top = jnp.maximum(top, t)
    e_self = jnp.where(first, jnp.exp(s_self - top), 0.0)
    den = e_self
    num = e_self * vself[...]
    for t, st, ac in zip(tops, stats, accs):
        e = jnp.exp(t - top)
        den = den + e * st[:, :, HALF:HALF + 1]
        num = num + e * ac
    attn[...] = num / den
    for g in range(2):
        for h in range(2):
            flat[g * BATCH:(g + 1) * BATCH, h * HEAD_DIM:(h + 1) * HEAD_DIM] = attn[:, 2 * g + h, :]

    def reduce_columns(i, base, jobs):
        sends = [remote(psend.at[i, near[d]], rrecv.at[i, d - 1], r_s.at[i, d - 1], r_r.at[i, d - 1], (rep, near[d])) for d in range(1, 8)]
        for c in sends:
            c.start()
        for job in jobs[0]:
            leave(*job)
        total = psend[i, me]
        for d in range(1, 8):
            sends[d - 1].wait_recv()
            total = total + rrecv[i, d - 1]
        hid[i, me] = (base + total).astype(BF)
        gets = [remote(hid.at[i, me], hid.at[i, me], a_s.at[i, d - 1], a_r.at[i, d - 1], (rep, near[d])) for d in range(1, 8)]
        for c in gets:
            c.start()
        for job in jobs[1]:
            leave(*job)
        for d in range(1, 8):
            remote(hid.at[i, near[d]], hid.at[i, near[d]], a_s.at[i, d - 1], a_r.at[i, d - 1], (rep, near[d])).wait_recv()
        return sends + gets

    a16 = flat[...].astype(BF)
    for j in range(8):
        psend[0, j] = jnp.dot(a16, wob[:, j * SHARD:(j + 1) * SHARD], preferred_element_type=F32)
    mine = pl.ds(pl.multiple_of(me * SHARD, SHARD), SHARD)
    done = reduce_columns(0, rows[:, mine], (waiting[2:3], waiting[3:6]))

    sq = jnp.zeros((2 * BATCH, 1), F32)
    for j in range(8):
        hj = hid[0, j].astype(F32)
        sq = sq + jnp.sum(hj * hj, axis=-1, keepdims=True)
    inv = lax.rsqrt(sq / D_MODEL + 1e-5)
    for j in range(8):
        cols = slice(j * SHARD, (j + 1) * SHARD)
        norm2[:, cols] = (hid[0, j].astype(F32) * inv * gain_m[:, cols].astype(F32)).astype(BF)
    n2 = norm2[...]
    gate = jnp.dot(n2, wgb[...], preferred_element_type=F32)
    up = jnp.dot(n2, wub[...], preferred_element_type=F32)
    mid = (gate * jax.nn.sigmoid(gate) * up).astype(BF)
    for j in range(8):
        psend[1, j] = jnp.dot(mid, wdb[:, j * SHARD:(j + 1) * SHARD], preferred_element_type=F32)
    done += reduce_columns(1, hid[0, me].astype(F32), (waiting[6:7], waiting[7:8]))
    for j in range(8):
        cols = slice(j * SHARD, (j + 1) * SHARD)
        dec_out[:, cols] = hid[1, j][:BATCH]
        last_out[:, cols] = hid[1, j][BATCH:]

    for c in [w_x, w_s, w_z, w_xs, w_zs] + l_copy + q_copy + p_copy + done:
        c.wait_send()

    @pl.loop(0, BATCH)
    def _(b):
        y_copy(b).wait_send()
        for kv in range(2):
            for s in range(2):
                out_copy(s, b, 1, kv).wait()

    for o in (2, 3):
        @pl.loop(0, BATCH, step=2)
        def _(b):
            for kv in range(2):
                own_two(b, o, kv).wait()

        @pl.loop(0, 6)
        def _(b):
            chunk_kv(b, o).wait()

    for b, kv, o in waiting:
        out_copy(1, b, o, kv).wait()


def layer(lens, prompt, new_tok, gain_a, gain_m, table, wq, wk, wv, wo, wg, wu, wd):
    vmem = pl.BlockSpec(memory_space=pltpu.VMEM)
    anym = pl.BlockSpec(memory_space=pl.ANY)
    dma = pltpu.SemaphoreType.DMA
    v = pltpu.VMEM
    return pl.pallas_call(
        layer_kernel,
        out_shape=(
            pltpu.VMEM((2, BATCH, 8 * ROWS, HEAD_DIM), BF),
            pltpu.VMEM((2, 2 * BATCH, HEAD_DIM), BF),
            pltpu.VMEM((BATCH, D_MODEL), BF),
            pltpu.VMEM((BATCH, D_MODEL), BF),
        ),
        in_specs=[pl.BlockSpec(memory_space=pltpu.SMEM), anym, vmem, vmem, vmem] + [anym] * 8,
        out_specs=(vmem, vmem, vmem, vmem),
        scratch_shapes=[
            v((BATCH, SEQ_LOC, D_MODEL), BF), v((BATCH, SEQ_LOC, D_MODEL), BF), v((4, 2, D_MODEL, SHARD), BF),
            v((D_MODEL, SHARD), BF), v((SHARD, D_MODEL), BF), v((D_MODEL, FF_LOC), BF), v((D_MODEL, FF_LOC), BF), v((FF_LOC, D_MODEL), BF),
            v((TAB_ROWS, HEAD_DIM), F32), v((ROWS, HEAD_DIM), F32), v((2, BATCH, 3, 2, ROWS, HEAD_DIM), BF),
            v((BATCH, D_MODEL), F32), v((3, BATCH, D_MODEL), BF), v((3, BATCH, D_MODEL), BF), v((2 * BATCH, D_MODEL), F32),
            v((4, BATCH, 4, HEAD_DIM), F32), v((4, 2, BATCH, 4, HEAD_DIM), F32), v((3, 2, BATCH, 4, HEAD_DIM), F32),
            v((BATCH, 4, HEAD_DIM), F32), v((BATCH, 4, HEAD_DIM), F32), v((BATCH, 4, HEAD_DIM), F32), v((2 * BATCH, SHARD), F32),
            v((2, 8, 2 * BATCH, SHARD), F32), v((2, 7, 2 * BATCH, SHARD), F32), v((2, 8, 2 * BATCH, SHARD), BF), v((2 * BATCH, D_MODEL), BF),
            dma((8,)), dma((BATCH,)), dma((BATCH,)), dma((BATCH,)), dma((5,)), dma((5,)),
            dma((3, 2, BATCH, 2)), dma((3, 2, BATCH, 2)),
            dma((3,)), dma((3,)), dma((3,)), dma((3,)), dma((3,)), dma((3,)),
            dma((2, 7)), dma((2, 7)), dma((2, 7)), dma((2, 7)),
        ],
        compiler_params=pltpu.CompilerParams(collective_id=0, has_side_effects=True, vmem_limit_bytes=49 * 1024 * 1024),
        cost_estimate=pl.CostEstimate(flops=26_000_000_000, bytes_accessed=60_000_000, transcendentals=0),
        name='layer',
    )(lens, prompt, new_tok, gain_a, gain_m, table, wq, wk, wv, wo, wg, wu, wd)


def cache_kernel(kv, new, dec, last, key_out, val_out, dec_out, last_out, store, row_sem):
    outs = (key_out, val_out)
    puts = []
    for i in range(2):
        for b in range(BATCH):
            puts.append(pltpu.make_async_copy(kv.at[i, b], outs[i].at[0, b, pl.ds(0, SEQ_LEN)], store.at[i, b]))
            puts[-1].start()
    for i in range(2):
        puts.append(pltpu.make_async_copy(new.at[i], outs[i].at[0, :, pl.ds(SEQ_LEN, 1)], row_sem.at[i]))
        puts[-1].start()
    dec_out[...] = dec[...]
    last_out[...] = last[...]
    for c in puts:
        c.wait()


def caches(kv, new, dec, last):
    anym = pl.BlockSpec(memory_space=pl.ANY)
    dma = pltpu.SemaphoreType.DMA
    vmem = pl.BlockSpec(memory_space=pltpu.VMEM)
    shape = jax.ShapeDtypeStruct((1, BATCH, SEQ_LEN + 1, 2, HEAD_DIM), BF)
    row = jax.ShapeDtypeStruct((BATCH, D_MODEL), BF)
    return pl.pallas_call(
        cache_kernel,
        out_shape=(shape, shape, row, row),
        in_specs=[anym, anym, vmem, vmem],
        out_specs=(anym, anym, vmem, vmem),
        scratch_shapes=[dma((2, BATCH)), dma((2,))],
        compiler_params=pltpu.CompilerParams(vmem_limit_bytes=4 * 1024 * 1024),
        cost_estimate=pl.CostEstimate(flops=0, bytes_accessed=13_000_000, transcendentals=0),
        name='caches',
    )(kv, new, dec, last)


def solution(mesh):
    seq_spec = P('replica', 'model', None)
    col_spec = P(None, None, 'model')
    row_spec = P(None, 'model', None)
    gain_spec = P(None, None)
    tok_spec = P('replica', None)
    cache_spec = P(None, 'replica', None, 'model', None)
    in_specs = (seq_spec, P('replica'), tok_spec, gain_spec, col_spec, col_spec, col_spec, row_spec, gain_spec, col_spec, col_spec, row_spec)
    out_specs = (tok_spec, tok_spec, cache_spec, cache_spec)
    table = rope_table()

    def per_device(prompt, lengths, new_tok, norm_attn, w_q, w_k, w_v, w_o, norm_mlp, w_gate, w_up, w_down):
        kv, new, dec, last = layer(lengths, prompt, new_tok, norm_attn, norm_mlp, jnp.asarray(table), w_q, w_k, w_v, w_o, w_gate, w_up, w_down)
        keys, vals, dec, last = caches(kv.reshape(2, BATCH, SEQ_LEN, 2, HEAD_DIM), new.reshape(2, BATCH, 1, 2, HEAD_DIM), dec, last)
        return dec, last, keys, vals

    return jax.shard_map(per_device, mesh=mesh, in_specs=in_specs, out_specs=out_specs, check_vma=False)
```

```python
import jax
import jax.numpy as jnp
import numpy as np
from jax import lax
from jax.experimental import pallas as pl
from jax.experimental.pallas import tpu as pltpu
from jax.sharding import PartitionSpec as P

HEAD_DIM = 128
HALF = HEAD_DIM // 2
NEG_BIG = -1e30
BATCH = 8
SEQ_LOC = 192
SEQ_LEN = 1536
D_MODEL = 2048
SHARD = 256
FF_LOC = 1024
ROWS = 2 * SEQ_LOC
TAB_ROWS = SEQ_LEN + 8
MESH = pl.DeviceIdType.MESH
BF = jnp.bfloat16
F32 = jnp.float32
SCALE = HEAD_DIM ** -0.5


def rope_table():
    inv_freq = np.float32(10000.0) ** (np.float32(-2.0) * np.arange(HALF, dtype=np.float32) / np.float32(HEAD_DIM))
    angles = np.arange(TAB_ROWS, dtype=np.float32)[:, None] * inv_freq.astype(np.float32)
    return np.concatenate([np.cos(angles), np.sin(angles)], axis=-1).astype(np.float32)


def norm_rows(x, gain):
    inv = lax.rsqrt(jnp.mean(x * x, axis=-1, keepdims=True) + 1e-5)
    return (x * inv * gain.astype(F32)).astype(BF)


def spread(tab):
    swapped = pltpu.roll(tab, HALF, 1)
    low = lax.broadcasted_iota(jnp.int32, tab.shape, 1) < HALF
    return jnp.where(low, tab, swapped), jnp.where(low, -swapped, tab)


def rotate(a, c, s):
    return a * c + pltpu.roll(a, HALF, 1) * s


def layer_kernel(lens, prompt, new_tok, gain_a, gain_m, table, wq, wk, wv, wo, wg, wu, wd,
                 kv_out, new_out, dec_out, last_out,
                 xbuf, xrecv, wbuf, wqb, wob, wgb, wub, wdb, tab, tmp, stage,
                 lastf, lsend, lrecv, rows, qall, part, precv, kself, vself, attn, flat,
                 psend, rrecv, hid, norm2,
                 lsem, xsem, ysend, yrecv, wsend, wrecv, osend, orecv,
                 l_s, l_r, q_s, q_r, p_s, p_r, r_s, r_r, a_s, a_r):
    rep = lax.axis_index('replica')
    me = lax.axis_index('model')
    core = lax.rem(me, 2)
    xpos = lax.rem(me // 2, 2)
    ypos = me // 4
    flips = (1 - 2 * core, 2 - 4 * xpos, 4 - 8 * ypos)
    near = [me + sum(f for i, f in enumerate(flips) if d >> i & 1) for d in range(8)]
    sib, xnb, xsb, ynb = near[1], near[2], near[3], near[4]
    znb = 1 - rep

    barrier = pltpu.get_barrier_semaphore()
    for peer in [(rep, near[d]) for d in range(1, 8)] + [(znb, me)]:
        pl.semaphore_signal(barrier, inc=1, device_id=peer, device_id_type=MESH)
    pl.semaphore_wait(barrier, 8)

    def remote(src, dst, send, recv, peer):
        return pltpu.make_async_remote_copy(src_ref=src, dst_ref=dst, send_sem=send, recv_sem=recv, device_id=peer, device_id_type=MESH)

    def y_copy(b):
        return remote(prompt.at[b], xrecv.at[b], ysend.at[b], yrecv.at[b], (rep, ynb))

    def x_load(b):
        return pltpu.make_async_copy(prompt.at[b], xbuf.at[b], xsem.at[b])

    loads = [pltpu.make_async_copy(a, b, lsem.at[i]) for i, (a, b) in enumerate((
        (wk.at[0], wbuf.at[0, 0]), (wv.at[0], wbuf.at[0, 1]), (table, tab), (wq.at[0], wqb), (wo.at[0], wob),
        (wg.at[0], wgb), (wu.at[0], wub), (wd.at[0], wdb)))]
    for i, w in enumerate((wk, wv)):
        @pl.when(rep == i)
        def _():
            remote(w.at[0], wbuf.at[2, rep], wsend.at[0], wrecv.at[0], (rep, xnb)).start()

    y_copy(0).start()
    loads[0].start()
    loads[1].start()

    @pl.loop(0, BATCH)
    def _(b):
        x_load(b).start()

    for load in loads[2:]:
        load.start()
    w_x = remote(wbuf.at[0, rep], wbuf.at[2, rep], wsend.at[0], wrecv.at[0], (rep, xnb))
    w_s = remote(wbuf.at[0], wbuf.at[1], wsend.at[1], wrecv.at[1], (rep, sib))
    w_z = remote(wbuf.at[2, rep], wbuf.at[2, rep], wsend.at[2], wrecv.at[2], (znb, me))
    w_xs = remote(wbuf.at[2, rep], wbuf.at[3, rep], wsend.at[3], wrecv.at[3], (rep, sib))
    w_zs = remote(wbuf.at[2, znb], wbuf.at[3, znb], wsend.at[4], wrecv.at[4], (rep, sib))
    loads[0].wait()
    loads[1].wait()
    w_s.start()

    def out_copy(s, b, o, kv):
        blk = me if s == 0 else ynb
        dst = kv_out.at[kv, b, pl.ds(pl.multiple_of(blk * ROWS, ROWS), ROWS), :]
        src = stage.at[s, b, o - 1, kv]
        return remote(src, dst, osend.at[o - 1, s, b, kv], orecv.at[o - 1, s, b, kv], (rep, near[o]))

    def own_two(b, o, kv):
        dst = kv_out.at[kv, pl.ds(b, 2), pl.ds(pl.multiple_of(me * ROWS, ROWS), ROWS), :]
        return remote(stage.at[0, pl.ds(b, 2), o - 1, kv], dst, osend.at[o - 1, 0, b, kv], orecv.at[o - 1, 0, b, kv], (rep, near[o]))

    def chunk_kv(b, o):
        dst = kv_out.at[:, b, pl.ds(pl.multiple_of(ynb * ROWS, ROWS), ROWS), :]
        return remote(stage.at[1, b, o - 1], dst, osend.at[o - 1, 1, b, 0], orecv.at[o - 1, 1, b, 0], (rep, near[o]))

    def project(buf, s, b, o, kv):
        acc = jnp.dot(buf[b], wbuf[o, kv], preferred_element_type=F32)
        blk = me if s == 0 else ynb
        c, sn = spread(tab[pl.ds(pl.multiple_of(blk * SEQ_LOC, SEQ_LOC), SEQ_LOC), :])
        is_k = kv == 0
        c = jnp.where(is_k, c, 1.0)
        sn = jnp.where(is_k, sn, 0.0)
        for h in range(2):
            tmp[pl.ds(h, SEQ_LOC, stride=2), :] = rotate(acc[:, h * HEAD_DIM:(h + 1) * HEAD_DIM], c, sn)
        if o == 0:
            kv_out[kv, b, pl.ds(pl.multiple_of(blk * ROWS, ROWS), ROWS), :] = tmp[...].astype(BF)
        else:
            stage[s, b, o - 1, kv] = tmp[...].astype(BF)

    @pl.loop(0, BATCH)
    def _(b):
        x_load(b).wait()
        here = me * SEQ_LOC + lax.broadcasted_iota(jnp.int32, (SEQ_LOC, 1), 0) == lens[b] - 1
        lastf[pl.ds(b, 1), :] = jnp.sum(jnp.where(here, xbuf[b].astype(F32), 0.0), axis=0, keepdims=True)

    l_copy = [remote(lsend.at[i], lrecv.at[i], l_s.at[i], l_r.at[i], (rep, near[d])) for i, d in enumerate((4, 1, 2))]
    lsend[0] = lastf[...].astype(BF)
    l_copy[0].start()
    y_copy(1).start()

    @pl.loop(0, BATCH)
    def _(b):
        xbuf[b] = norm_rows(xbuf[b].astype(F32), gain_a[...])

    @pl.loop(2, BATCH)
    def _(b):
        remote(xbuf.at[b], xrecv.at[b], ysend.at[b], yrecv.at[b], (rep, ynb)).start()

    def join_last(i):
        l_copy[i].wait_recv()
        return (lsend[i].astype(F32) + lrecv[i].astype(F32)).astype(BF)

    lsend[1] = join_last(0)
    l_copy[1].start()
    loads[2].wait()

    w_x.wait_recv()
    w_z.start()
    w_xs.start()
    lsend[2] = join_last(1)
    l_copy[2].start()

    def own_x_phase(kv, o):
        @pl.loop(0, BATCH, step=2)
        def _(b):
            project(xbuf, 0, b, o, kv)
            project(xbuf, 0, b + 1, o, kv)
            own_two(b, o, kv).start()

    own_x_phase(rep, 2)
    w_xs.wait_recv()
    own_x_phase(rep, 3)

    rows[0:BATCH, :] = new_tok[...].astype(F32)
    rows[BATCH:2 * BATCH, :] = join_last(2).astype(F32)
    loads[3].wait()
    n16 = norm_rows(rows[...], gain_a[...])
    q16 = jnp.dot(n16, wqb[...], preferred_element_type=F32)
    k16 = jnp.dot(n16, wbuf[0, 0], preferred_element_type=F32)
    v16 = jnp.dot(n16, wbuf[0, 1], preferred_element_type=F32)
    for b in range(BATCH):
        flat[pl.ds(b, 1), 0:HEAD_DIM] = tab[pl.ds(jnp.clip(lens[b], 0, SEQ_LEN), 1), :]
        flat[pl.ds(BATCH + b, 1), 0:HEAD_DIM] = tab[pl.ds(jnp.clip(lens[b] - 1, 0, SEQ_LEN), 1), :]
    c16, s16 = spread(flat[:, 0:HEAD_DIM])
    kself[...] = jnp.zeros_like(kself)
    vself[...] = jnp.zeros_like(vself)
    for h in range(2):
        lanes = slice(h * HEAD_DIM, (h + 1) * HEAD_DIM)
        qh = rotate(q16[:, lanes], c16, s16).astype(BF).astype(F32)
        kh = rotate(k16[:, lanes], c16, s16)[:BATCH].astype(BF).astype(F32)
        vh = v16[:BATCH, lanes].astype(BF).astype(F32)
        for g in range(2):
            qall[0, :, 2 * g + h, :] = qh[g * BATCH:(g + 1) * BATCH]
        kself[:, h, :] = kh
        vself[:, h, :] = vh
        tmp[pl.ds(h, BATCH, stride=2), :] = kh
        tmp[pl.ds(2 * BATCH + h, BATCH, stride=2), :] = vh
    new_out[0] = tmp[0:2 * BATCH, :].astype(BF)
    new_out[1] = tmp[2 * BATCH:4 * BATCH, :].astype(BF)
    low = lax.broadcasted_iota(jnp.int32, (4, HEAD_DIM), 1) < HALF
    part[:, 0] = jnp.zeros((4, BATCH, 4, HEAD_DIM), F32)
    part[:, 1] = jnp.broadcast_to(jnp.where(low, NEG_BIG, 0.0), (4, BATCH, 4, HEAD_DIM))
    q_copy = [remote(qall.at[0], qall.at[d], q_s.at[d - 1], q_r.at[d - 1], (rep, near[d])) for d in (1, 2, 3)]
    for c in q_copy:
        c.start()

    w_s.wait_recv()

    @pl.loop(0, BATCH)
    def _(b):
        @pl.loop(0, 2)
        def _(kv):
            project(xbuf, 0, b, 0, kv)
            project(xbuf, 0, b, 1, kv)
            out_copy(0, b, 1, kv).start()

    w_z.wait_recv()
    w_zs.start()
    w_zs.wait_recv()
    own_x_phase(znb, 2)
    own_x_phase(znb, 3)
    for c in q_copy:
        c.wait_recv()

    lane = lax.broadcasted_iota(jnp.int32, (4, ROWS), 1)
    same_head = lane % 2 == lax.broadcasted_iota(jnp.int32, (4, ROWS), 0) % 2

    def attend(s, b):
        blk = me if s == 0 else ynb
        seen = same_head & (blk * SEQ_LOC + lane // 2 < lens[b])
        four = range(4)
        mine = pl.ds(pl.multiple_of(blk * ROWS, ROWS), ROWS)
        keys, vals = ([kv_out[kv, b, mine, :]] + [stage[s, b, o - 1, kv] for o in (1, 2, 3)] for kv in range(2))
        old = [part[o, 1, b] for o in four]
        acc = [part[o, 0, b] for o in four]
        sc = [lax.dot_general(qall[o, b].astype(BF), keys[o], (((1,), (1,)), ((), ())), preferred_element_type=F32) for o in four]
        sc = [jnp.where(seen, x * SCALE, NEG_BIG) for x in sc]
        top = [jnp.maximum(old[o][:, 0:1], jnp.max(sc[o], axis=-1, keepdims=True)) for o in four]
        p = [jnp.where(seen, jnp.exp(sc[o] - top[o]), 0.0) for o in four]
        fade = [jnp.exp(old[o][:, 0:1] - top[o]) for o in four]
        den = [old[o][:, HALF:HALF + 1] * fade[o] + jnp.sum(p[o], axis=-1, keepdims=True) for o in four]
        add = [jnp.dot(p[o].astype(BF), vals[o], preferred_element_type=F32) for o in four]
        for o in four:
            part[o, 0, b] = acc[o] * fade[o] + add[o]
            part[o, 1, b] = jnp.where(low, top[o], den[o])

    waiting = [(b, kv, o) for b in range(5, BATCH) for kv in range(2) for o in (2, 3)]

    def leave(b, kv, o):
        out_copy(1, b, o, kv).start()

    @pl.loop(0, BATCH)
    def _(b):
        attend(0, b)
        y_copy(b).wait_recv()

        @pl.when(b < 2)
        def _():
            xrecv[b] = norm_rows(xrecv[b].astype(F32), gain_a[...])

        @pl.loop(0, 2)
        def _(kv):
            for o in (2, 3):
                project(xrecv, 1, b, o, kv)

                @pl.when((b < 5) & (kv == 1))
                def _():
                    chunk_kv(b, o).start()

            project(xrecv, 1, b, 1, kv)
            out_copy(1, b, 1, kv).start()
            project(xrecv, 1, b, 0, kv)

        attend(1, b)

    p_copy = [remote(part.at[d], precv.at[d - 1], p_s.at[d - 1], p_r.at[d - 1], (rep, near[d])) for d in (1, 2, 3)]
    for c in p_copy:
        c.start()
    for job in waiting[0:3]:
        leave(*job)
    for load in loads[4:]:
        load.wait()
    first = lax.broadcasted_iota(jnp.int32, (BATCH, 4, 1), 1) < 2
    s_self = jnp.where(first, jnp.sum(qall[0] * kself[...], axis=-1, keepdims=True) * SCALE, NEG_BIG)
    for c in p_copy:
        c.wait_recv()
    accs = [part[0, 0]] + [precv[i, 0] for i in range(3)]
    stats = [part[0, 1]] + [precv[i, 1] for i in range(3)]
    tops = [st[:, :, 0:1] for st in stats]
    top = s_self
    for t in tops:
        top = jnp.maximum(top, t)
    e_self = jnp.where(first, jnp.exp(s_self - top), 0.0)
    den = e_self
    num = e_self * vself[...]
    for t, st, ac in zip(tops, stats, accs):
        e = jnp.exp(t - top)
        den = den + e * st[:, :, HALF:HALF + 1]
        num = num + e * ac
    attn[...] = num / den
    for g in range(2):
        for h in range(2):
            flat[g * BATCH:(g + 1) * BATCH, h * HEAD_DIM:(h + 1) * HEAD_DIM] = attn[:, 2 * g + h, :]

    def reduce_columns(i, base, jobs):
        sends = [remote(psend.at[i, near[d]], rrecv.at[i, d - 1], r_s.at[i, d - 1], r_r.at[i, d - 1], (rep, near[d])) for d in range(1, 8)]
        for c in sends:
            c.start()
        for job in jobs[0]:
            leave(*job)
        total = psend[i, me]
        for d in range(1, 8):
            sends[d - 1].wait_recv()
            total = total + rrecv[i, d - 1]
        hid[i, me] = (base + total).astype(BF)
        gets = [remote(hid.at[i, me], hid.at[i, me], a_s.at[i, d - 1], a_r.at[i, d - 1], (rep, near[d])) for d in range(1, 8)]
        for c in gets:
            c.start()
        for job in jobs[1]:
            leave(*job)
        for d in range(1, 8):
            remote(hid.at[i, near[d]], hid.at[i, near[d]], a_s.at[i, d - 1], a_r.at[i, d - 1], (rep, near[d])).wait_recv()
        return sends + gets

    a16 = flat[...].astype(BF)
    for j in range(8):
        psend[0, j] = jnp.dot(a16, wob[:, j * SHARD:(j + 1) * SHARD], preferred_element_type=F32)
    mine = pl.ds(pl.multiple_of(me * SHARD, SHARD), SHARD)
    done = reduce_columns(0, rows[:, mine], (waiting[3:5], waiting[5:8]))

    sq = jnp.zeros((2 * BATCH, 1), F32)
    for j in range(8):
        hj = hid[0, j].astype(F32)
        sq = sq + jnp.sum(hj * hj, axis=-1, keepdims=True)
    inv = lax.rsqrt(sq / D_MODEL + 1e-5)
    for j in range(8):
        cols = slice(j * SHARD, (j + 1) * SHARD)
        norm2[:, cols] = (hid[0, j].astype(F32) * inv * gain_m[:, cols].astype(F32)).astype(BF)
    n2 = norm2[...]
    gate = jnp.dot(n2, wgb[...], preferred_element_type=F32)
    up = jnp.dot(n2, wub[...], preferred_element_type=F32)
    mid = (gate * jax.nn.sigmoid(gate) * up).astype(BF)
    for j in range(8):
        psend[1, j] = jnp.dot(mid, wdb[:, j * SHARD:(j + 1) * SHARD], preferred_element_type=F32)
    done += reduce_columns(1, hid[0, me].astype(F32), (waiting[8:10], waiting[10:12]))
    for j in range(8):
        cols = slice(j * SHARD, (j + 1) * SHARD)
        dec_out[:, cols] = hid[1, j][:BATCH]
        last_out[:, cols] = hid[1, j][BATCH:]

    for c in [w_x, w_s, w_z, w_xs, w_zs] + l_copy + q_copy + p_copy + done:
        c.wait_send()

    @pl.loop(0, BATCH)
    def _(b):
        y_copy(b).wait_send()
        for kv in range(2):
            for s in range(2):
                out_copy(s, b, 1, kv).wait()

    for o in (2, 3):
        @pl.loop(0, BATCH, step=2)
        def _(b):
            for kv in range(2):
                own_two(b, o, kv).wait()

        @pl.loop(0, 5)
        def _(b):
            chunk_kv(b, o).wait()

    for b, kv, o in waiting:
        out_copy(1, b, o, kv).wait()


def layer(lens, prompt, new_tok, gain_a, gain_m, table, wq, wk, wv, wo, wg, wu, wd):
    vmem = pl.BlockSpec(memory_space=pltpu.VMEM)
    anym = pl.BlockSpec(memory_space=pl.ANY)
    dma = pltpu.SemaphoreType.DMA
    v = pltpu.VMEM
    return pl.pallas_call(
        layer_kernel,
        out_shape=(
            pltpu.VMEM((2, BATCH, 8 * ROWS, HEAD_DIM), BF),
            pltpu.VMEM((2, 2 * BATCH, HEAD_DIM), BF),
            pltpu.VMEM((BATCH, D_MODEL), BF),
            pltpu.VMEM((BATCH, D_MODEL), BF),
        ),
        in_specs=[pl.BlockSpec(memory_space=pltpu.SMEM), anym, vmem, vmem, vmem] + [anym] * 8,
        out_specs=(vmem, vmem, vmem, vmem),
        scratch_shapes=[
            v((BATCH, SEQ_LOC, D_MODEL), BF), v((BATCH, SEQ_LOC, D_MODEL), BF), v((4, 2, D_MODEL, SHARD), BF),
            v((D_MODEL, SHARD), BF), v((SHARD, D_MODEL), BF), v((D_MODEL, FF_LOC), BF), v((D_MODEL, FF_LOC), BF), v((FF_LOC, D_MODEL), BF),
            v((TAB_ROWS, HEAD_DIM), F32), v((ROWS, HEAD_DIM), F32), v((2, BATCH, 3, 2, ROWS, HEAD_DIM), BF),
            v((BATCH, D_MODEL), F32), v((3, BATCH, D_MODEL), BF), v((3, BATCH, D_MODEL), BF), v((2 * BATCH, D_MODEL), F32),
            v((4, BATCH, 4, HEAD_DIM), F32), v((4, 2, BATCH, 4, HEAD_DIM), F32), v((3, 2, BATCH, 4, HEAD_DIM), F32),
            v((BATCH, 4, HEAD_DIM), F32), v((BATCH, 4, HEAD_DIM), F32), v((BATCH, 4, HEAD_DIM), F32), v((2 * BATCH, SHARD), F32),
            v((2, 8, 2 * BATCH, SHARD), F32), v((2, 7, 2 * BATCH, SHARD), F32), v((2, 8, 2 * BATCH, SHARD), BF), v((2 * BATCH, D_MODEL), BF),
            dma((8,)), dma((BATCH,)), dma((BATCH,)), dma((BATCH,)), dma((5,)), dma((5,)),
            dma((3, 2, BATCH, 2)), dma((3, 2, BATCH, 2)),
            dma((3,)), dma((3,)), dma((3,)), dma((3,)), dma((3,)), dma((3,)),
            dma((2, 7)), dma((2, 7)), dma((2, 7)), dma((2, 7)),
        ],
        compiler_params=pltpu.CompilerParams(collective_id=0, has_side_effects=True, vmem_limit_bytes=49 * 1024 * 1024),
        cost_estimate=pl.CostEstimate(flops=26_000_000_000, bytes_accessed=60_000_000, transcendentals=0),
        name='layer',
    )(lens, prompt, new_tok, gain_a, gain_m, table, wq, wk, wv, wo, wg, wu, wd)


def cache_kernel(kv, new, dec, last, key_out, val_out, dec_out, last_out, store, row_sem):
    outs = (key_out, val_out)
    puts = []
    for i in range(2):
        for b in range(BATCH):
            puts.append(pltpu.make_async_copy(kv.at[i, b], outs[i].at[0, b, pl.ds(0, SEQ_LEN)], store.at[i, b]))
            puts[-1].start()
    for i in range(2):
        puts.append(pltpu.make_async_copy(new.at[i], outs[i].at[0, :, pl.ds(SEQ_LEN, 1)], row_sem.at[i]))
        puts[-1].start()
    dec_out[...] = dec[...]
    last_out[...] = last[...]
    for c in puts:
        c.wait()


def caches(kv, new, dec, last):
    anym = pl.BlockSpec(memory_space=pl.ANY)
    dma = pltpu.SemaphoreType.DMA
    vmem = pl.BlockSpec(memory_space=pltpu.VMEM)
    shape = jax.ShapeDtypeStruct((1, BATCH, SEQ_LEN + 1, 2, HEAD_DIM), BF)
    row = jax.ShapeDtypeStruct((BATCH, D_MODEL), BF)
    return pl.pallas_call(
        cache_kernel,
        out_shape=(shape, shape, row, row),
        in_specs=[anym, anym, vmem, vmem],
        out_specs=(anym, anym, vmem, vmem),
        scratch_shapes=[dma((2, BATCH)), dma((2,))],
        compiler_params=pltpu.CompilerParams(vmem_limit_bytes=4 * 1024 * 1024),
        cost_estimate=pl.CostEstimate(flops=0, bytes_accessed=13_000_000, transcendentals=0),
        name='caches',
    )(kv, new, dec, last)


def solution(mesh):
    seq_spec = P('replica', 'model', None)
    col_spec = P(None, None, 'model')
    row_spec = P(None, 'model', None)
    gain_spec = P(None, None)
    tok_spec = P('replica', None)
    cache_spec = P(None, 'replica', None, 'model', None)
    in_specs = (seq_spec, P('replica'), tok_spec, gain_spec, col_spec, col_spec, col_spec, row_spec, gain_spec, col_spec, col_spec, row_spec)
    out_specs = (tok_spec, tok_spec, cache_spec, cache_spec)
    table = rope_table()

    def per_device(prompt, lengths, new_tok, norm_attn, w_q, w_k, w_v, w_o, norm_mlp, w_gate, w_up, w_down):
        kv, new, dec, last = layer(lengths, prompt, new_tok, norm_attn, norm_mlp, jnp.asarray(table), w_q, w_k, w_v, w_o, w_gate, w_up, w_down)
        keys, vals, dec, last = caches(kv.reshape(2, BATCH, SEQ_LEN, 2, HEAD_DIM), new.reshape(2, BATCH, 1, 2, HEAD_DIM), dec, last)
        return dec, last, keys, vals

    return jax.shard_map(per_device, mesh=mesh, in_specs=in_specs, out_specs=out_specs, check_vma=False)
```
